128 devices in a mesh: part: 1, row: 2 (over core), col: 64 (over z, y, x).
Axes of the slice: x: 4, y: 4, z: 4, core: 2. Of those that a mesh axis runs over, the one named last changes fastest.
Arguments:
- ratings: float32 [4096, 32768], P(('part', 'row'), 'col')
- mask: int32 [4096, 32768], P(('part', 'row'), 'col')
- v_init: float32 [32768, 50], P(('part', 'col'))
Outputs:
- output 1: float32 [4096, 50], P(('part', 'row', 'col'))
- output 2: float32 [32768, 50], P(('part', 'col', 'row'))
All inputs are finite; a program needn't handle non-finite values.
Results may differ from the reference program's by a relative error of at most 0.001.
Values are sent between devices in bfloat16 or wider.
A program may use at most 1 GiB of HBM per device.

```python
import jax
import jax.numpy as jnp
from jax import lax

NUM_USERS = 4096
NUM_ITEMS = 32768
FACTOR_DIM = 50
USER_BLOCK = 32
ITEM_BLOCK = 256
RIDGE_WEIGHT = 0.05


def setup_inputs(seed: int = 0, part: int = 0) -> dict:
    part_key = jax.random.fold_in(jax.random.key(seed), part)
    key_rate, key_mask, key_fac = jax.random.split(part_key, 3)
    ratings = jax.random.normal(key_rate, (NUM_USERS, NUM_ITEMS), dtype=jnp.float32)
    mask = jax.random.randint(key_mask, (NUM_USERS, NUM_ITEMS), 0, 2, dtype=jnp.int32)
    fac_scale = (NUM_USERS / 2) ** 0.25 / (NUM_ITEMS / 2) ** 0.5
    v_init = fac_scale * jax.random.normal(key_fac, (NUM_ITEMS, FACTOR_DIM), dtype=jnp.float32)
    return {"ratings": ratings, "mask": mask, "v_init": v_init}


def outer_rows(fac_b):
    row_count = fac_b.shape[0]
    fac_wide = fac_b.astype(jnp.float32)
    outer_prod = fac_wide[:, :, None] * fac_wide[:, None, :]
    return outer_prod.reshape(row_count, FACTOR_DIM * FACTOR_DIM).astype(jnp.bfloat16)


def solve_rows(gram, rhs):
    row_count = gram.shape[0]
    gram_mats = gram.reshape(row_count, FACTOR_DIM, FACTOR_DIM) + RIDGE_WEIGHT * jnp.eye(FACTOR_DIM, dtype=jnp.float32)
    chol_fac = jnp.linalg.cholesky(gram_mats)
    fwd_sol = lax.linalg.triangular_solve(chol_fac, rhs[:, :, None], left_side=True, lower=True)
    solved = lax.linalg.triangular_solve(chol_fac, fwd_sol, left_side=True, lower=True, transpose_a=True)
    return solved[:, :, 0]


def reference(ratings, mask, v_init):
    mask_b = mask.astype(jnp.bfloat16)
    rated_b = (ratings * mask.astype(jnp.float32)).astype(jnp.bfloat16)
    v_b = v_init.astype(jnp.bfloat16)
    outer_v = outer_rows(v_b)

    def user_block(block_idx):
        m_rows = lax.dynamic_slice_in_dim(mask_b, block_idx * USER_BLOCK, USER_BLOCK, 0)
        r_rows = lax.dynamic_slice_in_dim(rated_b, block_idx * USER_BLOCK, USER_BLOCK, 0)
        gram = jnp.dot(m_rows, outer_v, preferred_element_type=jnp.float32)
        rhs = jnp.dot(r_rows, v_b, preferred_element_type=jnp.float32)
        return solve_rows(gram, rhs)

    w_new = lax.map(user_block, jnp.arange(NUM_USERS // USER_BLOCK)).reshape(NUM_USERS, FACTOR_DIM)
    w_b = w_new.astype(jnp.bfloat16)
    outer_w = outer_rows(w_b)

    def item_block(block_idx):
        m_cols = lax.dynamic_slice_in_dim(mask_b, block_idx * ITEM_BLOCK, ITEM_BLOCK, 1)
        r_cols = lax.dynamic_slice_in_dim(rated_b, block_idx * ITEM_BLOCK, ITEM_BLOCK, 1)
        gram = jnp.dot(m_cols.T, outer_w, preferred_element_type=jnp.float32)
        rhs = jnp.dot(r_cols.T, w_b, preferred_element_type=jnp.float32)
        return solve_rows(gram, rhs)

    v_new = lax.map(item_block, jnp.arange(NUM_ITEMS // ITEM_BLOCK)).reshape(NUM_ITEMS, FACTOR_DIM)
    return w_new, v_new
```

```python
import jax
import jax.numpy as jnp
from jax import lax
from jax.experimental import pallas as pl
from jax.experimental.pallas import tpu as pltpu
from jax.sharding import PartitionSpec as P

RIDGE_WEIGHT = 0.05
WIDTH = 50
ROWS = 56
TRI = 1280
LANES = 128


def tri_off(j):
    return j * WIDTH - j * (j - 1) // 2


def outer_tile(vt, dst):
    lanes = vt.shape[1]
    for j in range(WIDTH):
        rows = WIDTH - j
        dst[tri_off(j):tri_off(j) + rows, :] = vt[j:WIDTH, :] * vt[j:j + 1, :]


def outer_kernel(vt_ref, out_ref, tmp):
    tmp[1272:1280, :] = jnp.zeros((8, tmp.shape[1]), jnp.float32)
    outer_tile(vt_ref, tmp)
    out_ref[...] = tmp[...].astype(jnp.bfloat16)


def outer_rows(vt):
    n = vt.shape[1]
    step = min(n, 512)
    return pl.pallas_call(
        outer_kernel,
        out_shape=jax.ShapeDtypeStruct((TRI, n), jnp.bfloat16),
        grid=(n // step,),
        in_specs=[pl.BlockSpec((64, step), lambda i: (0, i))],
        out_specs=pl.BlockSpec((TRI, step), lambda i: (0, i)),
        scratch_shapes=[pltpu.VMEM((TRI, step), jnp.float32)],
    )(vt)


def solve_tile(g_ref, rhs, fac, inv, sol):
    lanes = fac.shape[1]
    for pan in range(7):
        first = 8 * pan
        rows = ROWS - first
        count = min(8, WIDTH - first)
        ids = lax.broadcasted_iota(jnp.int32, (rows, lanes), 0)
        accs = []
        for c in range(count):
            j = first + c
            start = tri_off(j) - c
            if j < WIDTH - 1:
                raw = g_ref[start:start + rows, :]
            else:
                raw = jnp.broadcast_to(g_ref[tri_off(j):tri_off(j) + 1, :], (rows, lanes))
            col = jnp.where(ids < WIDTH - first, raw, 0.0)
            col = jnp.where(ids == c, col + RIDGE_WEIGHT, col)
            col = jnp.where(ids == WIDTH - first, rhs(j), col)
            accs.append(col)
        if pan:
            def body(k, accs):
                base = pl.multiple_of(k * ROWS, 8)
                left = fac[pl.ds(base + first, rows), :]
                return tuple(
                    acc - left * fac[pl.ds(base + first + c, 1), :] for c, acc in enumerate(accs)
                )
            accs = list(lax.fori_loop(0, first, body, tuple(accs), unroll=2))
        for c in range(count):
            j = first + c
            diag = accs[c][c:c + 1, :]
            root = lax.rsqrt(diag)
            root = root * (1.5 - 0.5 * (diag * root) * root)
            inv[j:j + 1, :] = root
            col = accs[c] * root
            fac[pl.ds(j * ROWS + first, rows), :] = col
            for later in range(c + 1, count):
                accs[later] = accs[later] - col * col[later:later + 1, :]
    sol[48:56, :] = jnp.zeros((8, lanes), jnp.float32)
    for pan in reversed(range(7)):
        first = 8 * pan
        count = min(8, WIDTH - first)
        left = []
        for c in range(count):
            j = first + c
            val = fac[j * ROWS + WIDTH:j * ROWS + WIDTH + 1, :]
            if pan < 6:
                dot = fac[j * ROWS + first + 8:j * ROWS + ROWS, :] * sol[first + 8:ROWS, :]
                val = val - jnp.sum(dot, axis=0, keepdims=True)
            left.append(val)
        for c in reversed(range(count)):
            j = first + c
            got = left[c] * inv[j:j + 1, :]
            sol[j:j + 1, :] = got
            for early in range(c):
                row = (first + early) * ROWS + j
                left[early] = left[early] - fac[row:row + 1, :] * got


def solve_kernel(g_ref, b_ref, out_ref, fac, inv, sol):
    solve_tile(g_ref, lambda j: b_ref[j:j + 1, :], fac, inv, sol)
    out_ref[...] = sol[...]


def solve_rows(gram, rhs):
    n = gram.shape[1]
    return pl.pallas_call(
        solve_kernel,
        out_shape=jax.ShapeDtypeStruct((ROWS, n), jnp.float32),
        grid=(n // LANES,),
        in_specs=[pl.BlockSpec((TRI, LANES), lambda i: (0, i)), pl.BlockSpec((ROWS, LANES), lambda i: (0, i))],
        out_specs=pl.BlockSpec((ROWS, LANES), lambda i: (0, i)),
        scratch_shapes=[
            pltpu.VMEM((WIDTH * ROWS, LANES), jnp.float32),
            pltpu.VMEM((ROWS, LANES), jnp.float32),
            pltpu.VMEM((ROWS, LANES), jnp.float32),
        ],
    )(gram, rhs)


def solution(mesh):
    block_spec = P(("part", "row"), "col")
    in_specs = (block_spec, block_spec, P(("part", "col"), None))
    out_specs = (P(("part", "row", "col"), None), P(("part", "col", "row"), None))
    contract_cols = (((1,), (1,)), ((), ()))
    contract_rows = (((1,), (0,)), ((), ()))

    def local_als(ratings, mask, v_init):
        mask_b = mask.astype(jnp.bfloat16)
        rated_b = jnp.where(mask != 0, ratings, 0.0).astype(jnp.bfloat16)
        v_b = v_init.T.astype(jnp.bfloat16)
        vt = jnp.pad(v_b.astype(jnp.float32), ((0, 64 - WIDTH), (0, 0)))
        contract_items = (((1,), (1,)), ((), ()))
        gram_part = lax.dot_general(mask_b, outer_rows(vt), contract_items, preferred_element_type=jnp.float32)
        rhs_part = lax.dot_general(rated_b, v_b, contract_items, preferred_element_type=jnp.float32)
        both = jnp.concatenate([gram_part, rhs_part], axis=1)
        own = lax.psum_scatter(both, "col", scatter_dimension=0, tiled=True).T
        own = jnp.pad(own, ((0, ROWS - WIDTH), (0, LANES - own.shape[1])))
        w_own = solve_rows(own[:TRI], own[TRI:])[:WIDTH, :32].T
        w_rows = lax.all_gather(w_own.astype(jnp.bfloat16), "col", axis=0, tiled=True)
        wt = jnp.pad(w_rows.T, ((0, 64 - WIDTH), (0, 0)))
        gram_item = lax.dot_general(outer_rows(wt.astype(jnp.float32)), mask_b, contract_rows, preferred_element_type=jnp.float32)
        rhs_item = lax.dot_general(wt[:ROWS], rated_b, contract_rows, preferred_element_type=jnp.float32)
        both_item = jnp.concatenate([gram_item, rhs_item], axis=0)
        iown = lax.psum_scatter(both_item, "row", scatter_dimension=1, tiled=True)
        v_own = solve_rows(iown[:TRI], iown[TRI:])[:WIDTH].T
        return w_own, v_own

    return jax.shard_map(local_als, mesh=mesh, in_specs=in_specs, out_specs=out_specs, check_vma=False)
```

```python
import jax
import jax.numpy as jnp
from jax import lax
from jax.experimental import pallas as pl
from jax.experimental.pallas import tpu as pltpu
from jax.sharding import PartitionSpec as P

RIDGE_WEIGHT = 0.05
WIDTH = 50
ROWS = 56
TRI = 1280
LANES = 128


def tri_off(j):
    return j * WIDTH - j * (j - 1) // 2


def outer_tile(vt, dst):
    lanes = vt.shape[1]
    for j in range(WIDTH):
        rows = WIDTH - j
        dst[tri_off(j):tri_off(j) + rows, :] = vt[j:WIDTH, :] * vt[j:j + 1, :]


def solve_tile(g_ref, rhs, fac, inv, sol):
    lanes = fac.shape[1]
    for pan in range(7):
        first = 8 * pan
        rows = ROWS - first
        count = min(8, WIDTH - first)
        ids = lax.broadcasted_iota(jnp.int32, (rows, lanes), 0)
        accs = []
        for c in range(count):
            j = first + c
            start = tri_off(j) - c
            if j < WIDTH - 1:
                raw = g_ref[start:start + rows, :]
            else:
                raw = jnp.broadcast_to(g_ref[tri_off(j):tri_off(j) + 1, :], (rows, lanes))
            col = jnp.where(ids < WIDTH - first, raw, 0.0)
            col = jnp.where(ids == c, col + RIDGE_WEIGHT, col)
            col = jnp.where(ids == WIDTH - first, rhs(j), col)
            accs.append(col)
        if pan:
            def body(k, accs):
                base = pl.multiple_of(k * ROWS, 8)
                left = fac[pl.ds(base + first, rows), :]
                return tuple(
                    acc - left * fac[pl.ds(base + first + c, 1), :] for c, acc in enumerate(accs)
                )
            accs = list(lax.fori_loop(0, first, body, tuple(accs), unroll=2))
        for c in range(count):
            j = first + c
            diag = accs[c][c:c + 1, :]
            root = lax.rsqrt(diag)
            root = root * (1.5 - 0.5 * (diag * root) * root)
            inv[j:j + 1, :] = root
            col = accs[c] * root
            fac[pl.ds(j * ROWS + first, rows), :] = col
            for later in range(c + 1, count):
                accs[later] = accs[later] - col * col[later:later + 1, :]
    sol[48:56, :] = jnp.zeros((8, lanes), jnp.float32)
    for pan in reversed(range(7)):
        first = 8 * pan
        count = min(8, WIDTH - first)
        left = []
        for c in range(count):
            j = first + c
            val = fac[j * ROWS + WIDTH:j * ROWS + WIDTH + 1, :]
            if pan < 6:
                dot = fac[j * ROWS + first + 8:j * ROWS + ROWS, :] * sol[first + 8:ROWS, :]
                val = val - jnp.sum(dot, axis=0, keepdims=True)
            left.append(val)
        for c in reversed(range(count)):
            j = first + c
            got = left[c] * inv[j:j + 1, :]
            sol[j:j + 1, :] = got
            for early in range(c):
                row = (first + early) * ROWS + j
                left[early] = left[early] - fac[row:row + 1, :] * got


def item_solve_kernel(g_ref, out_ref, fac, inv, sol):
    solve_tile(g_ref, lambda j: g_ref[TRI + j:TRI + j + 1, :], fac, inv, sol)
    out_ref[...] = sol[:WIDTH, :]


def solve_items(packed):
    n = packed.shape[1]
    return pl.pallas_call(
        item_solve_kernel,
        out_shape=jax.ShapeDtypeStruct((WIDTH, n), jnp.float32),
        grid=(n // LANES,),
        in_specs=[pl.BlockSpec((packed.shape[0], LANES), lambda i: (0, i))],
        out_specs=pl.BlockSpec((WIDTH, LANES), lambda i: (0, i)),
        scratch_shapes=[
            pltpu.VMEM((WIDTH * ROWS, LANES), jnp.float32),
            pltpu.VMEM((ROWS, LANES), jnp.float32),
            pltpu.VMEM((ROWS, LANES), jnp.float32),
        ],
    )(packed)


PACK = 1344
FULL = 1408
SIDE = 4
HALF = PACK // 2


def cast_kernel(rate_ref, mask_ref, out_ref):
    groups = out_ref.shape[0]
    mask = mask_ref[...]
    out_ref[:, 0] = mask.astype(jnp.float32).astype(jnp.bfloat16).reshape(groups, 16, mask.shape[1])
    rated = jnp.where(mask != 0, rate_ref[...], 0.0)
    out_ref[:, 1] = rated.astype(jnp.bfloat16).reshape(groups, 16, mask.shape[1])


def cast_rows(ratings, mask):
    users, items = ratings.shape
    step = users // 8
    return pl.pallas_call(
        cast_kernel,
        out_shape=jax.ShapeDtypeStruct((users // 16, 2, 16, items), jnp.bfloat16),
        grid=(8,),
        in_specs=[pl.BlockSpec((step, items), lambda i: (i, 0))] * 2,
        out_specs=pl.BlockSpec((step // 16, 2, 16, items), lambda i: (i, 0, 0, 0)),
    )(ratings, mask)


def dot_cols(left, right):
    return lax.dot_general(left, right, (((1,), (1,)), ((), ())), preferred_element_type=jnp.float32)


def gram_kernel(
    mq, vt_ref, out_ref, rhs, vt_all, o_all, tmp, gram, rel, got, tot, flat, fin,
    v_send, v_recv, m_send, m_recv, own_sem, rel_send, rel_recv, got_send, got_recv, fin_send, fin_recv,
):
    items = vt_ref.shape[1]
    col = lax.axis_index("col")
    x = lax.rem(col, SIDE)
    y = lax.rem(col // SIDE, SIDE)
    z = col // (SIDE * SIDE)

    def turn(pos, step):
        return lax.rem(pos + step, SIDE)

    def x_peer(step):
        return {"col": col - x + turn(x, step)}

    def y_peer(step):
        return {"col": col + SIDE * (turn(y, step) - y)}

    def z_peer(step):
        return {"col": col + SIDE * SIDE * (turn(z, step) - z)}

    def send(src, dst, send_sem, recv_sem, peer):
        return pltpu.make_async_remote_copy(
            src_ref=src, dst_ref=dst, send_sem=send_sem, recv_sem=recv_sem,
            device_id=peer, device_id_type=pl.DeviceIdType.MESH,
        )

    barrier = pltpu.get_barrier_semaphore()
    peers = [x_peer(1), x_peer(2), x_peer(3), y_peer(1), y_peer(2), y_peer(3), z_peer(1), z_peer(3)]
    for peer in peers:
        pl.semaphore_signal(barrier, inc=1, device_id=peer, device_id_type=pl.DeviceIdType.MESH)
    pl.semaphore_wait(barrier, len(peers))

    v_copies = []
    for d in (1, 3, 2):
        for axis, peer in enumerate((x_peer(d), y_peer(d))):
            slot = 3 * axis + d
            v_copies.append(send(
                vt_ref, vt_all.at[:, slot * items:(slot + 1) * items],
                v_send.at[slot - 1], v_recv.at[slot - 1], peer,
            ))
    for copy in v_copies:
        copy.start()

    owners = [turn(z, 2), turn(z, 1), turn(z, 3), z]
    m_copies = []
    for k, owner in enumerate(owners):
        chunk = []
        for c, src in enumerate((mq.at[owner, :, x, 0], mq.at[owner, y, :, 1])):
            copy = pltpu.make_async_copy(src, rhs.at[k, c, :, :, :, 0:items], own_sem.at[k, c])
            chunk.append(copy)
            copy.start()
        for d in (1, 3, 2):
            for c, (src, peer) in enumerate((
                (mq.at[owner, :, turn(x, d), 0], x_peer(d)), (mq.at[owner, turn(y, d), :, 1], y_peer(d)),
            )):
                slot = 3 * c + d
                copy = send(
                    src, rhs.at[k, c, :, :, :, slot * items:(slot + 1) * items],
                    m_send.at[k, slot - 1], m_recv.at[k, slot - 1], peer,
                )
                chunk.append(copy)
                copy.start()
        m_copies.append(chunk)

    for k in range(4):
        rhs[k, 0, :, :, :, 4 * items:7 * items] = jnp.zeros((4, 2, 16, 3 * items), jnp.bfloat16)
        rhs[k, 1, :, :, :, items:4 * items] = jnp.zeros((4, 2, 16, 3 * items), jnp.bfloat16)
    tmp[1272:1280, :] = jnp.zeros((8, items), jnp.float32)
    vt_all[:, 0:items] = vt_ref[...]

    def outer_slot(slot):
        cols = pl.ds(pl.multiple_of(slot * items, items), items)
        vt = vt_all[:, cols].astype(jnp.float32)
        outer_tile(vt, tmp)
        o_all[:, cols] = tmp[...].astype(jnp.bfloat16)

    def outer_step(slot, carry):
        outer_slot(slot)
        return carry

    outer_slot(0)
    for copy in v_copies:
        copy.wait()
    lax.fori_loop(1, 7, outer_step, 0)

    def partial(k, store):
        for copy in m_copies[k]:
            copy.wait()

        def rows_step(i, carry):
            rows = pl.ds(pl.multiple_of(i * 320, 320), 320)
            store(rows, dot_cols(o_all[rows, :], rhs[k, :, :, 0].reshape(128, 7 * items)))
            return carry

        store(pl.ds(TRI, 64), dot_cols(vt_all[...], rhs[k, :, :, 1].reshape(128, 7 * items)))
        lax.fori_loop(0, 4, rows_step, 0)

    def keep(k):
        def store(rows, val):
            gram[k, rows, :] = val
        return store

    partial(0, keep(0))
    relays = [
        send(gram.at[0, 0:HALF], rel.at[0], rel_send.at[0], rel_recv.at[0], z_peer(1)),
        send(gram.at[0, HALF:PACK], rel.at[1], rel_send.at[1], rel_recv.at[1], z_peer(3)),
    ]
    for copy in relays:
        copy.start()
    partial(1, keep(1))
    relays[0].wait()
    gram[1, 0:HALF, :] = gram[1, 0:HALF, :] + rel[0]
    up = send(gram.at[1], got.at[0], got_send.at[0], got_recv.at[0], z_peer(1))
    up.start()
    partial(2, keep(2))
    relays[1].wait()
    gram[2, HALF:PACK, :] = gram[2, HALF:PACK, :] + rel[1]
    down = send(gram.at[2], got.at[1], got_send.at[1], got_recv.at[1], z_peer(3))
    down.start()

    def keep_own(rows, val):
        tot[rows, :] = val

    partial(3, keep_own)
    up.wait()
    down.wait()
    tot[PACK:FULL, :] = jnp.zeros((FULL - PACK, 128), jnp.float32)
    tot[0:PACK, :] = tot[0:PACK, :] + got[0] + got[1]
    for i in range(FULL // 128):
        flat[:, i * 128:(i + 1) * 128] = tot[i * 128:(i + 1) * 128, :].T
    f_copies = []
    for d in (2, 1, 3):
        for c, (pos, peer) in enumerate(((turn(y, d), y_peer(d)), (turn(x, d), x_peer(d)))):
            rows = pl.ds(pl.multiple_of(64 * c + 16 * pos, 16), 16)
            copy = send(flat.at[rows], fin.at[c, d - 1], fin_send.at[c, d - 1], fin_recv.at[c, d - 1], peer)
            copy.start()
            f_copies.append(copy)
    for copy in f_copies:
        copy.wait()
    for c, pos in enumerate((y, x)):
        rows = pl.ds(pl.multiple_of(64 * c + 16 * pos, 16), 16)
        out_ref[c * 16:(c + 1) * 16, :] = flat[rows, :] + fin[c, 0] + fin[c, 1] + fin[c, 2]


def gram_users(mq, vt):
    items = vt.shape[1]
    dma = pltpu.SemaphoreType.DMA
    return pl.pallas_call(
        gram_kernel,
        out_shape=jax.ShapeDtypeStruct((32, FULL), jnp.float32),
        in_specs=[pl.BlockSpec(memory_space=pl.ANY), pl.BlockSpec(memory_space=pltpu.VMEM)],
        out_specs=pl.BlockSpec(memory_space=pltpu.VMEM),
        scratch_shapes=[
            pltpu.VMEM((4, 2, 4, 2, 16, 7 * items), jnp.bfloat16),
            pltpu.VMEM((64, 7 * items), jnp.bfloat16),
            pltpu.VMEM((TRI, 7 * items), jnp.bfloat16),
            pltpu.VMEM((TRI, items), jnp.float32),
            pltpu.VMEM((3, PACK, 128), jnp.float32),
            pltpu.VMEM((2, HALF, 128), jnp.float32),
            pltpu.VMEM((2, PACK, 128), jnp.float32),
            pltpu.VMEM((FULL, 128), jnp.float32),
            pltpu.VMEM((128, FULL), jnp.float32),
            pltpu.VMEM((2, 3, 16, FULL), jnp.float32),
            dma((6,)), dma((6,)), dma((4, 6)), dma((4, 6)), dma((4, 2)),
            dma((2,)), dma((2,)), dma((2,)), dma((2,)), dma((2, 3)), dma((2, 3)),
        ],
        compiler_params=pltpu.CompilerParams(
            collective_id=0, has_side_effects=True, vmem_limit_bytes=60 * 1024 * 1024
        ),
    )(mq, vt)


def user_kernel(flat_ref, w_ref, pack_ref, gram, fac, inv, sol):
    zeros = jnp.zeros((96, 128), jnp.float32)
    for i in range(FULL // 128):
        cols = slice(i * 128, (i + 1) * 128)
        gram[cols, :] = jnp.concatenate([flat_ref[:, cols], zeros], axis=0).T
    solve_tile(gram, lambda j: gram[TRI + j:TRI + j + 1, :], fac, inv, sol)
    turned = jnp.concatenate([sol[...], jnp.zeros((72, 128), jnp.float32)], axis=0).T
    w_ref[...] = turned[:32, :WIDTH]
    lane = lax.broadcasted_iota(jnp.int32, (16, 128), 1)
    pack_ref[...] = jnp.where(lane < 64, turned[:16], pltpu.roll(turned[16:32], 64, 1)).astype(jnp.bfloat16)


def solve_users(flat):
    return pl.pallas_call(
        user_kernel,
        out_shape=(jax.ShapeDtypeStruct((32, WIDTH), jnp.float32), jax.ShapeDtypeStruct((16, 128), jnp.bfloat16)),
        scratch_shapes=[
            pltpu.VMEM((FULL, 128), jnp.float32),
            pltpu.VMEM((WIDTH * ROWS, 128), jnp.float32),
            pltpu.VMEM((ROWS, 128), jnp.float32),
            pltpu.VMEM((ROWS, 128), jnp.float32),
        ],
    )(flat)


def item_kernel(
    count, mq, pack_ref, out_ref, w_all, mqv, wt, wb, prods, tmp, part, got,
    w_send, w_recv, mq_sem, own_sem, x_send, x_recv,
):
    items = mqv.shape[-1]
    share = items // 2
    col = lax.axis_index("col")
    row = lax.axis_index("row")
    other = {"row": 1 - row}

    barrier = pltpu.get_barrier_semaphore()

    def signal_step(d, carry):
        pl.semaphore_signal(
            barrier, inc=1, device_id={"col": lax.rem(col + d, count)}, device_id_type=pl.DeviceIdType.MESH
        )
        return carry

    lax.fori_loop(1, count, signal_step, 0)
    pl.semaphore_signal(barrier, inc=1, device_id=other, device_id_type=pl.DeviceIdType.MESH)
    pl.semaphore_wait(barrier, count)

    def w_copy(d):
        return pltpu.make_async_remote_copy(
            src_ref=pack_ref, dst_ref=w_all.at[col], send_sem=w_send.at[d], recv_sem=w_recv.at[d],
            device_id={"col": lax.rem(col + d, count)}, device_id_type=pl.DeviceIdType.MESH,
        )

    def send_step(d, carry):
        w_copy(d).start()
        return carry

    lax.fori_loop(1, count, send_step, 0)
    w_own = pltpu.make_async_copy(pack_ref, w_all.at[col], own_sem.at[0])
    w_own.start()
    loads = []
    for c in range(2):
        for m in range(2):
            copy = pltpu.make_async_copy(mq.at[:, c, m], mqv.at[m, c], mq_sem.at[m, c])
            copy.start()
            loads.append(copy)
    w_own.wait()

    def wait_step(d, carry):
        w_copy(d).wait()
        return carry

    lax.fori_loop(1, count, wait_step, 0)
    for copy in loads:
        copy.wait()

    users = 16 * count
    for i in range(users // 128):
        block = w_all[8 * i:8 * i + 8].reshape(128, 128).astype(jnp.float32).T
        wt[:, i * 128:(i + 1) * 128] = block
    for c in range(2):
        wb[:, c * users:(c + 1) * users] = wt[64 * c:64 * c + 64, :].astype(jnp.bfloat16)
    step = tmp.shape[1]
    tmp[1272:1280, :] = jnp.zeros((8, step), jnp.float32)
    per = users // step

    def outer_step(i, carry):
        c = i // per
        rows = pl.ds(pl.multiple_of(64 * c, 64), 64)
        cols = pl.ds(pl.multiple_of((i - c * per) * step, step), step)
        outer_tile(wt.at[rows, cols], tmp)
        prods[:, pl.ds(pl.multiple_of(i * step, step), step)] = tmp[...].astype(jnp.bfloat16)
        return carry

    lax.fori_loop(0, 2 * per, outer_step, 0)

    def partial(half, dst):
        cols = pl.ds(pl.multiple_of(half * share, share), share)
        dst[TRI:PACK, :] = jnp.dot(
            wb[...], mqv[1, :, :, :, cols].reshape(2 * users, share), preferred_element_type=jnp.float32
        )

        def rows_step(i, carry):
            rows = pl.ds(pl.multiple_of(i * 320, 320), 320)
            dst[rows, :] = jnp.dot(
                prods[rows, :], mqv[0, :, :, :, cols].reshape(2 * users, share), preferred_element_type=jnp.float32
            )
            return carry

        lax.fori_loop(0, 4, rows_step, 0)

    partial(1 - row, part)
    swap = pltpu.make_async_remote_copy(
        src_ref=part, dst_ref=got, send_sem=x_send, recv_sem=x_recv,
        device_id=other, device_id_type=pl.DeviceIdType.MESH,
    )
    swap.start()
    partial(row, out_ref)
    swap.wait()
    out_ref[...] = out_ref[...] + got[...]


def gram_items(mq, pack, count):
    items = mq.shape[-1]
    users = 16 * count
    step = min(512, users)
    dma = pltpu.SemaphoreType.DMA
    return pl.pallas_call(
        lambda *refs: item_kernel(count, *refs),
        out_shape=jax.ShapeDtypeStruct((PACK, items // 2), jnp.float32),
        in_specs=[pl.BlockSpec(memory_space=pl.ANY), pl.BlockSpec(memory_space=pltpu.VMEM)],
        out_specs=pl.BlockSpec(memory_space=pltpu.VMEM),
        scratch_shapes=[
            pltpu.VMEM((count, 16, 128), jnp.bfloat16),
            pltpu.VMEM((2, 2, count, 16, items), jnp.bfloat16),
            pltpu.VMEM((128, users), jnp.float32),
            pltpu.VMEM((64, 2 * users), jnp.bfloat16),
            pltpu.VMEM((TRI, 2 * users), jnp.bfloat16),
            pltpu.VMEM((TRI, step), jnp.float32),
            pltpu.VMEM((PACK, items // 2), jnp.float32),
            pltpu.VMEM((PACK, items // 2), jnp.float32),
            dma((count,)), dma((count,)), dma((2, 2)), dma((1,)), dma, dma,
        ],
        compiler_params=pltpu.CompilerParams(
            collective_id=1, has_side_effects=True, vmem_limit_bytes=60 * 1024 * 1024
        ),
    )(mq, pack)


def solution(mesh):
    block_spec = P(("part", "row"), "col")
    in_specs = (block_spec, block_spec, P(("part", "col"), None))
    out_specs = (P(("part", "row", "col"), None), P(("part", "col", "row"), None))
    count = mesh.shape["col"]

    def local_als(ratings, mask, v_init):
        items = ratings.shape[1]
        mq = cast_rows(ratings, mask)
        vt = jnp.pad(v_init.T.astype(jnp.bfloat16), ((0, 64 - WIDTH), (0, 0)))
        flat = gram_users(mq.reshape(SIDE, SIDE, SIDE, 2, 2, 16, items), vt)
        w_own, w_pack = solve_users(flat)
        packed = gram_items(mq.reshape(count, 2, 2, 16, items), w_pack, count)
        v_own = solve_items(packed).T
        return w_own, v_own

    return jax.shard_map(local_als, mesh=mesh, in_specs=in_specs, out_specs=out_specs, check_vma=False)
```

```python
import jax
import jax.numpy as jnp
from jax import lax
from jax.experimental import pallas as pl
from jax.experimental.pallas import tpu as pltpu
from jax.sharding import PartitionSpec as P

RIDGE_WEIGHT = 0.05
WIDTH = 50
ROWS = 56
TRI = 1280
LANES = 128


def tri_off(j):
    return j * WIDTH - j * (j - 1) // 2


def outer_tile(vt, dst):
    lanes = vt.shape[1]
    for j in range(WIDTH):
        rows = WIDTH - j
        dst[tri_off(j):tri_off(j) + rows, :] = vt[j:WIDTH, :] * vt[j:j + 1, :]


def solve_tile(g_ref, rhs, fac, inv, sol):
    lanes = fac.shape[1]
    for pan in range(7):
        first = 8 * pan
        rows = ROWS - first
        count = min(8, WIDTH - first)
        ids = lax.broadcasted_iota(jnp.int32, (rows, lanes), 0)
        accs = []
        for c in range(count):
            j = first + c
            start = tri_off(j) - c
            if j < WIDTH - 1:
                raw = g_ref[start:start + rows, :]
            else:
                raw = jnp.broadcast_to(g_ref[tri_off(j):tri_off(j) + 1, :], (rows, lanes))
            col = jnp.where(ids < WIDTH - first, raw, 0.0)
            col = jnp.where(ids == c, col + RIDGE_WEIGHT, col)
            col = jnp.where(ids == WIDTH - first, rhs(j), col)
            accs.append(col)
        if pan:
            def body(k, accs):
                base = pl.multiple_of(k * ROWS, 8)
                left = fac[pl.ds(base + first, rows), :]
                return tuple(
                    acc - left * fac[pl.ds(base + first + c, 1), :] for c, acc in enumerate(accs)
                )
            accs = list(lax.fori_loop(0, first, body, tuple(accs), unroll=2))
        for c in range(count):
            j = first + c
            diag = accs[c][c:c + 1, :]
            root = lax.rsqrt(diag)
            root = root * (1.5 - 0.5 * (diag * root) * root)
            inv[j:j + 1, :] = root
            col = accs[c] * root
            fac[pl.ds(j * ROWS + first, rows), :] = col
            for later in range(c + 1, count):
                accs[later] = accs[later] - col * col[later:later + 1, :]
    sol[48:56, :] = jnp.zeros((8, lanes), jnp.float32)
    for pan in reversed(range(7)):
        first = 8 * pan
        count = min(8, WIDTH - first)
        left = []
        for c in range(count):
            j = first + c
            val = fac[j * ROWS + WIDTH:j * ROWS + WIDTH + 1, :]
            if pan < 6:
                dot = fac[j * ROWS + first + 8:j * ROWS + ROWS, :] * sol[first + 8:ROWS, :]
                val = val - jnp.sum(dot, axis=0, keepdims=True)
            left.append(val)
        for c in reversed(range(count)):
            j = first + c
            got = left[c] * inv[j:j + 1, :]
            sol[j:j + 1, :] = got
            for early in range(c):
                row = (first + early) * ROWS + j
                left[early] = left[early] - fac[row:row + 1, :] * got


def item_solve_kernel(g_ref, out_ref, fac, inv, sol):
    solve_tile(g_ref, lambda j: g_ref[TRI + j:TRI + j + 1, :], fac, inv, sol)
    out_ref[...] = sol[:WIDTH, :]


def solve_items(packed):
    n = packed.shape[1]
    return pl.pallas_call(
        item_solve_kernel,
        out_shape=jax.ShapeDtypeStruct((WIDTH, n), jnp.float32),
        grid=(n // LANES,),
        in_specs=[pl.BlockSpec((packed.shape[0], LANES), lambda i: (0, i))],
        out_specs=pl.BlockSpec((WIDTH, LANES), lambda i: (0, i)),
        scratch_shapes=[
            pltpu.VMEM((WIDTH * ROWS, LANES), jnp.float32),
            pltpu.VMEM((ROWS, LANES), jnp.float32),
            pltpu.VMEM((ROWS, LANES), jnp.float32),
        ],
    )(packed)


PACK = 1344
FULL = 1408
SIDE = 4
HALF = PACK // 2


def dot_cols(left, right):
    return lax.dot_general(left, right, (((1,), (1,)), ((), ())), preferred_element_type=jnp.float32)


def gram_kernel(
    rate_hbm, mask_hbm, v_ref, out_ref, mq_out, rate, mask, mqs, hop, rhs, vt_all, o_all, tmp, gram, rel, got, tot, flat, fin,
    load_sem, save_sem, v_send, v_recv, m_send, m_recv, hop_send, hop_recv, fwd_send, fwd_recv, own_sem,
    rel_send, rel_recv, got_send, got_recv, fin_send, fin_recv,
):
    items = v_ref.shape[1]
    col = lax.axis_index("col")
    x = lax.rem(col, SIDE)
    y = lax.rem(col // SIDE, SIDE)
    z = col // (SIDE * SIDE)

    def turn(pos, step):
        return lax.rem(pos + step, SIDE)

    def x_peer(step):
        return {"col": col - x + turn(x, step)}

    def y_peer(step):
        return {"col": col + SIDE * (turn(y, step) - y)}

    def z_peer(step):
        return {"col": col + SIDE * SIDE * (turn(z, step) - z)}

    def send(src, dst, send_sem, recv_sem, peer):
        return pltpu.make_async_remote_copy(
            src_ref=src, dst_ref=dst, send_sem=send_sem, recv_sem=recv_sem,
            device_id=peer, device_id_type=pl.DeviceIdType.MESH,
        )

    owners = [turn(z, 2), turn(z, 1), turn(z, 3), z]
    block = rate.shape[1]
    loads = []
    for k, owner in enumerate(owners):
        rows = pl.ds(pl.multiple_of(owner * block, block), block)
        pair = [
            pltpu.make_async_copy(rate_hbm.at[rows], rate.at[k], load_sem.at[k, 0]),
            pltpu.make_async_copy(mask_hbm.at[rows], mask.at[k], load_sem.at[k, 1]),
        ]
        for copy in pair:
            copy.start()
        loads.append(pair)

    barrier = pltpu.get_barrier_semaphore()
    peers = [x_peer(1), x_peer(2), x_peer(3), y_peer(1), y_peer(2), y_peer(3), z_peer(1), z_peer(3)]
    for peer in peers:
        pl.semaphore_signal(barrier, inc=1, device_id=peer, device_id_type=pl.DeviceIdType.MESH)
    tmp[48:64, :] = jnp.zeros((16, items), jnp.float32)
    tmp[0:WIDTH, :] = v_ref[...]
    vt_all[:, 0:items] = tmp[0:64, :].astype(jnp.bfloat16)
    pl.semaphore_wait(barrier, len(peers))

    v_copies = []
    for d in (1, 3, 2):
        for axis, peer in enumerate((x_peer(d), y_peer(d))):
            slot = 3 * axis + d
            v_copies.append(send(
                vt_all.at[:, 0:items], vt_all.at[:, slot * items:(slot + 1) * items],
                v_send.at[slot - 1], v_recv.at[slot - 1], peer,
            ))
    for copy in v_copies:
        copy.start()

    def cast_chunk(k):
        for copy in loads[k]:
            copy.wait()

        def cast_step(i, carry):
            rows = pl.ds(pl.multiple_of(i * 128, 128), 128)
            seen = mask[k, rows, :]
            mqs[k, i, :, :, 0] = seen.astype(jnp.float32).astype(jnp.bfloat16).reshape(SIDE, 2, 16, items)
            rated = jnp.where(seen != 0, rate[k, rows, :], 0.0)
            mqs[k, i, :, :, 1] = rated.astype(jnp.bfloat16).reshape(SIDE, 2, 16, items)
            return carry

        lax.fori_loop(0, SIDE, cast_step, 0)

    def axis_peer(c, step):
        return y_peer(step) if c else x_peer(step)

    def share(k, c, pos):
        return mqs.at[k, pos, :, 1] if c else mqs.at[k, :, pos, 0]

    def columns(slot):
        return slice(slot * items, (slot + 1) * items)

    m_copies, hops, passes, saves = [], [], [], []
    for k, owner in enumerate(owners):
        saves.append(pltpu.make_async_copy(mqs.at[k], mq_out.at[owner], save_sem.at[k]))
        m_copies.append([])
        hops.append([])
        passes.append([])
        for c, pos in enumerate((x, y)):
            m_copies[k].append(pltpu.make_async_copy(
                share(k, c, pos), rhs.at[k, c, :, :, :, columns(0)], own_sem.at[k, c]
            ))
            for m, step in enumerate((1, 3)):
                hops[k].append(send(
                    share(k, c, turn(pos, 2)).at[:, m], hop.at[k, c, m],
                    hop_send.at[k, c, m], hop_recv.at[k, c, m], axis_peer(c, step),
                ))
                m_copies[k].append(send(
                    share(k, c, turn(pos, step)), rhs.at[k, c, :, :, :, columns(3 * c + step)],
                    m_send.at[k, c, m], m_recv.at[k, c, m], axis_peer(c, step),
                ))
                passes[k].append(send(
                    hop.at[k, c, m], rhs.at[k, c, :, m, :, columns(3 * c + 2)],
                    fwd_send.at[k, c, m], fwd_recv.at[k, c, m], axis_peer(c, step),
                ))

    def start_chunk(k):
        for copy in hops[k] + m_copies[k]:
            copy.start()
        saves[k].start()

    def pass_on(k):
        for copy, follow in zip(hops[k], passes[k]):
            copy.wait()
            follow.start()

    cast_chunk(0)
    start_chunk(0)
    cast_chunk(1)
    start_chunk(1)
    cast_chunk(2)
    cast_chunk(3)
    for k in range(4):
        rhs[k, 0, :, :, :, 4 * items:7 * items] = jnp.zeros((4, 2, 16, 3 * items), jnp.bfloat16)
        rhs[k, 1, :, :, :, items:4 * items] = jnp.zeros((4, 2, 16, 3 * items), jnp.bfloat16)
    tmp[1272:1280, :] = jnp.zeros((8, items), jnp.float32)

    def outer_step(slot, carry):
        cols = pl.ds(pl.multiple_of(slot * items, items), items)
        outer_tile(vt_all[:, cols].astype(jnp.float32), tmp)
        o_all[:, cols] = tmp[...].astype(jnp.bfloat16)
        return carry

    pass_on(0)
    start_chunk(2)
    for copy in v_copies:
        copy.wait()
    lax.fori_loop(0, 4, outer_step, 0)
    pass_on(1)
    start_chunk(3)
    lax.fori_loop(4, 7, outer_step, 0)

    def partial(k, store):
        for copy in m_copies[k] + passes[k]:
            copy.wait()

        def rows_step(i, carry):
            rows = pl.ds(pl.multiple_of(i * 320, 320), 320)
            store(rows, dot_cols(o_all[rows, :], rhs[k, :, :, 0].reshape(128, 7 * items)))
            return carry

        store(pl.ds(TRI, 64), dot_cols(vt_all[...], rhs[k, :, :, 1].reshape(128, 7 * items)))
        lax.fori_loop(0, 4, rows_step, 0)

    def keep(k):
        def store(rows, val):
            gram[k, rows, :] = val
        return store

    partial(0, keep(0))
    relays = [
        send(gram.at[0, 0:HALF], rel.at[0], rel_send.at[0], rel_recv.at[0], z_peer(1)),
        send(gram.at[0, HALF:PACK], rel.at[1], rel_send.at[1], rel_recv.at[1], z_peer(3)),
    ]
    for copy in relays:
        copy.start()
    pass_on(2)
    partial(1, keep(1))
    relays[0].wait()
    gram[1, 0:HALF, :] = gram[1, 0:HALF, :] + rel[0]
    up = send(gram.at[1], got.at[0], got_send.at[0], got_recv.at[0], z_peer(1))
    up.start()
    pass_on(3)
    partial(2, keep(2))
    relays[1].wait()
    gram[2, HALF:PACK, :] = gram[2, HALF:PACK, :] + rel[1]
    down = send(gram.at[2], got.at[1], got_send.at[1], got_recv.at[1], z_peer(3))
    down.start()

    def keep_own(rows, val):
        tot[rows, :] = val

    partial(3, keep_own)
    for copy in saves:
        copy.wait()
    up.wait()
    down.wait()
    tot[PACK:FULL, :] = jnp.zeros((FULL - PACK, 128), jnp.float32)
    tot[0:PACK, :] = tot[0:PACK, :] + got[0] + got[1]
    for i in range(FULL // 128):
        flat[:, i * 128:(i + 1) * 128] = tot[i * 128:(i + 1) * 128, :].T
    f_copies = []
    for d in (2, 1, 3):
        for c, (pos, peer) in enumerate(((turn(y, d), y_peer(d)), (turn(x, d), x_peer(d)))):
            rows = pl.ds(pl.multiple_of(64 * c + 16 * pos, 16), 16)
            copy = send(flat.at[rows], fin.at[c, d - 1], fin_send.at[c, d - 1], fin_recv.at[c, d - 1], peer)
            copy.start()
            f_copies.append(copy)
    for copy in f_copies:
        copy.wait()
    for c, pos in enumerate((y, x)):
        rows = pl.ds(pl.multiple_of(64 * c + 16 * pos, 16), 16)
        out_ref[c * 16:(c + 1) * 16, :] = flat[rows, :] + fin[c, 0] + fin[c, 1] + fin[c, 2]


def gram_users(ratings, mask, vt):
    users, items = ratings.shape
    block = users // SIDE
    dma = pltpu.SemaphoreType.DMA
    return pl.pallas_call(
        gram_kernel,
        out_shape=(
            jax.ShapeDtypeStruct((32, FULL), jnp.float32),
            jax.ShapeDtypeStruct((SIDE, SIDE, SIDE, 2, 2, 16, items), jnp.bfloat16),
        ),
        in_specs=[
            pl.BlockSpec(memory_space=pl.ANY), pl.BlockSpec(memory_space=pl.ANY), pl.BlockSpec(memory_space=pltpu.VMEM)
        ],
        out_specs=(pl.BlockSpec(memory_space=pltpu.VMEM), pl.BlockSpec(memory_space=pl.ANY)),
        scratch_shapes=[
            pltpu.VMEM((4, block, items), jnp.float32),
            pltpu.VMEM((4, block, items), jnp.int32),
            pltpu.VMEM((4, SIDE, SIDE, 2, 2, 16, items), jnp.bfloat16),
            pltpu.VMEM((4, 2, 2, SIDE, 16, items), jnp.bfloat16),
            pltpu.VMEM((4, 2, SIDE, 2, 16, 7 * items), jnp.bfloat16),
            pltpu.VMEM((64, 7 * items), jnp.bfloat16),
            pltpu.VMEM((TRI, 7 * items), jnp.bfloat16),
            pltpu.VMEM((TRI, items), jnp.float32),
            pltpu.VMEM((3, PACK, 128), jnp.float32),
            pltpu.VMEM((2, HALF, 128), jnp.float32),
            pltpu.VMEM((2, PACK, 128), jnp.float32),
            pltpu.VMEM((FULL, 128), jnp.float32),
            pltpu.VMEM((128, FULL), jnp.float32),
            pltpu.VMEM((2, 3, 16, FULL), jnp.float32),
            dma((4, 2)), dma((4,)), dma((6,)), dma((6,)), dma((4, 2, 2)), dma((4, 2, 2)), dma((4, 2, 2)), dma((4, 2, 2)),
            dma((4, 2, 2)), dma((4, 2, 2)), dma((4, 2)),
            dma((2,)), dma((2,)), dma((2,)), dma((2,)), dma((2, 3)), dma((2, 3)),
        ],
        compiler_params=pltpu.CompilerParams(
            collective_id=0, has_side_effects=True, vmem_limit_bytes=60 * 1024 * 1024
        ),
    )(ratings, mask, vt)


def user_kernel(flat_ref, w_ref, pack_ref, gram, fac, inv, sol):
    zeros = jnp.zeros((96, 128), jnp.float32)
    for i in range(FULL // 128):
        cols = slice(i * 128, (i + 1) * 128)
        gram[cols, :] = jnp.concatenate([flat_ref[:, cols], zeros], axis=0).T
    solve_tile(gram, lambda j: gram[TRI + j:TRI + j + 1, :], fac, inv, sol)
    turned = jnp.concatenate([sol[...], jnp.zeros((72, 128), jnp.float32)], axis=0).T
    w_ref[...] = turned[:32, :WIDTH]
    lane = lax.broadcasted_iota(jnp.int32, (16, 128), 1)
    pack_ref[...] = jnp.where(lane < 64, turned[:16], pltpu.roll(turned[16:32], 64, 1)).astype(jnp.bfloat16)


def solve_users(flat):
    return pl.pallas_call(
        user_kernel,
        out_shape=(jax.ShapeDtypeStruct((32, WIDTH), jnp.float32), jax.ShapeDtypeStruct((16, 128), jnp.bfloat16)),
        scratch_shapes=[
            pltpu.VMEM((FULL, 128), jnp.float32),
            pltpu.VMEM((WIDTH * ROWS, 128), jnp.float32),
            pltpu.VMEM((ROWS, 128), jnp.float32),
            pltpu.VMEM((ROWS, 128), jnp.float32),
        ],
    )(flat)


def item_kernel(
    count, mq, pack_ref, out_ref, w_all, mqv, wt, wb, prods, tmp, part, got,
    w_send, w_recv, mq_sem, own_sem, x_send, x_recv,
):
    items = mqv.shape[-1]
    share = items // 2
    col = lax.axis_index("col")
    row = lax.axis_index("row")
    other = {"row": 1 - row}

    barrier = pltpu.get_barrier_semaphore()

    def signal_step(d, carry):
        pl.semaphore_signal(
            barrier, inc=1, device_id={"col": lax.rem(col + d, count)}, device_id_type=pl.DeviceIdType.MESH
        )
        return carry

    lax.fori_loop(1, count, signal_step, 0)
    pl.semaphore_signal(barrier, inc=1, device_id=other, device_id_type=pl.DeviceIdType.MESH)
    pl.semaphore_wait(barrier, count)

    def w_copy(d):
        return pltpu.make_async_remote_copy(
            src_ref=pack_ref, dst_ref=w_all.at[col], send_sem=w_send.at[d], recv_sem=w_recv.at[d],
            device_id={"col": lax.rem(col + d, count)}, device_id_type=pl.DeviceIdType.MESH,
        )

    def send_step(d, carry):
        w_copy(d).start()
        return carry

    lax.fori_loop(1, count, send_step, 0)
    w_own = pltpu.make_async_copy(pack_ref, w_all.at[col], own_sem.at[0])
    w_own.start()
    loads = []
    for c in range(2):
        for m in range(2):
            copy = pltpu.make_async_copy(mq.at[:, c, m], mqv.at[m, c], mq_sem.at[m, c])
            copy.start()
            loads.append(copy)
    w_own.wait()

    def wait_step(d, carry):
        w_copy(d).wait()
        return carry

    lax.fori_loop(1, count, wait_step, 0)
    for copy in loads:
        copy.wait()

    users = 16 * count
    for i in range(users // 128):
        block = w_all[8 * i:8 * i + 8].reshape(128, 128).astype(jnp.float32).T
        wt[:, i * 128:(i + 1) * 128] = block
    for c in range(2):
        wb[:, c * users:(c + 1) * users] = wt[64 * c:64 * c + 64, :].astype(jnp.bfloat16)
    step = tmp.shape[1]
    tmp[1272:1280, :] = jnp.zeros((8, step), jnp.float32)
    per = users // step

    def outer_step(i, carry):
        c = i // per
        rows = pl.ds(pl.multiple_of(64 * c, 64), 64)
        cols = pl.ds(pl.multiple_of((i - c * per) * step, step), step)
        outer_tile(wt.at[rows, cols], tmp)
        prods[:, pl.ds(pl.multiple_of(i * step, step), step)] = tmp[...].astype(jnp.bfloat16)
        return carry

    lax.fori_loop(0, 2 * per, outer_step, 0)

    def partial(half, dst):
        cols = pl.ds(pl.multiple_of(half * share, share), share)
        dst[TRI:PACK, :] = jnp.dot(
            wb[...], mqv[1, :, :, :, cols].reshape(2 * users, share), preferred_element_type=jnp.float32
        )

        def rows_step(i, carry):
            rows = pl.ds(pl.multiple_of(i * 320, 320), 320)
            dst[rows, :] = jnp.dot(
                prods[rows, :], mqv[0, :, :, :, cols].reshape(2 * users, share), preferred_element_type=jnp.float32
            )
            return carry

        lax.fori_loop(0, 4, rows_step, 0)

    partial(1 - row, part)
    swap = pltpu.make_async_remote_copy(
        src_ref=part, dst_ref=got, send_sem=x_send, recv_sem=x_recv,
        device_id=other, device_id_type=pl.DeviceIdType.MESH,
    )
    swap.start()
    partial(row, out_ref)
    swap.wait()
    out_ref[...] = out_ref[...] + got[...]


def gram_items(mq, pack, count):
    items = mq.shape[-1]
    users = 16 * count
    step = min(512, users)
    dma = pltpu.SemaphoreType.DMA
    return pl.pallas_call(
        lambda *refs: item_kernel(count, *refs),
        out_shape=jax.ShapeDtypeStruct((PACK, items // 2), jnp.float32),
        in_specs=[pl.BlockSpec(memory_space=pl.ANY), pl.BlockSpec(memory_space=pltpu.VMEM)],
        out_specs=pl.BlockSpec(memory_space=pltpu.VMEM),
        scratch_shapes=[
            pltpu.VMEM((count, 16, 128), jnp.bfloat16),
            pltpu.VMEM((2, 2, count, 16, items), jnp.bfloat16),
            pltpu.VMEM((128, users), jnp.float32),
            pltpu.VMEM((64, 2 * users), jnp.bfloat16),
            pltpu.VMEM((TRI, 2 * users), jnp.bfloat16),
            pltpu.VMEM((TRI, step), jnp.float32),
            pltpu.VMEM((PACK, items // 2), jnp.float32),
            pltpu.VMEM((PACK, items // 2), jnp.float32),
            dma((count,)), dma((count,)), dma((2, 2)), dma((1,)), dma, dma,
        ],
        compiler_params=pltpu.CompilerParams(
            collective_id=1, has_side_effects=True, vmem_limit_bytes=60 * 1024 * 1024
        ),
    )(mq, pack)


def solution(mesh):
    block_spec = P(("part", "row"), "col")
    in_specs = (block_spec, block_spec, P(("part", "col"), None))
    out_specs = (P(("part", "row", "col"), None), P(("part", "col", "row"), None))
    count = mesh.shape["col"]

    def local_als(ratings, mask, v_init):
        items = ratings.shape[1]
        flat, mq = gram_users(ratings, mask, v_init.T)
        w_own, w_pack = solve_users(flat)
        packed = gram_items(mq.reshape(count, 2, 2, 16, items), w_pack, count)
        v_own = solve_items(packed).T
        return w_own, v_own

    return jax.shard_map(local_als, mesh=mesh, in_specs=in_specs, out_specs=out_specs, check_vma=False)
```

```python
import jax
import jax.numpy as jnp
from jax import lax
from jax.experimental import pallas as pl
from jax.experimental.pallas import tpu as pltpu
from jax.sharding import PartitionSpec as P

RIDGE_WEIGHT = 0.05
WIDTH = 50
ROWS = 56
TRI = 1280
LANES = 128


def tri_off(j):
    return j * WIDTH - j * (j - 1) // 2


def outer_tile(vt, dst):
    lanes = vt.shape[1]
    for j in range(WIDTH):
        rows = WIDTH - j
        dst[tri_off(j):tri_off(j) + rows, :] = vt[j:WIDTH, :] * vt[j:j + 1, :]


def solve_tile(g_ref, rhs, fac, inv, sol):
    lanes = fac.shape[1]
    for pan in range(7):
        first = 8 * pan
        rows = ROWS - first
        count = min(8, WIDTH - first)
        ids = lax.broadcasted_iota(jnp.int32, (rows, lanes), 0)
        accs = []
        for c in range(count):
            j = first + c
            start = tri_off(j) - c
            if j < WIDTH - 1:
                raw = g_ref[start:start + rows, :]
            else:
                raw = jnp.broadcast_to(g_ref[tri_off(j):tri_off(j) + 1, :], (rows, lanes))
            col = jnp.where(ids < WIDTH - first, raw, 0.0)
            col = jnp.where(ids == c, col + RIDGE_WEIGHT, col)
            col = jnp.where(ids == WIDTH - first, rhs(j), col)
            accs.append(col)
        if pan:
            def body(k, accs):
                base = pl.multiple_of(k * ROWS, 8)
                left = fac[pl.ds(base + first, rows), :]
                return tuple(
                    acc - left * fac[pl.ds(base + first + c, 1), :] for c, acc in enumerate(accs)
                )
            accs = list(lax.fori_loop(0, first, body, tuple(accs), unroll=2))
        for c in range(count):
            j = first + c
            diag = accs[c][c:c + 1, :]
            root = lax.rsqrt(diag)
            root = root * (1.5 - 0.5 * (diag * root) * root)
            inv[j:j + 1, :] = root
            col = accs[c] * root
            fac[pl.ds(j * ROWS + first, rows), :] = col
            for later in range(c + 1, count):
                accs[later] = accs[later] - col * col[later:later + 1, :]
    sol[48:56, :] = jnp.zeros((8, lanes), jnp.float32)
    for pan in reversed(range(7)):
        first = 8 * pan
        count = min(8, WIDTH - first)
        left = []
        for c in range(count):
            j = first + c
            val = fac[j * ROWS + WIDTH:j * ROWS + WIDTH + 1, :]
            if pan < 6:
                dot = fac[j * ROWS + first + 8:j * ROWS + ROWS, :] * sol[first + 8:ROWS, :]
                val = val - jnp.sum(dot, axis=0, keepdims=True)
            left.append(val)
        for c in reversed(range(count)):
            j = first + c
            got = left[c] * inv[j:j + 1, :]
            sol[j:j + 1, :] = got
            for early in range(c):
                row = (first + early) * ROWS + j
                left[early] = left[early] - fac[row:row + 1, :] * got


def item_solve_kernel(g_ref, out_ref, fac, inv, sol):
    solve_tile(g_ref, lambda j: g_ref[TRI + j:TRI + j + 1, :], fac, inv, sol)
    out_ref[...] = sol[:WIDTH, :]


def solve_items(packed):
    n = packed.shape[1]
    return pl.pallas_call(
        item_solve_kernel,
        out_shape=jax.ShapeDtypeStruct((WIDTH, n), jnp.float32),
        grid=(n // LANES,),
        in_specs=[pl.BlockSpec((packed.shape[0], LANES), lambda i: (0, i))],
        out_specs=pl.BlockSpec((WIDTH, LANES), lambda i: (0, i)),
        scratch_shapes=[
            pltpu.VMEM((WIDTH * ROWS, LANES), jnp.float32),
            pltpu.VMEM((ROWS, LANES), jnp.float32),
            pltpu.VMEM((ROWS, LANES), jnp.float32),
        ],
    )(packed)


PACK = 1344
FULL = 1408
SIDE = 4
HALF = PACK // 2


def dot_cols(left, right):
    return lax.dot_general(left, right, (((1,), (1,)), ((), ())), preferred_element_type=jnp.float32)


def als_kernel(
    rate_hbm, mask_hbm, v_ref, w_ref, item_ref,
    rate, mask, mqs, hop, rhs, vt_all, o_all, tmp, gram, unit, rel, got, tot, flat, fin,
    fac, inv, sol, pack, w_all, wt, wb, part, swap_got,
    load_sem, v_send, v_recv, m_send, m_recv, hop_send, hop_recv, fwd_send, fwd_recv, own_sem,
    rel_send, rel_recv, got_send, got_recv, fin_send, fin_recv, w_send, w_recv, w_sem, x_send, x_recv, y_in, z_in,
):
    items = v_ref.shape[1]
    count = w_all.shape[0]
    col = lax.axis_index("col")
    row = lax.axis_index("row")
    other = {"row": 1 - row}
    x = lax.rem(col, SIDE)
    y = lax.rem(col // SIDE, SIDE)
    z = col // (SIDE * SIDE)

    def turn(pos, step):
        return lax.rem(pos + step, SIDE)

    def x_peer(step):
        return {"col": col - x + turn(x, step)}

    def y_peer(step):
        return {"col": col + SIDE * (turn(y, step) - y)}

    def z_peer(step):
        return {"col": col + SIDE * SIDE * (turn(z, step) - z)}

    def send(src, dst, send_sem, recv_sem, peer):
        return pltpu.make_async_remote_copy(
            src_ref=src, dst_ref=dst, send_sem=send_sem, recv_sem=recv_sem,
            device_id=peer, device_id_type=pl.DeviceIdType.MESH,
        )

    def signal(sem, peer):
        pl.semaphore_signal(sem, inc=1, device_id=peer, device_id_type=pl.DeviceIdType.MESH)

    barrier = pltpu.get_barrier_semaphore()
    peers = [peer(step) for step in (1, 2, 3) for peer in (x_peer, y_peer, z_peer)] + [other]
    for peer in peers:
        signal(barrier, peer)

    owners = [turn(z, 2), turn(z, 1), turn(z, 3), z]
    block = rate.shape[1]
    loads = []
    for k, owner in enumerate(owners):
        rows = pl.ds(pl.multiple_of(owner * block, block), block)
        pair = [
            pltpu.make_async_copy(rate_hbm.at[rows], rate.at[k], load_sem.at[k, 0]),
            pltpu.make_async_copy(mask_hbm.at[rows], mask.at[k], load_sem.at[k, 1]),
        ]
        for copy in pair:
            copy.start()
        loads.append(pair)

    def cast_chunk(k):
        for copy in loads[k]:
            copy.wait()

        def cast_step(i, carry):
            rows = pl.ds(pl.multiple_of(i * 128, 128), 128)
            seen = mask[k, rows, :]
            mqs[k, i, :, :, 0] = seen.astype(jnp.float32).astype(jnp.bfloat16).reshape(SIDE, 2, 16, items)
            rated = jnp.where(seen != 0, rate[k, rows, :], 0.0)
            mqs[k, i, :, :, 1] = rated.astype(jnp.bfloat16).reshape(SIDE, 2, 16, items)
            return carry

        lax.fori_loop(0, SIDE, cast_step, 0)

    def axis_peer(c, step):
        return y_peer(step) if c else x_peer(step)

    def share(s, c, pos):
        return mqs.at[(0, 2, 1, 3)[s], pos, :, 1] if c else mqs.at[s, :, pos, 0]

    def columns(slot):
        return slice(slot * items, (slot + 1) * items)

    m_copies, hops, passes = [], [], []
    for s in range(4):
        m_copies.append([])
        hops.append([])
        passes.append([])
        for c, pos in enumerate((x, y)):
            for m, step in enumerate((1, 3)):
                hops[s].append(send(
                    share(s, c, turn(pos, 2)).at[:, m], hop.at[s, c, m],
                    hop_send.at[s, c, m], hop_recv.at[s, c, m], axis_peer(c, step),
                ))
                m_copies[s].append(send(
                    share(s, c, turn(pos, step)), rhs.at[s, c, :, :, :, columns(3 * c + step)],
                    m_send.at[s, c, m], m_recv.at[s, c, m], axis_peer(c, step),
                ))
                passes[s].append(send(
                    hop.at[s, c, m], rhs.at[s, c, :, m, :, columns(3 * c + 2)],
                    fwd_send.at[s, c, m], fwd_recv.at[s, c, m], axis_peer(c, step),
                ))
            m_copies[s].append(pltpu.make_async_copy(
                share(s, c, pos), rhs.at[s, c, :, :, :, columns(0)], own_sem.at[s, c]
            ))

    def start_stage(s):
        for copy in hops[s] + m_copies[s]:
            copy.start()

    def pass_on(s):
        for copy, follow in zip(hops[s], passes[s]):
            copy.wait()
            follow.start()

    tmp[48:64, :] = jnp.zeros((16, items), jnp.float32)
    tmp[0:WIDTH, :] = v_ref[...]
    vt_all[:, 0:items] = tmp[0:64, :].astype(jnp.bfloat16)
    cast_chunk(0)
    pl.semaphore_wait(barrier, len(peers))
    start_stage(0)
    v_copies = []
    for d in (1, 3, 2):
        for axis in range(2):
            slot = 3 * axis + d
            v_copies.append(send(
                vt_all.at[:, columns(0)], vt_all.at[:, columns(slot)],
                v_send.at[slot - 1], v_recv.at[slot - 1], axis_peer(axis, d),
            ))
    for copy in v_copies:
        copy.start()
    for step in (1, 2, 3):
        signal(y_in, y_peer(step))
    for k in range(1, 4):
        cast_chunk(k)
    for s in range(4):
        rhs[s, 0, :, :, :, 4 * items:7 * items] = jnp.zeros((4, 2, 16, 3 * items), jnp.bfloat16)
        rhs[s, 1, :, :, :, items:4 * items] = jnp.zeros((4, 2, 16, 3 * items), jnp.bfloat16)
    tmp[1272:1280, :] = jnp.zeros((8, items), jnp.float32)

    def outer_step(slot, carry):
        cols = pl.ds(pl.multiple_of(slot * items, items), items)
        outer_tile(vt_all[:, cols].astype(jnp.float32), tmp)
        o_all[:, cols] = tmp[...].astype(jnp.bfloat16)
        return carry

    lax.fori_loop(0, 1, outer_step, 0)
    pass_on(0)
    start_stage(1)
    pl.semaphore_wait(y_in, 3)
    for step in (1, 2, 3):
        signal(z_in, z_peer(step))
    for copy in v_copies:
        copy.wait()
    lax.fori_loop(1, 7, outer_step, 0)

    def partial(s, dst):
        for copy in m_copies[s] + passes[s]:
            copy.wait()

        def rows_step(i, carry):
            rows = pl.ds(pl.multiple_of(i * 320, 320), 320)
            dst[rows, :] = dot_cols(o_all[rows, :], rhs[s, :, :, 0].reshape(128, 7 * items))
            return carry

        dst[TRI:PACK, :] = dot_cols(vt_all[...], rhs[s, :, :, 1].reshape(128, 7 * items))
        lax.fori_loop(0, 4, rows_step, 0)

    low = lax.broadcasted_iota(jnp.int32, (HALF, 128), 1) < 64

    def pack_units(s):
        top, bottom = gram[0:HALF, :], gram[HALF:PACK, :]
        unit[s, 0] = jnp.where(low, top, pltpu.roll(bottom, 64, 1))
        unit[s, 1] = jnp.where(low, pltpu.roll(top, 64, 1), bottom)

    pieces = (slice(0, HALF // 2), slice(HALF // 2, HALF))
    ways = (1, 3)
    partial(0, gram)
    pack_units(0)
    relays = [[
        send(unit.at[0, c, rows], rel.at[c, rows], rel_send.at[c, p], rel_recv.at[c, p], z_peer(ways[c]))
        for c in range(2)
    ] for p, rows in enumerate(pieces)]
    for piece in relays:
        for copy in piece:
            copy.start()
    pass_on(1)
    start_stage(2)
    partial(1, gram)
    pack_units(1)
    z_copies = []
    pass_on(2)
    start_stage(3)
    for p, rows in enumerate(pieces):
        for c in range(2):
            relays[p][c].wait()
            unit[1, c, rows, :] = unit[1, c, rows, :] + rel[c, rows, :]
            copy = send(
                unit.at[1, c, rows], got.at[0, c, rows], got_send.at[0, c, p], got_recv.at[0, c, p], z_peer(ways[c])
            )
            copy.start()
            z_copies.append(copy)
    pass_on(3)
    partial(2, gram)
    pack_units(2)
    for c in range(2):
        copy = send(
            unit.at[2, c], got.at[1, c], got_send.at[1, c, 0], got_recv.at[1, c, 0], z_peer(ways[1 - c])
        )
        copy.start()
        z_copies.append(copy)
    partial(3, tot)
    tot[PACK:FULL, :] = jnp.zeros((FULL - PACK, 128), jnp.float32)
    for copy in z_copies:
        copy.wait()
    sum_a = got[0, 0] + got[1, 0]
    sum_b = got[0, 1] + got[1, 1]
    tot[0:HALF, :] = tot[0:HALF, :] + jnp.where(low, sum_a, pltpu.roll(sum_b, 64, 1))
    tot[HALF:PACK, :] = tot[HALF:PACK, :] + jnp.where(low, pltpu.roll(sum_a, 64, 1), sum_b)
    for i in range(FULL // 128):
        flat[:, i * 128:(i + 1) * 128] = tot[i * 128:(i + 1) * 128, :].T
    f_copies = []
    for d in (2, 1, 3):
        for c, pos in enumerate((y, x)):
            rows = pl.ds(pl.multiple_of(64 * c + 16 * turn(pos, d), 16), 16)
            copy = send(
                flat.at[rows], fin.at[c, d - 1], fin_send.at[c, d - 1], fin_recv.at[c, d - 1], axis_peer(1 - c, d)
            )
            copy.start()
            f_copies.append(copy)
    pl.semaphore_wait(z_in, 3)
    for copy in f_copies:
        copy.wait()

    zeros = jnp.zeros((96, 128), jnp.float32)
    for i in range(FULL // 128):
        cols = slice(i * 128, (i + 1) * 128)
        mine = [zeros]
        for c, pos in ((1, x), (0, y)):
            rows = pl.ds(pl.multiple_of(64 * c + 16 * pos, 16), 16)
            mine.insert(0, flat[rows, cols] + fin[c, 0, :, cols] + fin[c, 1, :, cols] + fin[c, 2, :, cols])
        tot[cols, :] = jnp.concatenate(mine, axis=0).T
    solve_tile(tot, lambda j: tot[TRI + j:TRI + j + 1, :], fac, inv, sol)
    turned = jnp.concatenate([sol[...], jnp.zeros((72, 128), jnp.float32)], axis=0).T
    lane = lax.broadcasted_iota(jnp.int32, (16, 128), 1)
    pack[...] = jnp.where(lane < 64, turned[:16], pltpu.roll(turned[16:32], 64, 1)).astype(jnp.bfloat16)

    def w_copy(d):
        return send(pack, w_all.at[col], w_send.at[d], w_recv.at[d], {"col": lax.rem(col + d, count)})

    def send_step(d, carry):
        w_copy(d).start()
        return carry

    def wait_step(d, carry):
        w_copy(d).wait()
        return carry

    lax.fori_loop(1, count, send_step, 0)
    w_own = pltpu.make_async_copy(pack, w_all.at[col], w_sem)
    w_own.start()
    w_ref[...] = turned[:32, :WIDTH]
    w_own.wait()
    lax.fori_loop(1, count, wait_step, 0)

    users = 16 * count
    for i in range(users // 128):
        wt[:, i * 128:(i + 1) * 128] = w_all[8 * i:8 * i + 8].reshape(128, 128).astype(jnp.float32).T
    step = users // SIDE
    tall = tmp.at[:, 0:step]
    tall[1272:1280, :] = jnp.zeros((8, step), jnp.float32)

    def w_step(i, carry):
        c = i // SIDE
        k = i - c * SIDE
        owner = turn(z, 2 - k + (k // 2) * (2 * k - 1))
        rows = pl.ds(pl.multiple_of(64 * c, 64), 64)
        vals = wt[rows, pl.ds(pl.multiple_of(owner * step, step), step)]
        cols = pl.ds(pl.multiple_of(i * step, step), step)
        wb[:, cols] = vals.astype(jnp.bfloat16)
        outer_tile(vals, tall)
        o_all[:, cols] = tall[...].astype(jnp.bfloat16)
        return carry

    lax.fori_loop(0, 2 * SIDE, w_step, 0)
    half = items // 2

    def item_partial(side, dst):
        cols = pl.ds(pl.multiple_of(side * half, half), half)

        def both(left, m):
            total = None
            for c in range(2):
                right = mqs[:, :, :, c, m, :, cols].reshape(users, half)
                term = jnp.dot(left(c), right, preferred_element_type=jnp.float32)
                total = term if total is None else total + term
            return total

        dst[TRI:PACK, :] = both(lambda c: wb[:, c * users:(c + 1) * users], 1)

        def rows_step(i, carry):
            rows = pl.ds(pl.multiple_of(i * 320, 320), 320)
            dst[rows, :] = both(lambda c: o_all[rows, c * users:(c + 1) * users], 0)
            return carry

        lax.fori_loop(0, 4, rows_step, 0)

    item_partial(1 - row, part)
    swap = send(part, swap_got, x_send, x_recv, other)
    swap.start()
    item_partial(row, item_ref)
    swap.wait()
    item_ref[...] = item_ref[...] + swap_got[...]


def half_steps(ratings, mask, vt, count):
    users, items = ratings.shape
    block = users // SIDE
    dma = pltpu.SemaphoreType.DMA
    any_spec = pl.BlockSpec(memory_space=pl.ANY)
    vmem_spec = pl.BlockSpec(memory_space=pltpu.VMEM)
    f32, bf16 = jnp.float32, jnp.bfloat16
    return pl.pallas_call(
        als_kernel,
        out_shape=(
            jax.ShapeDtypeStruct((32, WIDTH), f32),
            jax.ShapeDtypeStruct((PACK, items // 2), f32),
        ),
        in_specs=[any_spec, any_spec, vmem_spec],
        out_specs=(vmem_spec, vmem_spec),
        scratch_shapes=[
            pltpu.VMEM((4, block, items), f32),
            pltpu.VMEM((4, block, items), jnp.int32),
            pltpu.VMEM((4, SIDE, SIDE, 2, 2, 16, items), bf16),
            pltpu.VMEM((4, 2, 2, SIDE, 16, items), bf16),
            pltpu.VMEM((4, 2, SIDE, 2, 16, 7 * items), bf16),
            pltpu.VMEM((64, 7 * items), bf16),
            pltpu.VMEM((TRI, 7 * items), bf16),
            pltpu.VMEM((TRI, items), f32),
            pltpu.VMEM((PACK, 128), f32),
            pltpu.VMEM((3, 2, HALF, 128), f32),
            pltpu.VMEM((2, HALF, 128), f32),
            pltpu.VMEM((2, 2, HALF, 128), f32),
            pltpu.VMEM((FULL, 128), f32),
            pltpu.VMEM((128, FULL), f32),
            pltpu.VMEM((2, 3, 16, FULL), f32),
            pltpu.VMEM((WIDTH * ROWS, 128), f32),
            pltpu.VMEM((ROWS, 128), f32),
            pltpu.VMEM((ROWS, 128), f32),
            pltpu.VMEM((16, 128), bf16),
            pltpu.VMEM((count, 16, 128), bf16),
            pltpu.VMEM((128, 16 * count), f32),
            pltpu.VMEM((64, 32 * count), bf16),
            pltpu.VMEM((PACK, items // 2), f32),
            pltpu.VMEM((PACK, items // 2), f32),
            dma((4, 2)), dma((6,)), dma((6,)), dma((4, 2, 2)), dma((4, 2, 2)), dma((4, 2, 2)), dma((4, 2, 2)),
            dma((4, 2, 2)), dma((4, 2, 2)), dma((4, 2)),
            dma((2, 2)), dma((2, 2)), dma((2, 2, 2)), dma((2, 2, 2)), dma((2, 3)), dma((2, 3)),
            dma((count,)), dma((count,)), dma, dma, dma,
            pltpu.SemaphoreType.REGULAR, pltpu.SemaphoreType.REGULAR,
        ],
        compiler_params=pltpu.CompilerParams(
            collective_id=0, has_side_effects=True, vmem_limit_bytes=60 * 1024 * 1024
        ),
    )(ratings, mask, vt)


def solution(mesh):
    block_spec = P(("part", "row"), "col")
    in_specs = (block_spec, block_spec, P(("part", "col"), None))
    out_specs = (P(("part", "row", "col"), None), P(("part", "col", "row"), None))
    count = mesh.shape["col"]

    def local_als(ratings, mask, v_init):
        w_own, packed = half_steps(ratings, mask, v_init.T, count)
        v_own = solve_items(packed).T
        return w_own, v_own

    return jax.shard_map(local_als, mesh=mesh, in_specs=in_specs, out_specs=out_specs, check_vma=False)
```

```python
import jax
import jax.numpy as jnp
from jax import lax
from jax.experimental import pallas as pl
from jax.experimental.pallas import tpu as pltpu
from jax.sharding import PartitionSpec as P

RIDGE_WEIGHT = 0.05
WIDTH = 50
ROWS = 56
TRI = 1280
LANES = 128


def tri_off(j):
    return j * WIDTH - j * (j - 1) // 2


def outer_tile(vt, dst):
    lanes = vt.shape[1]
    for j in range(WIDTH):
        rows = WIDTH - j
        dst[tri_off(j):tri_off(j) + rows, :] = vt[j:WIDTH, :] * vt[j:j + 1, :]


def solve_tile(g_ref, rhs, fac, inv, sol):
    lanes = fac.shape[1]
    for pan in range(7):
        first = 8 * pan
        rows = ROWS - first
        count = min(8, WIDTH - first)
        ids = lax.broadcasted_iota(jnp.int32, (rows, lanes), 0)
        accs = []
        for c in range(count):
            j = first + c
            start = tri_off(j) - c
            if j < WIDTH - 1:
                raw = g_ref[start:start + rows, :]
            else:
                raw = jnp.broadcast_to(g_ref[tri_off(j):tri_off(j) + 1, :], (rows, lanes))
            col = jnp.where(ids < WIDTH - first, raw, 0.0)
            col = jnp.where(ids == c, col + RIDGE_WEIGHT, col)
            col = jnp.where(ids == WIDTH - first, rhs(j), col)
            accs.append(col)
        if pan:
            def body(k, accs):
                base = pl.multiple_of(k * ROWS, 8)
                left = fac[pl.ds(base + first, rows), :]
                return tuple(
                    acc - left * fac[pl.ds(base + first + c, 1), :] for c, acc in enumerate(accs)
                )
            accs = list(lax.fori_loop(0, first, body, tuple(accs), unroll=2))
        for c in range(count):
            j = first + c
            diag = accs[c][c:c + 1, :]
            root = lax.rsqrt(diag)
            root = root * (1.5 - 0.5 * (diag * root) * root)
            inv[j:j + 1, :] = root
            col = accs[c] * root
            fac[pl.ds(j * ROWS + first, rows), :] = col
            for later in range(c + 1, count):
                accs[later] = accs[later] - col * col[later:later + 1, :]
    sol[48:56, :] = jnp.zeros((8, lanes), jnp.float32)
    for pan in reversed(range(7)):
        first = 8 * pan
        count = min(8, WIDTH - first)
        left = []
        for c in range(count):
            j = first + c
            val = fac[j * ROWS + WIDTH:j * ROWS + WIDTH + 1, :]
            if pan < 6:
                dot = fac[j * ROWS + first + 8:j * ROWS + ROWS, :] * sol[first + 8:ROWS, :]
                val = val - jnp.sum(dot, axis=0, keepdims=True)
            left.append(val)
        for c in reversed(range(count)):
            j = first + c
            got = left[c] * inv[j:j + 1, :]
            sol[j:j + 1, :] = got
            for early in range(c):
                row = (first + early) * ROWS + j
                left[early] = left[early] - fac[row:row + 1, :] * got


def item_solve_kernel(g_ref, w_ref, out_ref, w_out, fac, inv, sol):
    w_out[...] = w_ref[...]
    solve_tile(g_ref, lambda j: g_ref[TRI + j:TRI + j + 1, :], fac, inv, sol)
    out_ref[...] = sol[:WIDTH, :]


def solve_items(packed, w_own):
    n = packed.shape[1]
    w_spec = pl.BlockSpec(w_own.shape, lambda i: (0, 0))
    return pl.pallas_call(
        item_solve_kernel,
        out_shape=(jax.ShapeDtypeStruct((WIDTH, n), jnp.float32), jax.ShapeDtypeStruct(w_own.shape, jnp.float32)),
        grid=(n // LANES,),
        in_specs=[pl.BlockSpec((packed.shape[0], LANES), lambda i: (0, i)), w_spec],
        out_specs=(pl.BlockSpec((WIDTH, LANES), lambda i: (0, i)), w_spec),
        scratch_shapes=[
            pltpu.VMEM((WIDTH * ROWS, LANES), jnp.float32),
            pltpu.VMEM((ROWS, LANES), jnp.float32),
            pltpu.VMEM((ROWS, LANES), jnp.float32),
        ],
    )(packed, w_own)


PACK = 1344
FULL = 1408
SIDE = 4
HALF = PACK // 2
CUT = 384


def dot_cols(left, right):
    return lax.dot_general(left, right, (((1,), (1,)), ((), ())), preferred_element_type=jnp.float32)


def als_kernel(
    rate_hbm, mask_hbm, v_hbm, w_hbm, item_hbm,
    rate, mask, v_raw, mqs, hop, rhs, vt_all, o_all, tmp, gram, unit, rel, got, tot, acc, flat, fin,
    fac, inv, sol, w_new, pack, w_all, wt, wb, part, swap_got, item_sum,
    v_sem, load_sem, v_send, v_recv, m_send, m_recv, hop_send, hop_recv, fwd_send, fwd_recv, own_sem,
    rel_send, rel_recv, got_send, got_recv, fin_send, fin_recv, w_send, w_recv, w_sem, x_send, x_recv, out_sem, y_in, z_in,
):
    items = v_raw.shape[1]
    count = w_all.shape[0]
    col = lax.axis_index("col")
    row = lax.axis_index("row")
    other = {"row": 1 - row}
    x = lax.rem(col, SIDE)
    y = lax.rem(col // SIDE, SIDE)
    z = col // (SIDE * SIDE)

    def turn(pos, step):
        return lax.rem(pos + step, SIDE)

    def x_peer(step):
        return {"col": col - x + turn(x, step)}

    def y_peer(step):
        return {"col": col + SIDE * (turn(y, step) - y)}

    def z_peer(step):
        return {"col": col + SIDE * SIDE * (turn(z, step) - z)}

    def send(src, dst, send_sem, recv_sem, peer):
        return pltpu.make_async_remote_copy(
            src_ref=src, dst_ref=dst, send_sem=send_sem, recv_sem=recv_sem,
            device_id=peer, device_id_type=pl.DeviceIdType.MESH,
        )

    def signal(sem, peer):
        pl.semaphore_signal(sem, inc=1, device_id=peer, device_id_type=pl.DeviceIdType.MESH)

    barrier = pltpu.get_barrier_semaphore()
    peers = [peer(step) for step in (1, 2, 3) for peer in (x_peer, y_peer, z_peer)] + [other]
    for peer in peers:
        signal(barrier, peer)

    owners = [turn(z, 2), turn(z, 1), turn(z, 3), z]
    block = rate.shape[1]
    v_load = pltpu.make_async_copy(v_hbm, v_raw, v_sem)
    loads = []
    for k, owner in enumerate(owners):
        rows = pl.ds(pl.multiple_of(owner * block, block), block)
        pair = [
            pltpu.make_async_copy(rate_hbm.at[rows], rate.at[k], load_sem.at[k, 0]),
            pltpu.make_async_copy(mask_hbm.at[rows], mask.at[k], load_sem.at[k, 1]),
        ]
        for copy in pair:
            copy.start()
        loads.append(pair)
        if k == 0:
            v_load.start()

    def cast_chunk(k):
        for copy in loads[k]:
            copy.wait()

        def cast_step(i, carry):
            rows = pl.ds(pl.multiple_of(i * 128, 128), 128)
            seen = mask[k, rows, :]
            mqs[k, i, :, :, 0] = seen.astype(jnp.float32).astype(jnp.bfloat16).reshape(SIDE, 2, 16, items)
            rated = jnp.where(seen != 0, rate[k, rows, :], 0.0)
            mqs[k, i, :, :, 1] = rated.astype(jnp.bfloat16).reshape(SIDE, 2, 16, items)
            return carry

        lax.fori_loop(0, SIDE, cast_step, 0)

    def axis_peer(c, step):
        return y_peer(step) if c else x_peer(step)

    def share(s, c, pos):
        return mqs.at[(0, 2, 1, 3)[s], pos, :, 1] if c else mqs.at[s, :, pos, 0]

    def columns(slot):
        return slice(slot * items, (slot + 1) * items)

    m_copies, hops, passes = [], [], []
    for s in range(4):
        m_copies.append([])
        hops.append([])
        passes.append([])
        for c, pos in enumerate((x, y)):
            for m, step in enumerate((1, 3)):
                hops[s].append(send(
                    share(s, c, turn(pos, 2)).at[:, m], hop.at[s, c, m],
                    hop_send.at[s, c, m], hop_recv.at[s, c, m], axis_peer(c, step),
                ))
                m_copies[s].append(send(
                    share(s, c, turn(pos, step)), rhs.at[s, c, :, :, :, columns(3 * c + step)],
                    m_send.at[s, c, m], m_recv.at[s, c, m], axis_peer(c, step),
                ))
                passes[s].append(send(
                    hop.at[s, c, m], rhs.at[s, c, :, m, :, columns(3 * c + 2)],
                    fwd_send.at[s, c, m], fwd_recv.at[s, c, m], axis_peer(c, step),
                ))
            m_copies[s].append(pltpu.make_async_copy(
                share(s, c, pos), rhs.at[s, c, :, :, :, columns(0)], own_sem.at[s, c]
            ))

    def start_stage(s):
        for copy in hops[s] + m_copies[s]:
            copy.start()

    def pass_on(s):
        for copy, follow in zip(hops[s], passes[s]):
            copy.wait()
            follow.start()

    tmp[48:64, :] = jnp.zeros((16, items), jnp.float32)
    cast_chunk(0)
    v_load.wait()
    tmp[0:WIDTH, :] = v_raw[...]
    vt_all[:, 0:items] = tmp[0:64, :].astype(jnp.bfloat16)
    pl.semaphore_wait(barrier, len(peers))
    start_stage(0)
    v_copies = []
    for d in (1, 3, 2):
        for axis in range(2):
            slot = 3 * axis + d
            v_copies.append(send(
                vt_all.at[:, columns(0)], vt_all.at[:, columns(slot)],
                v_send.at[slot - 1], v_recv.at[slot - 1], axis_peer(axis, d),
            ))
    for copy in v_copies:
        copy.start()
    for step in (1, 2, 3):
        signal(y_in, y_peer(step))
    for k in range(1, 4):
        cast_chunk(k)
    for s in range(4):
        rhs[s, 0, :, :, :, 4 * items:7 * items] = jnp.zeros((4, 2, 16, 3 * items), jnp.bfloat16)
        rhs[s, 1, :, :, :, items:4 * items] = jnp.zeros((4, 2, 16, 3 * items), jnp.bfloat16)
    tmp[1272:1280, :] = jnp.zeros((8, items), jnp.float32)

    def outer_step(slot, carry):
        cols = pl.ds(pl.multiple_of(slot * items, items), items)
        outer_tile(vt_all[:, cols].astype(jnp.float32), tmp)
        o_all[:, cols] = tmp[...].astype(jnp.bfloat16)
        return carry

    lax.fori_loop(0, 1, outer_step, 0)
    pass_on(0)
    start_stage(1)
    pl.semaphore_wait(y_in, 3)
    for step in (1, 2, 3):
        signal(z_in, z_peer(step))
    for copy in v_copies:
        copy.wait()
    lax.fori_loop(1, 7, outer_step, 0)

    def partial(s, dst):
        for copy in m_copies[s] + passes[s]:
            copy.wait()

        def rows_step(i, carry):
            rows = pl.ds(pl.multiple_of(i * 320, 320), 320)
            dst[rows, :] = dot_cols(o_all[rows, :], rhs[s, :, :, 0].reshape(128, 7 * items))
            return carry

        dst[TRI:PACK, :] = dot_cols(vt_all[...], rhs[s, :, :, 1].reshape(128, 7 * items))
        lax.fori_loop(0, 4, rows_step, 0)

    low = lax.broadcasted_iota(jnp.int32, (HALF, 128), 1) < 64

    def pack_units(s):
        top, bottom = gram[0:HALF, :], gram[HALF:PACK, :]
        unit[s, 0] = jnp.where(low, top, pltpu.roll(bottom, 64, 1))
        unit[s, 1] = jnp.where(low, pltpu.roll(top, 64, 1), bottom)

    pieces = (slice(0, CUT), slice(CUT, HALF))
    ways = (1, 3)
    partial(0, gram)
    pack_units(0)
    relays = [[
        send(unit.at[0, c, rows], rel.at[c, rows], rel_send.at[c, p], rel_recv.at[c, p], z_peer(ways[c]))
        for c in range(2)
    ] for p, rows in enumerate(pieces)]
    for piece in relays:
        for copy in piece:
            copy.start()
    pass_on(1)
    start_stage(2)
    partial(1, gram)
    pack_units(1)
    z_copies = []
    pass_on(2)
    start_stage(3)
    for p, rows in enumerate(pieces):
        for c in range(2):
            relays[p][c].wait()
            unit[1, c, rows, :] = unit[1, c, rows, :] + rel[c, rows, :]
            copy = send(
                unit.at[1, c, rows], got.at[0, c, rows], got_send.at[0, c, p], got_recv.at[0, c, p], z_peer(ways[c])
            )
            copy.start()
            z_copies.append(copy)
    pass_on(3)
    partial(2, gram)
    pack_units(2)
    last = [[
        send(unit.at[2, c, rows], got.at[1, c, rows], got_send.at[1, c, p], got_recv.at[1, c, p], z_peer(ways[1 - c]))
        for c in range(2)
    ] for p, rows in enumerate(pieces)]
    for piece in last:
        for copy in piece:
            copy.start()
    partial(3, tot)
    acc[PACK:FULL, :] = jnp.zeros((FULL - PACK, 128), jnp.float32)
    for copy in z_copies:
        copy.wait()
    pl.semaphore_wait(z_in, 3)
    f_copies = []
    for p, rows in enumerate(pieces):
        size = rows.stop - rows.start
        for copy in last[p]:
            copy.wait()
        sum_a = got[0, 0, rows] + got[1, 0, rows]
        sum_b = got[0, 1, rows] + got[1, 1, rows]
        here = low[:size]
        at = 2 * rows.start
        acc[at:at + size, :] = tot[rows, :] + jnp.where(here, sum_a, pltpu.roll(sum_b, 64, 1))
        acc[at + size:at + 2 * size, :] = (
            tot[HALF + rows.start:HALF + rows.stop, :] + jnp.where(here, pltpu.roll(sum_a, 64, 1), sum_b)
        )
        cols = slice(at, FULL if p else 2 * CUT)
        for i in range(cols.start // 128, cols.stop // 128):
            flat[:, i * 128:(i + 1) * 128] = acc[i * 128:(i + 1) * 128, :].T
        for d in (2, 1, 3):
            for c, pos in enumerate((y, x)):
                users = pl.ds(pl.multiple_of(64 * c + 16 * turn(pos, d), 16), 16)
                copy = send(
                    flat.at[users, cols], fin.at[c, d - 1, :, cols],
                    fin_send.at[p, c, d - 1], fin_recv.at[p, c, d - 1], axis_peer(1 - c, d),
                )
                copy.start()
                f_copies.append(copy)
    for copy in f_copies:
        copy.wait()

    zeros = jnp.zeros((96, 128), jnp.float32)
    for i in range(FULL // 128):
        cols = slice(i * 128, (i + 1) * 128)
        mine = [zeros]
        for c, pos in ((1, x), (0, y)):
            rows = pl.ds(pl.multiple_of(64 * c + 16 * pos, 16), 16)
            mine.insert(0, flat[rows, cols] + fin[c, 0, :, cols] + fin[c, 1, :, cols] + fin[c, 2, :, cols])
        acc[cols, :] = jnp.concatenate(mine, axis=0).T
    for rows in pieces:
        size = rows.stop - rows.start
        tot[rows, :] = acc[2 * rows.start:2 * rows.start + size, :]
        tot[HALF + rows.start:HALF + rows.stop, :] = acc[2 * rows.start + size:2 * rows.stop, :]
    solve_tile(tot, lambda j: tot[TRI + j:TRI + j + 1, :], fac, inv, sol)
    turned = jnp.concatenate([sol[...], jnp.zeros((72, 128), jnp.float32)], axis=0).T
    lane = lax.broadcasted_iota(jnp.int32, (16, 128), 1)
    pack[...] = jnp.where(lane < 64, turned[:16], pltpu.roll(turned[16:32], 64, 1)).astype(jnp.bfloat16)

    def w_copy(d):
        return send(pack, w_all.at[col], w_send.at[d], w_recv.at[d], {"col": lax.rem(col + d, count)})

    def send_step(i, carry):
        w_copy(1 + lax.rem(i + count // 2 - 1, count - 1)).start()
        return carry

    w_own = pltpu.make_async_copy(pack, w_all.at[col], w_recv.at[0])
    w_own.start()
    lax.fori_loop(0, count - 1, send_step, 0)
    w_new[...] = turned[:32, :WIDTH]
    w_out = pltpu.make_async_copy(w_new, w_hbm, w_sem)
    w_out.start()

    plane = SIDE * SIDE
    users = 16 * count
    step = 16 * plane
    tall = tmp.at[:, 0:step]
    tall[1272:1280, :] = jnp.zeros((8, step), jnp.float32)

    def plane_step(t, carry):
        k = 3 - 2 * t + 3 * (t // 2)
        owner = turn(z, t + (t // 2) * (5 - 2 * t))

        def arrive_step(i, carry):
            source = owner * plane + i
            pltpu.make_async_copy(pack, w_all.at[source], w_recv.at[lax.rem(col - source + count, count)]).wait()
            return carry

        lax.fori_loop(0, plane, arrive_step, 0)
        for i in range(step // 128):
            rows = w_all[pl.ds(owner * plane + 8 * i, 8)].reshape(128, 128)
            wt[:, i * 128:(i + 1) * 128] = rows.astype(jnp.float32).T

        def colour_step(c, carry):
            vals = wt[pl.ds(pl.multiple_of(64 * c, 64), 64), :]
            cols = pl.ds(pl.multiple_of(c * users + k * step, step), step)
            wb[:, cols] = vals.astype(jnp.bfloat16)
            outer_tile(vals, tall)
            o_all[:, cols] = tall[...].astype(jnp.bfloat16)
            return carry

        lax.fori_loop(0, 2, colour_step, 0)
        return carry

    lax.fori_loop(0, SIDE, plane_step, 0)
    half = items // 2

    def item_rows(side, left, m):
        cols = pl.ds(pl.multiple_of(side * half, half), half)
        total = None
        for c in range(2):
            right = mqs[:, :, :, c, m, :, cols].reshape(users, half)
            term = jnp.dot(left(c), right, preferred_element_type=jnp.float32)
            total = term if total is None else total + term
        return total

    def rhs_rows(side):
        return item_rows(side, lambda c: wb[:, c * users:(c + 1) * users], 1)

    def gram_rows(side, rows):
        return item_rows(side, lambda c: o_all[rows, c * users:(c + 1) * users], 0)

    def swap_copy(i, rows):
        return send(part.at[rows], swap_got.at[rows], x_send.at[i], x_recv.at[i], other)

    def finish(i, rows, val):
        swap_copy(i, rows).wait()
        item_sum[rows, :] = val + swap_got[rows, :]
        pltpu.make_async_copy(item_sum.at[rows], item_hbm.at[rows], out_sem.at[i]).start()

    tail = pl.ds(TRI, PACK - TRI)
    part[tail, :] = rhs_rows(1 - row)
    swap_copy(4, tail).start()

    def away_step(i, carry):
        rows = pl.ds(pl.multiple_of(i * 320, 320), 320)
        part[rows, :] = gram_rows(1 - row, rows)
        swap_copy(i, rows).start()
        return carry

    def home_step(i, carry):
        rows = pl.ds(pl.multiple_of(i * 320, 320), 320)
        finish(i, rows, gram_rows(row, rows))
        return carry

    lax.fori_loop(0, 4, away_step, 0)
    finish(4, tail, rhs_rows(row))
    lax.fori_loop(0, 4, home_step, 0)
    w_out.wait()
    for i in range(4):
        rows = pl.ds(i * 320, 320)
        pltpu.make_async_copy(item_sum.at[rows], item_hbm.at[rows], out_sem.at[i]).wait()
    pltpu.make_async_copy(item_sum.at[tail], item_hbm.at[tail], out_sem.at[4]).wait()

    def sent_step(d, carry):
        w_copy(d).wait_send()
        return carry

    lax.fori_loop(1, count, sent_step, 0)


def half_steps(ratings, mask, vt, count):
    users, items = ratings.shape
    block = users // SIDE
    dma = pltpu.SemaphoreType.DMA
    any_spec = pl.BlockSpec(memory_space=pl.ANY)
    f32, bf16 = jnp.float32, jnp.bfloat16
    return pl.pallas_call(
        als_kernel,
        out_shape=(
            jax.ShapeDtypeStruct((32, WIDTH), f32),
            jax.ShapeDtypeStruct((PACK, items // 2), f32),
        ),
        in_specs=[any_spec, any_spec, any_spec],
        out_specs=(any_spec, any_spec),
        scratch_shapes=[
            pltpu.VMEM((4, block, items), f32),
            pltpu.VMEM((4, block, items), jnp.int32),
            pltpu.VMEM((WIDTH, items), f32),
            pltpu.VMEM((4, SIDE, SIDE, 2, 2, 16, items), bf16),
            pltpu.VMEM((4, 2, 2, SIDE, 16, items), bf16),
            pltpu.VMEM((4, 2, SIDE, 2, 16, 7 * items), bf16),
            pltpu.VMEM((64, 7 * items), bf16),
            pltpu.VMEM((TRI, 7 * items), bf16),
            pltpu.VMEM((TRI, items), f32),
            pltpu.VMEM((PACK, 128), f32),
            pltpu.VMEM((3, 2, HALF, 128), f32),
            pltpu.VMEM((2, HALF, 128), f32),
            pltpu.VMEM((2, 2, HALF, 128), f32),
            pltpu.VMEM((PACK, 128), f32),
            pltpu.VMEM((FULL, 128), f32),
            pltpu.VMEM((128, FULL), f32),
            pltpu.VMEM((2, 3, 16, FULL), f32),
            pltpu.VMEM((WIDTH * ROWS, 128), f32),
            pltpu.VMEM((ROWS, 128), f32),
            pltpu.VMEM((ROWS, 128), f32),
            pltpu.VMEM((32, WIDTH), f32),
            pltpu.VMEM((16, 128), bf16),
            pltpu.VMEM((count, 16, 128), bf16),
            pltpu.VMEM((128, 16 * SIDE * SIDE), f32),
            pltpu.VMEM((64, 32 * count), bf16),
            pltpu.VMEM((PACK, items // 2), f32),
            pltpu.VMEM((PACK, items // 2), f32),
            pltpu.VMEM((PACK, items // 2), f32),
            dma, dma((4, 2)), dma((6,)), dma((6,)), dma((4, 2, 2)), dma((4, 2, 2)), dma((4, 2, 2)), dma((4, 2, 2)),
            dma((4, 2, 2)), dma((4, 2, 2)), dma((4, 2)),
            dma((2, 2)), dma((2, 2)), dma((2, 2, 2)), dma((2, 2, 2)), dma((2, 2, 3)), dma((2, 2, 3)),
            dma((count,)), dma((count,)), dma, dma((5,)), dma((5,)), dma((5,)),
            pltpu.SemaphoreType.REGULAR, pltpu.SemaphoreType.REGULAR,
        ],
        compiler_params=pltpu.CompilerParams(
            collective_id=0, has_side_effects=True, vmem_limit_bytes=60 * 1024 * 1024
        ),
    )(ratings, mask, vt)


def solution(mesh):
    block_spec = P(("part", "row"), "col")
    in_specs = (block_spec, block_spec, P(("part", "col"), None))
    out_specs = (P(("part", "row", "col"), None), P(("part", "col", "row"), None))
    count = mesh.shape["col"]

    def local_als(ratings, mask, v_init):
        w_own, packed = half_steps(ratings, mask, v_init.T, count)
        v_own, w_own = solve_items(packed, w_own)
        return w_own, v_own.T

    return jax.shard_map(local_als, mesh=mesh, in_specs=in_specs, out_specs=out_specs, check_vma=False)
```

```python
import jax
import jax.numpy as jnp
from jax import lax
from jax.experimental import pallas as pl
from jax.experimental.pallas import tpu as pltpu
from jax.sharding import PartitionSpec as P

RIDGE_WEIGHT = 0.05
WIDTH = 50
ROWS = 56
TRI = 1280
LANES = 128


def tri_off(j):
    return j * WIDTH - j * (j - 1) // 2


def outer_tile(vt, dst):
    lanes = vt.shape[1]
    for j in range(WIDTH):
        rows = WIDTH - j
        dst[tri_off(j):tri_off(j) + rows, :] = vt[j:WIDTH, :] * vt[j:j + 1, :]


def solve_tile(g_ref, rhs, fac, inv, sol):
    lanes = fac.shape[1]
    for pan in range(7):
        first = 8 * pan
        rows = ROWS - first
        count = min(8, WIDTH - first)
        ids = lax.broadcasted_iota(jnp.int32, (rows, lanes), 0)
        accs = []
        for c in range(count):
            j = first + c
            start = tri_off(j) - c
            if j < WIDTH - 1:
                raw = g_ref[start:start + rows, :]
            else:
                raw = jnp.broadcast_to(g_ref[tri_off(j):tri_off(j) + 1, :], (rows, lanes))
            col = jnp.where(ids < WIDTH - first, raw, 0.0)
            col = jnp.where(ids == c, col + RIDGE_WEIGHT, col)
            col = jnp.where(ids == WIDTH - first, rhs(j), col)
            accs.append(col)
        if pan:
            def body(k, accs):
                base = pl.multiple_of(k * ROWS, 8)
                left = fac[pl.ds(base + first, rows), :]
                return tuple(
                    acc - left * fac[pl.ds(base + first + c, 1), :] for c, acc in enumerate(accs)
                )
            accs = list(lax.fori_loop(0, first, body, tuple(accs), unroll=2))
        for c in range(count):
            j = first + c
            diag = accs[c][c:c + 1, :]
            root = lax.rsqrt(diag)
            root = root * (1.5 - 0.5 * (diag * root) * root)
            inv[j:j + 1, :] = root
            col = accs[c] * root
            fac[pl.ds(j * ROWS + first, rows), :] = col
            for later in range(c + 1, count):
                accs[later] = accs[later] - col * col[later:later + 1, :]
    sol[48:56, :] = jnp.zeros((8, lanes), jnp.float32)
    for pan in reversed(range(7)):
        first = 8 * pan
        count = min(8, WIDTH - first)
        left = []
        for c in range(count):
            j = first + c
            val = fac[j * ROWS + WIDTH:j * ROWS + WIDTH + 1, :]
            if pan < 6:
                dot = fac[j * ROWS + first + 8:j * ROWS + ROWS, :] * sol[first + 8:ROWS, :]
                val = val - jnp.sum(dot, axis=0, keepdims=True)
            left.append(val)
        for c in reversed(range(count)):
            j = first + c
            got = left[c] * inv[j:j + 1, :]
            sol[j:j + 1, :] = got
            for early in range(c):
                row = (first + early) * ROWS + j
                left[early] = left[early] - fac[row:row + 1, :] * got


def item_solve_kernel(g_ref, w_ref, out_ref, w_out, fac, inv, sol):
    w_out[...] = w_ref[...]
    solve_tile(g_ref, lambda j: g_ref[TRI + j:TRI + j + 1, :], fac, inv, sol)
    out_ref[...] = sol[:WIDTH, :]


def solve_items(packed, w_own):
    n = packed.shape[1]
    w_spec = pl.BlockSpec(w_own.shape, lambda i: (0, 0))
    return pl.pallas_call(
        item_solve_kernel,
        out_shape=(jax.ShapeDtypeStruct((WIDTH, n), jnp.float32), jax.ShapeDtypeStruct(w_own.shape, jnp.float32)),
        grid=(n // LANES,),
        in_specs=[pl.BlockSpec((packed.shape[0], LANES), lambda i: (0, i)), w_spec],
        out_specs=(pl.BlockSpec((WIDTH, LANES), lambda i: (0, i)), w_spec),
        scratch_shapes=[
            pltpu.VMEM((WIDTH * ROWS, LANES), jnp.float32),
            pltpu.VMEM((ROWS, LANES), jnp.float32),
            pltpu.VMEM((ROWS, LANES), jnp.float32),
        ],
    )(packed, w_own)


PACK = 1344
FULL = 1408
SIDE = 4
HALF = PACK // 2
CUT = 384


def dot_cols(left, right):
    return lax.dot_general(left, right, (((1,), (1,)), ((), ())), preferred_element_type=jnp.float32)


def als_kernel(
    rate_hbm, mask_hbm, v_hbm, w_hbm, item_hbm,
    rate, mask, v_raw, mqs, hop, rhs, vt_all, o_all, tmp, gram, home, unit, rel, got, tot, acc, flat, fin,
    fac, inv, sol, w_new, pack, w_all, wt, wb, part, swap_got, item_sum,
    v_sem, load_sem, v_send, v_recv, m_send, m_recv, hop_send, hop_recv, fwd_send, own_sem,
    rel_send, rel_recv, got_send, got_recv, fin_send, fin_recv, w_send, w_recv, w_sem, x_send, x_recv, out_sem, y_in, z_in,
):
    items = v_raw.shape[1]
    count = w_all.shape[0]
    col = lax.axis_index("col")
    row = lax.axis_index("row")
    other = {"row": 1 - row}
    x = lax.rem(col, SIDE)
    y = lax.rem(col // SIDE, SIDE)
    z = col // (SIDE * SIDE)

    def turn(pos, step):
        return lax.rem(pos + step, SIDE)

    def x_peer(step):
        return {"col": col - x + turn(x, step)}

    def y_peer(step):
        return {"col": col + SIDE * (turn(y, step) - y)}

    def z_peer(step):
        return {"col": col + SIDE * SIDE * (turn(z, step) - z)}

    def send(src, dst, send_sem, recv_sem, peer):
        return pltpu.make_async_remote_copy(
            src_ref=src, dst_ref=dst, send_sem=send_sem, recv_sem=recv_sem,
            device_id=peer, device_id_type=pl.DeviceIdType.MESH,
        )

    def signal(sem, peer):
        pl.semaphore_signal(sem, inc=1, device_id=peer, device_id_type=pl.DeviceIdType.MESH)

    def start(copies):
        for copy in copies:
            copy.start()

    def take(ref, sem):
        pltpu.make_async_copy(ref, ref, sem).wait()

    barrier = pltpu.get_barrier_semaphore()
    peers = [peer(step) for step in (1, 2, 3) for peer in (x_peer, y_peer, z_peer)] + [other]
    for peer in peers:
        signal(barrier, peer)

    owners = [turn(z, 2), turn(z, 1), turn(z, 3), z]
    block = rate.shape[1]
    v_load = pltpu.make_async_copy(v_hbm, v_raw, v_sem)
    v_load.start()
    loads = []
    for k, owner in enumerate(owners):
        rows = pl.ds(pl.multiple_of(owner * block, block), block)
        pair = [
            pltpu.make_async_copy(rate_hbm.at[rows], rate.at[k], load_sem.at[k]),
            pltpu.make_async_copy(mask_hbm.at[rows], mask.at[k], load_sem.at[k]),
        ]
        loads.append(pair)
    start(loads[0])

    def cast_chunk(k):
        def cast_step(i, carry):
            rows = pl.ds(pl.multiple_of(i * 128, 128), 128)
            seen = mask[k, rows, :]
            mqs[k, i, :, :, 0] = seen.astype(jnp.float32).astype(jnp.bfloat16).reshape(SIDE, 2, 16, items)
            rated = jnp.where(seen != 0, rate[k, rows, :], 0.0)
            mqs[k, i, :, :, 1] = rated.astype(jnp.bfloat16).reshape(SIDE, 2, 16, items)
            return carry

        with jax.named_scope("p00__0__cast_step_0"):
            lax.fori_loop(0, SIDE, cast_step, 0)

    def axis_peer(c, step):
        return y_peer(step) if c else x_peer(step)

    def share(s, c, pos):
        return mqs.at[(0, 2, 1, 3)[s], pos, :, 1] if c else mqs.at[s, :, pos, 0]

    def columns(slot):
        return slice(slot * items, (slot + 1) * items)

    m_copies, own_copies, hops, passes = [], [], [], []
    for s in range(4):
        m_copies.append([])
        own_copies.append([])
        hops.append([])
        passes.append([])
        for c, pos in enumerate((x, y)):
            for m, step in enumerate((1, 3)):
                hops[s].append(send(
                    share(s, c, turn(pos, 2)).at[:, m], hop.at[s, c, m],
                    hop_send, hop_recv.at[s], axis_peer(c, step),
                ))
                m_copies[s].append(send(
                    share(s, c, turn(pos, step)), rhs.at[s, c, :, :, :, columns(3 * c + step)],
                    m_send, m_recv.at[s], axis_peer(c, step),
                ))
                passes[s].append(send(
                    hop.at[s, c, m], rhs.at[s, c, :, m, :, columns(3 * c + 2)],
                    fwd_send, m_recv.at[s], axis_peer(c, step),
                ))
            own_copies[s].append(pltpu.make_async_copy(
                share(s, c, pos), rhs.at[s, c, :, :, :, columns(0)], own_sem.at[s]
            ))

    def pass_on(s):
        with jax.named_scope("p01_take_hopats_hop_recvats"):
            take(hop.at[s], hop_recv.at[s])
        start(passes[s])

    def half_columns(slot, side):
        return pl.ds(pl.multiple_of(slot * items + side * (items // 2), items // 2), items // 2)

    v_copies, v_swaps = [], []
    for d in (1, 3, 2):
        for axis in range(2):
            slot = 3 * axis + d
            v_copies.append(send(
                vt_all.at[:, half_columns(0, row)], vt_all.at[:, half_columns(slot, row)],
                v_send.at[0], v_recv.at[d], axis_peer(axis, d),
            ))
            v_swaps.append(send(
                vt_all.at[:, half_columns(slot, row)], vt_all.at[:, half_columns(slot, row)],
                v_send.at[1], v_recv.at[0], other,
            ))

    tmp[48:64, :] = jnp.zeros((16, items), jnp.float32)
    v_load.wait()
    tmp[0:WIDTH, :] = v_raw[...]
    vt_all[:, 0:items] = tmp[0:64, :].astype(jnp.bfloat16)
    with jax.named_scope("p02_take_rateat02_load_semat0"):
        take(rate.at[0:2], load_sem.at[0])
    for k in range(1, 4):
        start(loads[k])
    with jax.named_scope("p03_cast_chunk_0"):
        cast_chunk(0)
    with jax.named_scope("p04_plsemaphore_wait_barrier_len_p"):
        pl.semaphore_wait(barrier, len(peers))
    start(v_copies)
    start(hops[0])
    start(m_copies[0])
    for step in (1, 2, 3):
        signal(y_in, y_peer(step))
    for k in range(1, 4):
        with jax.named_scope("p05_take_rateat02_load_sematk"):
            take(rate.at[0:2], load_sem.at[k])
        with jax.named_scope("p06_cast_chunk_k"):
            cast_chunk(k)
    for s in range(4):
        start(own_copies[s])
    for s in range(4):
        rhs[s, 0, :, :, :, 4 * items:7 * items] = jnp.zeros((4, 2, 16, 3 * items), jnp.bfloat16)
        rhs[s, 1, :, :, :, items:4 * items] = jnp.zeros((4, 2, 16, 3 * items), jnp.bfloat16)
    tmp[1272:1280, :] = jnp.zeros((8, items), jnp.float32)

    def outer_step(slot, carry):
        cols = pl.ds(pl.multiple_of(slot * items, items), items)
        outer_tile(vt_all[:, cols].astype(jnp.float32), tmp)
        o_all[:, cols] = tmp[...].astype(jnp.bfloat16)
        return carry

    with jax.named_scope("p07__0_1_outer_step_0"):
        lax.fori_loop(0, 1, outer_step, 0)
    for i, d in enumerate((1, 3, 2)):
        with jax.named_scope("p08_take_vt_allat_0items_v_recvatd"):
            take(vt_all.at[:, 0:items], v_recv.at[d])
        start(v_swaps[2 * i:2 * i + 2])
    with jax.named_scope("p09_pass_on_0"):
        pass_on(0)
    start(hops[1])
    start(m_copies[1])
    start(hops[2])
    with jax.named_scope("p10_plsemaphore_wait_y_in_3"):
        pl.semaphore_wait(y_in, 3)
    for step in (1, 2, 3):
        signal(z_in, z_peer(step))

    def users_of(s, m, cols):
        return rhs[s, :, :, m, :, cols].reshape(128, cols.stop - cols.start)

    near, far = slice(0, items), slice(items, 7 * items)
    def own_part(s):
        with jax.named_scope("p11_take_hopats_own_semats"):
            take(hop.at[s], own_sem.at[s])

        def near_step(i, carry):
            rows = pl.ds(pl.multiple_of(i * 640, 640), 640)
            home[s, rows, :] = dot_cols(o_all[rows, near], users_of(s, 0, near))
            return carry

        home[s, TRI:PACK, :] = dot_cols(vt_all[:, near], users_of(s, 1, near))
        with jax.named_scope("p12__0_2_near_step_0"):
            lax.fori_loop(0, 2, near_step, 0)
    with jax.named_scope("p13_own_part_0"):
        own_part(0)
    with jax.named_scope("p14_take_vt_allat_03items_v_recvat"):
        take(vt_all.at[:, 0:3 * items], v_recv.at[0])
    with jax.named_scope("p15__1_7_outer_step_0"):
        lax.fori_loop(1, 7, outer_step, 0)

    def partial(s, dst):
        with jax.named_scope("p16_take_mqsat0_03_m_recvats"):
            take(mqs.at[0, 0:3], m_recv.at[s])

        def rows_step(i, carry):
            rows = pl.ds(pl.multiple_of(i * 640, 640), 640)
            dst[rows, :] = home[s, rows, :] + dot_cols(o_all[rows, far], users_of(s, 0, far))
            return carry

        dst[TRI:PACK, :] = home[s, TRI:PACK, :] + dot_cols(vt_all[:, far], users_of(s, 1, far))
        with jax.named_scope("p17__0_2_rows_step_0"):
            lax.fori_loop(0, 2, rows_step, 0)

    low = lax.broadcasted_iota(jnp.int32, (HALF, 128), 1) < 64

    def pack_units(s):
        top, bottom = gram[0:HALF, :], gram[HALF:PACK, :]
        unit[s, 0] = jnp.where(low, top, pltpu.roll(bottom, 64, 1))
        unit[s, 1] = jnp.where(low, pltpu.roll(top, 64, 1), bottom)

    pieces = (slice(0, CUT), slice(CUT, HALF))
    ways = (1, 3)
    with jax.named_scope("p18_partial_0_gram"):
        partial(0, gram)
    with jax.named_scope("p19_pack_units_0"):
        pack_units(0)
    relays = [[
        send(unit.at[0, c, rows], rel.at[c, rows], rel_send, rel_recv.at[p], z_peer(ways[c]))
        for c in range(2)
    ] for p, rows in enumerate(pieces)]
    for piece in relays:
        for copy in piece:
            copy.start()
    with jax.named_scope("p20_pass_on_1"):
        pass_on(1)
    start(m_copies[2])
    start(hops[3])
    with jax.named_scope("p21_own_part_1"):
        own_part(1)
    with jax.named_scope("p22_pass_on_2"):
        pass_on(2)
    start(m_copies[3])
    with jax.named_scope("p23_own_part_2"):
        own_part(2)
    with jax.named_scope("p24_partial_1_gram"):
        partial(1, gram)
    with jax.named_scope("p25_pack_units_1"):
        pack_units(1)
    for p, rows in enumerate(pieces):
        with jax.named_scope("p26_take_relat_rows_rel_recvatp"):
            take(rel.at[:, rows], rel_recv.at[p])
        for c in range(2):
            unit[1, c, rows, :] = unit[1, c, rows, :] + rel[c, rows, :]
            send(unit.at[1, c, rows], got.at[0, c, rows], got_send, got_recv.at[0], z_peer(ways[c])).start()
    with jax.named_scope("p27_pass_on_3"):
        pass_on(3)
    with jax.named_scope("p28_partial_2_gram"):
        partial(2, gram)
    with jax.named_scope("p29_pack_units_2"):
        pack_units(2)
    last = [[
        send(unit.at[2, c, rows], got.at[1, c, rows], got_send, got_recv.at[1 + p], z_peer(ways[1 - c]))
        for c in range(2)
    ] for p, rows in enumerate(pieces)]
    for piece in last:
        for copy in piece:
            copy.start()
    with jax.named_scope("p30_own_part_3"):
        own_part(3)
    with jax.named_scope("p31_partial_3_tot"):
        partial(3, tot)
    acc[PACK:FULL, :] = jnp.zeros((FULL - PACK, 128), jnp.float32)
    with jax.named_scope("p32_take_gotat0_got_recvat0"):
        take(got.at[0], got_recv.at[0])
    with jax.named_scope("p33_plsemaphore_wait_z_in_3"):
        pl.semaphore_wait(z_in, 3)
    for p, rows in enumerate(pieces):
        size = rows.stop - rows.start
        with jax.named_scope("p34_take_gotat1__rows_got_recvat1p"):
            take(got.at[1, :, rows], got_recv.at[1 + p])
        sum_a = got[0, 0, rows] + got[1, 0, rows]
        sum_b = got[0, 1, rows] + got[1, 1, rows]
        here = low[:size]
        at = 2 * rows.start
        acc[at:at + size, :] = tot[rows, :] + jnp.where(here, sum_a, pltpu.roll(sum_b, 64, 1))
        acc[at + size:at + 2 * size, :] = (
            tot[HALF + rows.start:HALF + rows.stop, :] + jnp.where(here, pltpu.roll(sum_a, 64, 1), sum_b)
        )
        cols = slice(at, FULL if p else 2 * CUT)
        for i in range(cols.start // 128, cols.stop // 128):
            flat[:, i * 128:(i + 1) * 128] = acc[i * 128:(i + 1) * 128, :].T
        for d in (2, 1, 3):
            for c, pos in enumerate((y, x)):
                users = pl.ds(pl.multiple_of(64 * c + 16 * turn(pos, d), 16), 16)
                send(
                    flat.at[users, cols], fin.at[c, d - 1, :, cols], fin_send, fin_recv, axis_peer(1 - c, d)
                ).start()
    with jax.named_scope("p35_take_fin_fin_recv"):
        take(fin, fin_recv)

    zeros = jnp.zeros((96, 128), jnp.float32)
    for i in range(FULL // 128):
        cols = slice(i * 128, (i + 1) * 128)
        mine = [zeros]
        for c, pos in ((1, x), (0, y)):
            rows = pl.ds(pl.multiple_of(64 * c + 16 * pos, 16), 16)
            mine.insert(0, flat[rows, cols] + fin[c, 0, :, cols] + fin[c, 1, :, cols] + fin[c, 2, :, cols])
        acc[cols, :] = jnp.concatenate(mine, axis=0).T
    for rows in pieces:
        size = rows.stop - rows.start
        tot[rows, :] = acc[2 * rows.start:2 * rows.start + size, :]
        tot[HALF + rows.start:HALF + rows.stop, :] = acc[2 * rows.start + size:2 * rows.stop, :]
    with jax.named_scope("p36_solve_tile_tot_lambdajtotjj1__"):
        solve_tile(tot, lambda j: tot[TRI + j:TRI + j + 1, :], fac, inv, sol)
    turned = jnp.concatenate([sol[...], jnp.zeros((72, 128), jnp.float32)], axis=0).T
    lane = lax.broadcasted_iota(jnp.int32, (16, 128), 1)
    pack[...] = jnp.where(lane < 64, turned[:16], pltpu.roll(turned[16:32], 64, 1)).astype(jnp.bfloat16)

    plane = SIDE * SIDE

    place = col - z * plane
    w_own = pltpu.make_async_copy(pack, w_all.at[col], w_recv.at[0])
    w_own.start()
    for t, turned_by in enumerate((0, 1, 3, 2)):
        base = turn(z, turned_by) * plane

        def send_step(i, carry):
            target = place + i
            target = base + jnp.where(target < plane, target, target - plane)
            send(pack, w_all.at[col], w_send, w_recv.at[(0, 2, 1, 3)[t]], {"col": target}).start()
            return carry

        with jax.named_scope("p37__0iftelse1_plane_send_step_0"):
            lax.fori_loop(0 if t else 1, plane, send_step, 0)
    w_new[...] = turned[:32, :WIDTH]
    w_out = pltpu.make_async_copy(w_new, w_hbm, w_sem)
    w_out.start()

    users = 16 * count
    step = 16 * plane
    tall = tmp.at[:, 0:step]
    tall[1272:1280, :] = jnp.zeros((8, step), jnp.float32)

    def plane_step(t, carry):
        k = 3 - 2 * t + 3 * (t // 2)
        owner = turn(z, t + (t // 2) * (5 - 2 * t))

        with jax.named_scope("p38_take_w_allat0plane_w_recvatt"):
            take(w_all.at[0:plane], w_recv.at[t])
        for i in range(step // 128):
            rows = w_all[pl.ds(owner * plane + 8 * i, 8)].reshape(128, 128)
            wt[:, i * 128:(i + 1) * 128] = rows.astype(jnp.float32).T

        def colour_step(c, carry):
            vals = wt[pl.ds(pl.multiple_of(64 * c, 64), 64), :]
            cols = pl.ds(pl.multiple_of(c * users + k * step, step), step)
            wb[:, cols] = vals.astype(jnp.bfloat16)
            outer_tile(vals, tall)
            o_all[:, cols] = tall[...].astype(jnp.bfloat16)
            return carry

        with jax.named_scope("p39__0_2_colour_step_0"):
            lax.fori_loop(0, 2, colour_step, 0)
        return carry

    with jax.named_scope("p40__0__plane_step_0"):
        lax.fori_loop(0, SIDE, plane_step, 0)
    half = items // 2

    def item_rows(side, left, m):
        cols = pl.ds(pl.multiple_of(side * half, half), half)
        total = None
        for c in range(2):
            right = mqs[:, :, :, c, m, :, cols].reshape(users, half)
            term = jnp.dot(left(c), right, preferred_element_type=jnp.float32)
            total = term if total is None else total + term
        return total

    def rhs_rows(side):
        return item_rows(side, lambda c: wb[:, c * users:(c + 1) * users], 1)

    def gram_rows(side, rows):
        return item_rows(side, lambda c: o_all[rows, c * users:(c + 1) * users], 0)

    def swap_copy(i, rows):
        return send(part.at[rows], swap_got.at[rows], x_send, x_recv.at[i], other)

    def finish(i, rows, val):
        with jax.named_scope("p41_swap_copy_i_rowswait_recv_"):
            swap_copy(i, rows).wait_recv()
        item_sum[rows, :] = val + swap_got[rows, :]
        pltpu.make_async_copy(item_sum.at[rows], item_hbm.at[rows], out_sem).start()

    tail = pl.ds(TRI, PACK - TRI)
    part[tail, :] = rhs_rows(1 - row)
    swap_copy(4, tail).start()

    def away_step(i, carry):
        rows = pl.ds(pl.multiple_of(i * 320, 320), 320)
        part[rows, :] = gram_rows(1 - row, rows)
        swap_copy(i, rows).start()
        return carry

    def home_step(i, carry):
        rows = pl.ds(pl.multiple_of(i * 320, 320), 320)
        finish(i, rows, gram_rows(row, rows))
        return carry

    with jax.named_scope("p42__0_4_away_step_0"):
        lax.fori_loop(0, 4, away_step, 0)
    finish(4, tail, rhs_rows(row))
    with jax.named_scope("p43__0_4_home_step_0"):
        lax.fori_loop(0, 4, home_step, 0)
    w_out.wait()
    with jax.named_scope("p44_take_part_out_sem"):
        take(part, out_sem)
    with jax.named_scope("p45_take_vt_allat_03items_v_sendat"):
        take(vt_all.at[:, 0:3 * items], v_send.at[0])
    with jax.named_scope("p46_take_vt_allat_03items_v_sendat"):
        take(vt_all.at[:, 0:3 * items], v_send.at[1])
    with jax.named_scope("p47_take_mqsat02_m_send"):
        take(mqs.at[0:2], m_send)
    with jax.named_scope("p48_take_hop_hop_send"):
        take(hop, hop_send)
    with jax.named_scope("p49_take_hop_fwd_send"):
        take(hop, fwd_send)
    with jax.named_scope("p50_take_rel_rel_send"):
        take(rel, rel_send)
    with jax.named_scope("p51_take_got_got_send"):
        take(got, got_send)
    with jax.named_scope("p52_take_fin_fin_send"):
        take(fin, fin_send)
    with jax.named_scope("p53_take_w_allat0count1_w_send"):
        take(w_all.at[0:count - 1], w_send)
    with jax.named_scope("p54_take_part_x_send"):
        take(part, x_send)


def half_steps(ratings, mask, vt, count):
    users, items = ratings.shape
    block = users // SIDE
    dma = pltpu.SemaphoreType.DMA
    any_spec = pl.BlockSpec(memory_space=pl.ANY)
    f32, bf16 = jnp.float32, jnp.bfloat16
    return pl.pallas_call(
        als_kernel,
        out_shape=(
            jax.ShapeDtypeStruct((32, WIDTH), f32),
            jax.ShapeDtypeStruct((PACK, items // 2), f32),
        ),
        in_specs=[any_spec, any_spec, any_spec],
        out_specs=(any_spec, any_spec),
        scratch_shapes=[
            pltpu.VMEM((4, block, items), f32),
            pltpu.VMEM((4, block, items), jnp.int32),
            pltpu.VMEM((WIDTH, items), f32),
            pltpu.VMEM((4, SIDE, SIDE, 2, 2, 16, items), bf16),
            pltpu.VMEM((4, 2, 2, SIDE, 16, items), bf16),
            pltpu.VMEM((4, 2, SIDE, 2, 16, 7 * items), bf16),
            pltpu.VMEM((64, 7 * items), bf16),
            pltpu.VMEM((TRI, 7 * items), bf16),
            pltpu.VMEM((TRI, items), f32),
            pltpu.VMEM((PACK, 128), f32),
            pltpu.VMEM((4, PACK, 128), f32),
            pltpu.VMEM((3, 2, HALF, 128), f32),
            pltpu.VMEM((2, HALF, 128), f32),
            pltpu.VMEM((2, 2, HALF, 128), f32),
            pltpu.VMEM((PACK, 128), f32),
            pltpu.VMEM((FULL, 128), f32),
            pltpu.VMEM((128, FULL), f32),
            pltpu.VMEM((2, 3, 16, FULL), f32),
            pltpu.VMEM((WIDTH * ROWS, 128), f32),
            pltpu.VMEM((ROWS, 128), f32),
            pltpu.VMEM((ROWS, 128), f32),
            pltpu.VMEM((32, WIDTH), f32),
            pltpu.VMEM((16, 128), bf16),
            pltpu.VMEM((count, 16, 128), bf16),
            pltpu.VMEM((128, 16 * SIDE * SIDE), f32),
            pltpu.VMEM((64, 32 * count), bf16),
            pltpu.VMEM((PACK, items // 2), f32),
            pltpu.VMEM((PACK, items // 2), f32),
            pltpu.VMEM((PACK, items // 2), f32),
            dma, dma((4,)), dma((2,)), dma((4,)), dma, dma((4,)), dma, dma((4,)), dma, dma((4,)),
            dma, dma((2,)), dma, dma((3,)), dma, dma, dma, dma((4,)), dma, dma, dma((5,)), dma,
            pltpu.SemaphoreType.REGULAR, pltpu.SemaphoreType.REGULAR,
        ],
        compiler_params=pltpu.CompilerParams(
            collective_id=0, has_side_effects=True, vmem_limit_bytes=60 * 1024 * 1024
        ),
    )(ratings, mask, vt)


def solution(mesh):
    block_spec = P(("part", "row"), "col")
    in_specs = (block_spec, block_spec, P(("part", "col"), None))
    out_specs = (P(("part", "row", "col"), None), P(("part", "col", "row"), None))
    count = mesh.shape["col"]

    def local_als(ratings, mask, v_init):
        w_own, packed = half_steps(ratings, mask, v_init.T, count)
        v_own, w_own = solve_items(packed, w_own)
        return w_own, v_own.T

    return jax.shard_map(local_als, mesh=mesh, in_specs=in_specs, out_specs=out_specs, check_vma=False)
```

```python
import jax
import jax.numpy as jnp
from jax import lax
from jax.experimental import pallas as pl
from jax.experimental.pallas import tpu as pltpu
from jax.sharding import PartitionSpec as P

RIDGE_WEIGHT = 0.05
WIDTH = 50
ROWS = 56
TRI = 1280
LANES = 128


def tri_off(j):
    return j * WIDTH - j * (j - 1) // 2


def outer_tile(vt, dst):
    lanes = vt.shape[1]
    for j in range(WIDTH):
        rows = WIDTH - j
        dst[tri_off(j):tri_off(j) + rows, :] = vt[j:WIDTH, :] * vt[j:j + 1, :]


def solve_tile(g_ref, rhs, fac, inv, sol):
    lanes = fac.shape[1]
    for pan in range(7):
        first = 8 * pan
        rows = ROWS - first
        count = min(8, WIDTH - first)
        ids = lax.broadcasted_iota(jnp.int32, (rows, lanes), 0)
        accs = []
        for c in range(count):
            j = first + c
            start = tri_off(j) - c
            if j < WIDTH - 1:
                raw = g_ref[start:start + rows, :]
            else:
                raw = jnp.broadcast_to(g_ref[tri_off(j):tri_off(j) + 1, :], (rows, lanes))
            col = jnp.where(ids < WIDTH - first, raw, 0.0)
            col = jnp.where(ids == c, col + RIDGE_WEIGHT, col)
            col = jnp.where(ids == WIDTH - first, rhs(j), col)
            accs.append(col)
        if pan:
            def body(k, accs):
                base = pl.multiple_of(k * ROWS, 8)
                left = fac[pl.ds(base + first, rows), :]
                return tuple(
                    acc - left * fac[pl.ds(base + first + c, 1), :] for c, acc in enumerate(accs)
                )
            accs = list(lax.fori_loop(0, first, body, tuple(accs), unroll=2))
        for c in range(count):
            j = first + c
            diag = accs[c][c:c + 1, :]
            root = lax.rsqrt(diag)
            root = root * (1.5 - 0.5 * (diag * root) * root)
            inv[j:j + 1, :] = root
            col = accs[c] * root
            fac[pl.ds(j * ROWS + first, rows), :] = col
            for later in range(c + 1, count):
                accs[later] = accs[later] - col * col[later:later + 1, :]
    sol[48:56, :] = jnp.zeros((8, lanes), jnp.float32)
    for pan in reversed(range(7)):
        first = 8 * pan
        count = min(8, WIDTH - first)
        left = []
        for c in range(count):
            j = first + c
            val = fac[j * ROWS + WIDTH:j * ROWS + WIDTH + 1, :]
            if pan < 6:
                dot = fac[j * ROWS + first + 8:j * ROWS + ROWS, :] * sol[first + 8:ROWS, :]
                val = val - jnp.sum(dot, axis=0, keepdims=True)
            left.append(val)
        for c in reversed(range(count)):
            j = first + c
            got = left[c] * inv[j:j + 1, :]
            sol[j:j + 1, :] = got
            for early in range(c):
                row = (first + early) * ROWS + j
                left[early] = left[early] - fac[row:row + 1, :] * got


def item_solve_kernel(g_ref, w_ref, out_ref, w_out, fac, inv, sol):
    w_out[...] = w_ref[...]
    solve_tile(g_ref, lambda j: g_ref[TRI + j:TRI + j + 1, :], fac, inv, sol)
    out_ref[...] = sol[:WIDTH, :]


def solve_items(packed, w_own):
    n = packed.shape[1]
    w_spec = pl.BlockSpec(w_own.shape, lambda i: (0, 0))
    return pl.pallas_call(
        item_solve_kernel,
        out_shape=(jax.ShapeDtypeStruct((WIDTH, n), jnp.float32), jax.ShapeDtypeStruct(w_own.shape, jnp.float32)),
        grid=(n // LANES,),
        in_specs=[pl.BlockSpec((packed.shape[0], LANES), lambda i: (0, i)), w_spec],
        out_specs=(pl.BlockSpec((WIDTH, LANES), lambda i: (0, i)), w_spec),
        scratch_shapes=[
            pltpu.VMEM((WIDTH * ROWS, LANES), jnp.float32),
            pltpu.VMEM((ROWS, LANES), jnp.float32),
            pltpu.VMEM((ROWS, LANES), jnp.float32),
        ],
    )(packed, w_own)


PACK = 1344
FULL = 1408
SIDE = 4
HALF = PACK // 2
CUT = 384


def dot_cols(left, right):
    return lax.dot_general(left, right, (((1,), (1,)), ((), ())), preferred_element_type=jnp.float32)


def als_kernel(
    rate_hbm, mask_hbm, v_hbm, w_hbm, item_hbm,
    rate, mask, v_raw, mqs, hop, rhs, vt_all, o_all, tmp, gram, home, unit, rel, got, tot, acc, flat, fin,
    fac, inv, sol, w_new, pack, w_all, wt, wb, part, swap_got, item_sum,
    v_sem, load_sem, v_send, v_recv, m_send, m_recv, hop_send, hop_recv, fwd_send, own_sem,
    rel_send, rel_recv, got_send, got_recv, fin_send, fin_recv, w_send, w_recv, w_sem, x_send, x_recv, out_sem, y_in, z_in,
):
    items = v_raw.shape[1]
    count = w_all.shape[0]
    col = lax.axis_index("col")
    row = lax.axis_index("row")
    other = {"row": 1 - row}
    x = lax.rem(col, SIDE)
    y = lax.rem(col // SIDE, SIDE)
    z = col // (SIDE * SIDE)

    def turn(pos, step):
        return lax.rem(pos + step, SIDE)

    def x_peer(step):
        return {"col": col - x + turn(x, step)}

    def y_peer(step):
        return {"col": col + SIDE * (turn(y, step) - y)}

    def z_peer(step):
        return {"col": col + SIDE * SIDE * (turn(z, step) - z)}

    def send(src, dst, send_sem, recv_sem, peer):
        return pltpu.make_async_remote_copy(
            src_ref=src, dst_ref=dst, send_sem=send_sem, recv_sem=recv_sem,
            device_id=peer, device_id_type=pl.DeviceIdType.MESH,
        )

    def signal(sem, peer):
        pl.semaphore_signal(sem, inc=1, device_id=peer, device_id_type=pl.DeviceIdType.MESH)

    def start(copies):
        for copy in copies:
            copy.start()

    def take(ref, sem):
        pltpu.make_async_copy(ref, ref, sem).wait()

    barrier = pltpu.get_barrier_semaphore()
    peers = [peer(step) for step in (1, 2, 3) for peer in (x_peer, y_peer, z_peer)] + [other]
    for peer in peers:
        signal(barrier, peer)

    owners = [turn(z, 2), turn(z, 1), turn(z, 3), z]
    block = rate.shape[1]
    v_load = pltpu.make_async_copy(v_hbm, v_raw, v_sem)
    v_load.start()
    loads = []
    for k, owner in enumerate(owners):
        rows = pl.ds(pl.multiple_of(owner * block, block), block)
        pair = [
            pltpu.make_async_copy(rate_hbm.at[rows], rate.at[k], load_sem.at[k]),
            pltpu.make_async_copy(mask_hbm.at[rows], mask.at[k], load_sem.at[k]),
        ]
        loads.append(pair)
    start(loads[0])

    def cast_chunk(k):
        def cast_step(i, carry):
            rows = pl.ds(pl.multiple_of(i * 128, 128), 128)
            seen = mask[k, rows, :]
            mqs[k, i, :, :, 0] = seen.astype(jnp.float32).astype(jnp.bfloat16).reshape(SIDE, 2, 16, items)
            rated = jnp.where(seen != 0, rate[k, rows, :], 0.0)
            mqs[k, i, :, :, 1] = rated.astype(jnp.bfloat16).reshape(SIDE, 2, 16, items)
            return carry

        with jax.named_scope("p00__0__cast_step_0"):
            lax.fori_loop(0, SIDE, cast_step, 0)

    def axis_peer(c, step):
        return y_peer(step) if c else x_peer(step)

    def share(s, c, pos):
        return mqs.at[(0, 2, 1, 3)[s], pos, :, 1] if c else mqs.at[s, :, pos, 0]

    def columns(slot):
        return slice(slot * items, (slot + 1) * items)

    m_copies, own_copies, hops, passes = [], [], [], []
    for s in range(4):
        m_copies.append([])
        own_copies.append([])
        hops.append([])
        passes.append([])
        for c, pos in enumerate((x, y)):
            for m, step in enumerate((1, 3)):
                hops[s].append(send(
                    share(s, c, turn(pos, 2)).at[:, m], hop.at[s, c, m],
                    hop_send, hop_recv.at[s], axis_peer(c, step),
                ))
                m_copies[s].append(send(
                    share(s, c, turn(pos, step)), rhs.at[s, c, :, :, :, columns(3 * c + step)],
                    m_send, m_recv.at[s], axis_peer(c, step),
                ))
                passes[s].append(send(
                    hop.at[s, c, m], rhs.at[s, c, :, m, :, columns(3 * c + 2)],
                    fwd_send, m_recv.at[s], axis_peer(c, step),
                ))
            own_copies[s].append(pltpu.make_async_copy(
                share(s, c, pos), rhs.at[s, c, :, :, :, columns(0)], own_sem.at[s]
            ))

    def pass_on(s):
        with jax.named_scope("p01_take_hopats_hop_recvats"):
            take(hop.at[s], hop_recv.at[s])
        start(passes[s])

    def half_columns(slot, side):
        return pl.ds(pl.multiple_of(slot * items + side * (items // 2), items // 2), items // 2)

    v_copies, v_swaps = [], []
    for d in (1, 3, 2):
        for axis in range(2):
            slot = 3 * axis + d
            v_copies.append(send(
                vt_all.at[:, half_columns(0, row)], vt_all.at[:, half_columns(slot, row)],
                v_send.at[0], v_recv.at[d], axis_peer(axis, d),
            ))
            v_swaps.append(send(
                vt_all.at[:, half_columns(slot, row)], vt_all.at[:, half_columns(slot, row)],
                v_send.at[1], v_recv.at[0], other,
            ))

    tmp[48:64, :] = jnp.zeros((16, items), jnp.float32)
    v_load.wait()
    tmp[0:WIDTH, :] = v_raw[...]
    vt_all[:, 0:items] = tmp[0:64, :].astype(jnp.bfloat16)
    with jax.named_scope("p02_take_rateat02_load_semat0"):
        take(rate.at[0:2], load_sem.at[0])
    for k in range(1, 4):
        start(loads[k])
    with jax.named_scope("p03_cast_chunk_0"):
        cast_chunk(0)
    with jax.named_scope("p04_plsemaphore_wait_barrier_len_p"):
        pl.semaphore_wait(barrier, len(peers))
    start(v_copies)
    start(hops[0])
    start(m_copies[0])
    for step in (1, 2, 3):
        signal(y_in, y_peer(step))
    for k in range(1, 4):
        with jax.named_scope("p05_take_rateat02_load_sematk"):
            take(rate.at[0:2], load_sem.at[k])
        with jax.named_scope("p06_cast_chunk_k"):
            cast_chunk(k)
    for s in range(4):
        start(own_copies[s])
    for s in range(4):
        rhs[s, 0, :, :, :, 4 * items:7 * items] = jnp.zeros((4, 2, 16, 3 * items), jnp.bfloat16)
        rhs[s, 1, :, :, :, items:4 * items] = jnp.zeros((4, 2, 16, 3 * items), jnp.bfloat16)
    tmp[1272:1280, :] = jnp.zeros((8, items), jnp.float32)

    def outer_step(slot, carry):
        cols = pl.ds(pl.multiple_of(slot * items, items), items)
        outer_tile(vt_all[:, cols].astype(jnp.float32), tmp)
        o_all[:, cols] = tmp[...].astype(jnp.bfloat16)
        return carry

    with jax.named_scope("p07__0_1_outer_step_0"):
        lax.fori_loop(0, 1, outer_step, 0)
    for i, d in enumerate((1, 3, 2)):
        with jax.named_scope("p08_take_vt_allat_0items_v_recvatd"):
            take(vt_all.at[:, 0:items], v_recv.at[d])
        start(v_swaps[2 * i:2 * i + 2])
    with jax.named_scope("p09_pass_on_0"):
        pass_on(0)
    start(hops[1])
    start(m_copies[1])
    start(hops[2])
    with jax.named_scope("p10_plsemaphore_wait_y_in_3"):
        pl.semaphore_wait(y_in, 3)
    for step in (1, 2, 3):
        signal(z_in, z_peer(step))

    def users_of(s, m, cols):
        return rhs[s, :, :, m, :, cols].reshape(128, cols.stop - cols.start)

    near, far = slice(0, items), slice(items, 7 * items)
    def own_part(s):
        with jax.named_scope("p11_take_hopats_own_semats"):
            take(hop.at[s], own_sem.at[s])

        def near_step(i, carry):
            rows = pl.ds(pl.multiple_of(i * 640, 640), 640)
            home[s, rows, :] = dot_cols(o_all[rows, near], users_of(s, 0, near))
            return carry

        home[s, TRI:PACK, :] = dot_cols(vt_all[:, near], users_of(s, 1, near))
        with jax.named_scope("p12__0_2_near_step_0"):
            lax.fori_loop(0, 2, near_step, 0)
    with jax.named_scope("p13_own_part_0"):
        own_part(0)
    with jax.named_scope("p14_take_vt_allat_03items_v_recvat"):
        take(vt_all.at[:, 0:3 * items], v_recv.at[0])
    with jax.named_scope("p15__1_7_outer_step_0"):
        lax.fori_loop(1, 7, outer_step, 0)

    low = lax.broadcasted_iota(jnp.int32, (HALF, 128), 1) < 64
    pieces = (slice(0, CUT), slice(CUT, HALF))
    ways = (1, 3)

    def partial(s, dst, p):
        rows = pieces[p]
        for rows in (rows, slice(HALF + rows.start, min(HALF + rows.stop, TRI))):
            dst[rows, :] = home[s, rows, :] + dot_cols(o_all[rows, far], users_of(s, 0, far))
        if p:
            dst[TRI:PACK, :] = home[s, TRI:PACK, :] + dot_cols(vt_all[:, far], users_of(s, 1, far))

    def arrived(s):
        with jax.named_scope("p16_take_mqsat0_03_m_recvats"):
            take(mqs.at[0, 0:3], m_recv.at[s])

    def pack_units(s, p):
        rows = pieces[p]
        partial(s, gram, p)
        here = low[:rows.stop - rows.start]
        top, bottom = gram[rows, :], gram[HALF + rows.start:HALF + rows.stop, :]
        unit[s, 0, rows, :] = jnp.where(here, top, pltpu.roll(bottom, 64, 1))
        unit[s, 1, rows, :] = jnp.where(here, pltpu.roll(top, 64, 1), bottom)

    arrived(0)
    for p, rows in enumerate(pieces):
        pack_units(0, p)
        for c in range(2):
            send(unit.at[0, c, rows], rel.at[c, rows], rel_send, rel_recv.at[p], z_peer(ways[c])).start()
    with jax.named_scope("p17_pass_on_1"):
        pass_on(1)
    start(m_copies[2])
    start(hops[3])
    with jax.named_scope("p18_own_part_1"):
        own_part(1)
    with jax.named_scope("p19_pass_on_2"):
        pass_on(2)
    start(m_copies[3])
    with jax.named_scope("p20_own_part_2"):
        own_part(2)
    arrived(1)
    for p, rows in enumerate(pieces):
        pack_units(1, p)
        with jax.named_scope("p21_take_relat_rows_rel_recvatp"):
            take(rel.at[:, rows], rel_recv.at[p])
        for c in range(2):
            unit[1, c, rows, :] = unit[1, c, rows, :] + rel[c, rows, :]
            send(unit.at[1, c, rows], got.at[0, c, rows], got_send, got_recv.at[0], z_peer(ways[c])).start()
    with jax.named_scope("p22_pass_on_3"):
        pass_on(3)
    arrived(2)
    for p, rows in enumerate(pieces):
        pack_units(2, p)
        for c in range(2):
            send(
                unit.at[2, c, rows], got.at[1, c, rows], got_send, got_recv.at[1 + p], z_peer(ways[1 - c])
            ).start()
    with jax.named_scope("p23_own_part_3"):
        own_part(3)
    arrived(3)
    for p in range(2):
        partial(3, tot, p)
    acc[PACK:FULL, :] = jnp.zeros((FULL - PACK, 128), jnp.float32)
    with jax.named_scope("p24_take_gotat0_got_recvat0"):
        take(got.at[0], got_recv.at[0])
    with jax.named_scope("p25_plsemaphore_wait_z_in_3"):
        pl.semaphore_wait(z_in, 3)
    for p, rows in enumerate(pieces):
        size = rows.stop - rows.start
        with jax.named_scope("p26_take_gotat1__rows_got_recvat1p"):
            take(got.at[1, :, rows], got_recv.at[1 + p])
        sum_a = got[0, 0, rows] + got[1, 0, rows]
        sum_b = got[0, 1, rows] + got[1, 1, rows]
        here = low[:size]
        at = 2 * rows.start
        acc[at:at + size, :] = tot[rows, :] + jnp.where(here, sum_a, pltpu.roll(sum_b, 64, 1))
        acc[at + size:at + 2 * size, :] = (
            tot[HALF + rows.start:HALF + rows.stop, :] + jnp.where(here, pltpu.roll(sum_a, 64, 1), sum_b)
        )
        cols = slice(at, FULL if p else 2 * CUT)
        for i in range(cols.start // 128, cols.stop // 128):
            flat[:, i * 128:(i + 1) * 128] = acc[i * 128:(i + 1) * 128, :].T
        for d in (2, 1, 3):
            for c, pos in enumerate((y, x)):
                users = pl.ds(pl.multiple_of(64 * c + 16 * turn(pos, d), 16), 16)
                send(
                    flat.at[users, cols], fin.at[c, d - 1, :, cols], fin_send, fin_recv, axis_peer(1 - c, d)
                ).start()
    with jax.named_scope("p27_take_fin_fin_recv"):
        take(fin, fin_recv)

    zeros = jnp.zeros((96, 128), jnp.float32)
    for i in range(FULL // 128):
        cols = slice(i * 128, (i + 1) * 128)
        mine = [zeros]
        for c, pos in ((1, x), (0, y)):
            rows = pl.ds(pl.multiple_of(64 * c + 16 * pos, 16), 16)
            mine.insert(0, flat[rows, cols] + fin[c, 0, :, cols] + fin[c, 1, :, cols] + fin[c, 2, :, cols])
        acc[cols, :] = jnp.concatenate(mine, axis=0).T
    for rows in pieces:
        size = rows.stop - rows.start
        tot[rows, :] = acc[2 * rows.start:2 * rows.start + size, :]
        tot[HALF + rows.start:HALF + rows.stop, :] = acc[2 * rows.start + size:2 * rows.stop, :]
    with jax.named_scope("p28_solve_tile_tot_lambdajtotjj1__"):
        solve_tile(tot, lambda j: tot[TRI + j:TRI + j + 1, :], fac, inv, sol)
    turned = jnp.concatenate([sol[...], jnp.zeros((72, 128), jnp.float32)], axis=0).T
    lane = lax.broadcasted_iota(jnp.int32, (16, 128), 1)
    pack[...] = jnp.where(lane < 64, turned[:16], pltpu.roll(turned[16:32], 64, 1)).astype(jnp.bfloat16)

    plane = SIDE * SIDE

    place = col - z * plane
    w_own = pltpu.make_async_copy(pack, w_all.at[col], w_recv.at[0])
    w_own.start()
    for t, turned_by in enumerate((0, 1, 3, 2)):
        base = turn(z, turned_by) * plane

        def send_step(i, carry):
            target = place + i
            target = base + jnp.where(target < plane, target, target - plane)
            send(pack, w_all.at[col], w_send, w_recv.at[(0, 2, 1, 3)[t]], {"col": target}).start()
            return carry

        with jax.named_scope("p29__0iftelse1_plane_send_step_0"):
            lax.fori_loop(0 if t else 1, plane, send_step, 0)
    w_new[...] = turned[:32, :WIDTH]
    w_out = pltpu.make_async_copy(w_new, w_hbm, w_sem)
    w_out.start()

    users = 16 * count
    step = 16 * plane
    tall = tmp.at[:, 0:step]
    tall[1272:1280, :] = jnp.zeros((8, step), jnp.float32)

    def plane_step(t, carry):
        k = 3 - 2 * t + 3 * (t // 2)
        owner = turn(z, t + (t // 2) * (5 - 2 * t))

        with jax.named_scope("p30_take_w_allat0plane_w_recvatt"):
            take(w_all.at[0:plane], w_recv.at[t])
        for i in range(step // 128):
            rows = w_all[pl.ds(owner * plane + 8 * i, 8)].reshape(128, 128)
            wt[:, i * 128:(i + 1) * 128] = rows.astype(jnp.float32).T

        def colour_step(c, carry):
            vals = wt[pl.ds(pl.multiple_of(64 * c, 64), 64), :]
            cols = pl.ds(pl.multiple_of(c * users + k * step, step), step)
            wb[:, cols] = vals.astype(jnp.bfloat16)
            outer_tile(vals, tall)
            o_all[:, cols] = tall[...].astype(jnp.bfloat16)
            return carry

        with jax.named_scope("p31__0_2_colour_step_0"):
            lax.fori_loop(0, 2, colour_step, 0)
        return carry

    with jax.named_scope("p32__0__plane_step_0"):
        lax.fori_loop(0, SIDE, plane_step, 0)
    half = items // 2

    def item_rows(side, left, m):
        cols = pl.ds(pl.multiple_of(side * half, half), half)
        total = None
        for c in range(2):
            right = mqs[:, :, :, c, m, :, cols].reshape(users, half)
            term = jnp.dot(left(c), right, preferred_element_type=jnp.float32)
            total = term if total is None else total + term
        return total

    def rhs_rows(side):
        return item_rows(side, lambda c: wb[:, c * users:(c + 1) * users], 1)

    def gram_rows(side, rows):
        return item_rows(side, lambda c: o_all[rows, c * users:(c + 1) * users], 0)

    def swap_copy(i, rows):
        return send(part.at[rows], swap_got.at[rows], x_send, x_recv.at[i], other)

    def finish(i, rows, val):
        with jax.named_scope("p33_swap_copy_i_rowswait_recv_"):
            swap_copy(i, rows).wait_recv()
        item_sum[rows, :] = val + swap_got[rows, :]
        pltpu.make_async_copy(item_sum.at[rows], item_hbm.at[rows], out_sem).start()

    tail = pl.ds(TRI, PACK - TRI)
    part[tail, :] = rhs_rows(1 - row)
    swap_copy(2, tail).start()

    def away_step(i, carry):
        rows = pl.ds(pl.multiple_of(i * 640, 640), 640)
        part[rows, :] = gram_rows(1 - row, rows)
        swap_copy(i, rows).start()
        return carry

    def home_step(i, carry):
        rows = pl.ds(pl.multiple_of(i * 640, 640), 640)
        finish(i, rows, gram_rows(row, rows))
        return carry

    with jax.named_scope("p34__0_2_away_step_0"):
        lax.fori_loop(0, 2, away_step, 0)
    finish(2, tail, rhs_rows(row))
    with jax.named_scope("p35__0_2_home_step_0"):
        lax.fori_loop(0, 2, home_step, 0)
    w_out.wait()
    with jax.named_scope("p36_take_part_out_sem"):
        take(part, out_sem)
    with jax.named_scope("p37_take_vt_allat_03items_v_sendat"):
        take(vt_all.at[:, 0:3 * items], v_send.at[0])
    with jax.named_scope("p38_take_vt_allat_03items_v_sendat"):
        take(vt_all.at[:, 0:3 * items], v_send.at[1])
    with jax.named_scope("p39_take_mqsat02_m_send"):
        take(mqs.at[0:2], m_send)
    with jax.named_scope("p40_take_hop_hop_send"):
        take(hop, hop_send)
    with jax.named_scope("p41_take_hop_fwd_send"):
        take(hop, fwd_send)
    with jax.named_scope("p42_take_rel_rel_send"):
        take(rel, rel_send)
    with jax.named_scope("p43_take_got_got_send"):
        take(got, got_send)
    with jax.named_scope("p44_take_fin_fin_send"):
        take(fin, fin_send)
    with jax.named_scope("p45_take_w_allat0count1_w_send"):
        take(w_all.at[0:count - 1], w_send)
    with jax.named_scope("p46_take_part_x_send"):
        take(part, x_send)


def half_steps(ratings, mask, vt, count):
    users, items = ratings.shape
    block = users // SIDE
    dma = pltpu.SemaphoreType.DMA
    any_spec = pl.BlockSpec(memory_space=pl.ANY)
    f32, bf16 = jnp.float32, jnp.bfloat16
    return pl.pallas_call(
        als_kernel,
        out_shape=(
            jax.ShapeDtypeStruct((32, WIDTH), f32),
            jax.ShapeDtypeStruct((PACK, items // 2), f32),
        ),
        in_specs=[any_spec, any_spec, any_spec],
        out_specs=(any_spec, any_spec),
        scratch_shapes=[
            pltpu.VMEM((4, block, items), f32),
            pltpu.VMEM((4, block, items), jnp.int32),
            pltpu.VMEM((WIDTH, items), f32),
            pltpu.VMEM((4, SIDE, SIDE, 2, 2, 16, items), bf16),
            pltpu.VMEM((4, 2, 2, SIDE, 16, items), bf16),
            pltpu.VMEM((4, 2, SIDE, 2, 16, 7 * items), bf16),
            pltpu.VMEM((64, 7 * items), bf16),
            pltpu.VMEM((TRI, 7 * items), bf16),
            pltpu.VMEM((TRI, items), f32),
            pltpu.VMEM((PACK, 128), f32),
            pltpu.VMEM((4, PACK, 128), f32),
            pltpu.VMEM((3, 2, HALF, 128), f32),
            pltpu.VMEM((2, HALF, 128), f32),
            pltpu.VMEM((2, 2, HALF, 128), f32),
            pltpu.VMEM((PACK, 128), f32),
            pltpu.VMEM((FULL, 128), f32),
            pltpu.VMEM((128, FULL), f32),
            pltpu.VMEM((2, 3, 16, FULL), f32),
            pltpu.VMEM((WIDTH * ROWS, 128), f32),
            pltpu.VMEM((ROWS, 128), f32),
            pltpu.VMEM((ROWS, 128), f32),
            pltpu.VMEM((32, WIDTH), f32),
            pltpu.VMEM((16, 128), bf16),
            pltpu.VMEM((count, 16, 128), bf16),
            pltpu.VMEM((128, 16 * SIDE * SIDE), f32),
            pltpu.VMEM((64, 32 * count), bf16),
            pltpu.VMEM((PACK, items // 2), f32),
            pltpu.VMEM((PACK, items // 2), f32),
            pltpu.VMEM((PACK, items // 2), f32),
            dma, dma((4,)), dma((2,)), dma((4,)), dma, dma((4,)), dma, dma((4,)), dma, dma((4,)),
            dma, dma((2,)), dma, dma((3,)), dma, dma, dma, dma((4,)), dma, dma, dma((3,)), dma,
            pltpu.SemaphoreType.REGULAR, pltpu.SemaphoreType.REGULAR,
        ],
        compiler_params=pltpu.CompilerParams(
            collective_id=0, has_side_effects=True, vmem_limit_bytes=60 * 1024 * 1024
        ),
    )(ratings, mask, vt)


def solution(mesh):
    block_spec = P(("part", "row"), "col")
    in_specs = (block_spec, block_spec, P(("part", "col"), None))
    out_specs = (P(("part", "row", "col"), None), P(("part", "col", "row"), None))
    count = mesh.shape["col"]

    def local_als(ratings, mask, v_init):
        w_own, packed = half_steps(ratings, mask, v_init.T, count)
        v_own, w_own = solve_items(packed, w_own)
        return w_own, v_own.T

    return jax.shard_map(local_als, mesh=mesh, in_specs=in_specs, out_specs=out_specs, check_vma=False)
```

```python
import jax
import jax.numpy as jnp
from jax import lax
from jax.experimental import pallas as pl
from jax.experimental.pallas import tpu as pltpu
from jax.sharding import PartitionSpec as P

RIDGE_WEIGHT = 0.05
WIDTH = 50
ROWS = 56
TRI = 1280
LANES = 128


def tri_off(j):
    return j * WIDTH - j * (j - 1) // 2


def outer_tile(vt, dst):
    lanes = vt.shape[1]
    for j in range(WIDTH):
        rows = WIDTH - j
        dst[tri_off(j):tri_off(j) + rows, :] = vt[j:WIDTH, :] * vt[j:j + 1, :]


def solve_tiles(g_ref, rhs_ref, facs, inv, sol, ready=None):
    groups = [slice(i * LANES, (i + 1) * LANES) for i in range(len(facs))]
    for pan in range(7):
        first = 8 * pan
        rows = ROWS - first
        count = min(8, WIDTH - first)
        if ready is not None:
            ready(pan)
        ids = lax.broadcasted_iota(jnp.int32, (rows, LANES), 0)

        def panel(here):
            accs = []
            for c in range(count):
                j = first + c
                start = tri_off(j) - c
                if j < WIDTH - 1:
                    raw = g_ref[start:start + rows, here]
                else:
                    raw = jnp.broadcast_to(g_ref[tri_off(j):tri_off(j) + 1, here], (rows, LANES))
                col = jnp.where(ids < WIDTH - first, raw, 0.0)
                col = jnp.where(ids == c, col + RIDGE_WEIGHT, col)
                accs.append(jnp.where(ids == WIDTH - first, rhs_ref[j:j + 1, here], col))
            return accs

        def update(fac, k, accs):
            base = pl.multiple_of(k * ROWS, 8)
            left = fac[pl.ds(base + first, rows), :]
            return [acc - left * fac[pl.ds(base + first + c, 1), :] for c, acc in enumerate(accs)]

        if not pan:
            parts = [panel(here) for here in groups]
        elif len(groups) * count * rows <= 48 * 8:
            parts = lax.fori_loop(
                0, first, lambda k, parts: [update(fac, k, accs) for fac, accs in zip(facs, parts)],
                [panel(here) for here in groups], unroll=2,
            )
        else:
            parts = []
            for here, fac in zip(groups, facs):
                parts.append(lax.fori_loop(0, first, lambda k, accs: update(fac, k, accs), panel(here), unroll=2))
        parts = [list(accs) for accs in parts]
        for c in range(count):
            j = first + c
            for here, fac, accs in zip(groups, facs, parts):
                diag = accs[c][c:c + 1, :]
                root = lax.rsqrt(diag)
                root = root * (1.5 - 0.5 * (diag * root) * root)
                inv[j:j + 1, here] = root
                col = accs[c] * root
                fac[pl.ds(j * ROWS + first, rows), :] = col
                for later in range(c + 1, count):
                    accs[later] = accs[later] - col * col[later:later + 1, :]
    for here in groups:
        sol[48:56, here] = jnp.zeros((8, LANES), jnp.float32)
    for pan in reversed(range(7)):
        first = 8 * pan
        count = min(8, WIDTH - first)
        lefts = []
        for here, fac in zip(groups, facs):
            left = []
            for c in range(count):
                j = first + c
                val = fac[j * ROWS + WIDTH:j * ROWS + WIDTH + 1, :]
                if pan < 6:
                    dot = fac[j * ROWS + first + 8:j * ROWS + ROWS, :] * sol[first + 8:ROWS, here]
                    val = val - jnp.sum(dot, axis=0, keepdims=True)
                left.append(val)
            lefts.append(left)
        for c in reversed(range(count)):
            j = first + c
            for here, fac, left in zip(groups, facs, lefts):
                got = left[c] * inv[j:j + 1, here]
                sol[j:j + 1, here] = got
                for early in range(c):
                    row = (first + early) * ROWS + j
                    left[early] = left[early] - fac[row:row + 1, :] * got


def item_solve_kernel(g_hbm, w_ref, out_ref, w_out, gram, inv, sol, sems, *facs):
    copies = []
    for i, (start, stop) in enumerate(((0, 384), (TRI, gram.shape[0]), (384, 688), (688, TRI))):
        copy = pltpu.make_async_copy(g_hbm.at[start:stop], gram.at[start:stop], sems.at[i])
        copy.start()
        copies.append(copy)
    w_out[...] = w_ref[...]

    def ready(pan):
        for copy in (copies[:2], copies[2:3], copies[3:], [], [], [], [])[pan]:
            copy.wait()

    solve_tiles(gram, gram.at[TRI:gram.shape[0]], facs, inv, sol, ready)
    out_ref[...] = sol[:WIDTH, :]


def solve_items(packed, w_own):
    n = packed.shape[1]
    vmem_spec = pl.BlockSpec(memory_space=pltpu.VMEM)
    return pl.pallas_call(
        item_solve_kernel,
        out_shape=(jax.ShapeDtypeStruct((WIDTH, n), jnp.float32), jax.ShapeDtypeStruct(w_own.shape, jnp.float32)),
        in_specs=[pl.BlockSpec(memory_space=pl.ANY), vmem_spec],
        out_specs=(vmem_spec, vmem_spec),
        scratch_shapes=[
            pltpu.VMEM(packed.shape, jnp.float32),
            pltpu.VMEM((ROWS, n), jnp.float32),
            pltpu.VMEM((ROWS, n), jnp.float32),
            pltpu.SemaphoreType.DMA((4,)),
        ] + [pltpu.VMEM((WIDTH * ROWS, LANES), jnp.float32)] * (n // LANES),
    )(packed, w_own)


PACK = 1344
FULL = 1408
SIDE = 4
HALF = PACK // 2
CUT = 384


def dot_cols(left, right):
    return lax.dot_general(left, right, (((1,), (1,)), ((), ())), preferred_element_type=jnp.float32)


def als_kernel(
    rate_hbm, mask_hbm, v_hbm, w_hbm, item_hbm,
    rate, mask, v_raw, mqs, hop, rhs, vt_all, o_all, tmp, gram, home, unit, rel, got, tot, acc, flat, fin,
    fac, inv, sol, w_new, pack, w_all, wt, wb, part, swap_got, item_sum,
    v_sem, load_sem, v_send, v_recv, m_send, m_recv, hop_send, hop_recv, fwd_send, own_sem,
    rel_send, rel_recv, got_send, got_recv, fin_send, fin_recv, w_send, w_recv, w_sem, x_send, x_recv, out_sem, y_in, z_in,
):
    items = v_raw.shape[1]
    count = w_all.shape[0]
    col = lax.axis_index("col")
    row = lax.axis_index("row")
    other = {"row": 1 - row}
    x = lax.rem(col, SIDE)
    y = lax.rem(col // SIDE, SIDE)
    z = col // (SIDE * SIDE)

    def turn(pos, step):
        return lax.rem(pos + step, SIDE)

    def x_peer(step):
        return {"col": col - x + turn(x, step)}

    def y_peer(step):
        return {"col": col + SIDE * (turn(y, step) - y)}

    def z_peer(step):
        return {"col": col + SIDE * SIDE * (turn(z, step) - z)}

    def send(src, dst, send_sem, recv_sem, peer):
        return pltpu.make_async_remote_copy(
            src_ref=src, dst_ref=dst, send_sem=send_sem, recv_sem=recv_sem,
            device_id=peer, device_id_type=pl.DeviceIdType.MESH,
        )

    def signal(sem, peer):
        pl.semaphore_signal(sem, inc=1, device_id=peer, device_id_type=pl.DeviceIdType.MESH)

    def start(copies):
        for copy in copies:
            copy.start()

    def take(ref, sem):
        pltpu.make_async_copy(ref, ref, sem).wait()

    barrier = pltpu.get_barrier_semaphore()
    peers = [peer(step) for step in (1, 2, 3) for peer in (x_peer, y_peer, z_peer)] + [other]
    for peer in peers:
        signal(barrier, peer)

    owners = [turn(z, 2), turn(z, 1), turn(z, 3), z]
    block = rate.shape[1]
    v_load = pltpu.make_async_copy(v_hbm, v_raw, v_sem)
    v_load.start()
    loads = []
    for k, owner in enumerate(owners):
        rows = pl.ds(pl.multiple_of(owner * block, block), block)
        pair = [
            pltpu.make_async_copy(rate_hbm.at[rows], rate.at[k], load_sem.at[k]),
            pltpu.make_async_copy(mask_hbm.at[rows], mask.at[k], load_sem.at[k]),
        ]
        loads.append(pair)
    start(loads[0])

    def cast_chunk(k):
        def cast_step(i, carry):
            rows = pl.ds(pl.multiple_of(i * 128, 128), 128)
            seen = mask[k, rows, :]
            mqs[k, i, :, :, 0] = seen.astype(jnp.float32).astype(jnp.bfloat16).reshape(SIDE, 2, 16, items)
            rated = jnp.where(seen != 0, rate[k, rows, :], 0.0)
            mqs[k, i, :, :, 1] = rated.astype(jnp.bfloat16).reshape(SIDE, 2, 16, items)
            return carry

        lax.fori_loop(0, SIDE, cast_step, 0)

    def axis_peer(c, step):
        return y_peer(step) if c else x_peer(step)

    def share(s, c, pos):
        return mqs.at[(0, 2, 1, 3)[s], pos, :, 1] if c else mqs.at[s, :, pos, 0]

    def columns(slot):
        return slice(slot * items, (slot + 1) * items)

    m_copies, own_copies, hops, passes = [], [], [], []
    for s in range(4):
        m_copies.append([])
        own_copies.append([])
        hops.append([])
        passes.append([])
        for c, pos in enumerate((x, y)):
            for m, step in enumerate((1, 3)):
                hops[s].append(send(
                    share(s, c, turn(pos, 2)).at[:, m], hop.at[s, c, m],
                    hop_send, hop_recv.at[s], axis_peer(c, step),
                ))
                m_copies[s].append(send(
                    share(s, c, turn(pos, step)), rhs.at[s, c, :, :, :, columns(3 * c + step)],
                    m_send, m_recv.at[s], axis_peer(c, step),
                ))
                passes[s].append(send(
                    hop.at[s, c, m], rhs.at[s, c, :, m, :, columns(3 * c + 2)],
                    fwd_send, m_recv.at[s], axis_peer(c, step),
                ))
            own_copies[s].append(pltpu.make_async_copy(
                share(s, c, pos), rhs.at[s, c, :, :, :, columns(0)], own_sem.at[s]
            ))

    def pass_on(s):
        take(hop.at[s], hop_recv.at[s])
        start(passes[s])

    def half_columns(slot, side):
        return pl.ds(pl.multiple_of(slot * items + side * (items // 2), items // 2), items // 2)

    v_copies, v_swaps = [], []
    for d in (1, 3, 2):
        for axis in range(2):
            slot = 3 * axis + d
            v_copies.append(send(
                vt_all.at[:, half_columns(0, row)], vt_all.at[:, half_columns(slot, row)],
                v_send.at[0], v_recv.at[d], axis_peer(axis, d),
            ))
            v_swaps.append(send(
                vt_all.at[:, half_columns(slot, row)], vt_all.at[:, half_columns(slot, row)],
                v_send.at[1], v_recv.at[0], other,
            ))

    tmp[48:64, :] = jnp.zeros((16, items), jnp.float32)
    v_load.wait()
    tmp[0:WIDTH, :] = v_raw[...]
    vt_all[:, 0:items] = tmp[0:64, :].astype(jnp.bfloat16)
    take(rate.at[0:2], load_sem.at[0])
    for k in range(1, 4):
        start(loads[k])
    cast_chunk(0)
    pl.semaphore_wait(barrier, len(peers))
    start(v_copies)
    start(hops[0])
    start(m_copies[0])
    for step in (1, 2, 3):
        signal(y_in, y_peer(step))
    for k in range(1, 4):
        take(rate.at[0:2], load_sem.at[k])
        cast_chunk(k)
    for s in range(4):
        start(own_copies[s])
    for s in range(4):
        rhs[s, 0, :, :, :, 4 * items:7 * items] = jnp.zeros((4, 2, 16, 3 * items), jnp.bfloat16)
        rhs[s, 1, :, :, :, items:4 * items] = jnp.zeros((4, 2, 16, 3 * items), jnp.bfloat16)
    tmp[1272:1280, :] = jnp.zeros((8, items), jnp.float32)

    def outer_step(slot, carry):
        cols = pl.ds(pl.multiple_of(slot * items, items), items)
        outer_tile(vt_all[:, cols].astype(jnp.float32), tmp)
        o_all[:, cols] = tmp[...].astype(jnp.bfloat16)
        return carry

    lax.fori_loop(0, 1, outer_step, 0)
    for i, d in enumerate((1, 3, 2)):
        take(vt_all.at[:, 0:items], v_recv.at[d])
        start(v_swaps[2 * i:2 * i + 2])
    pass_on(0)
    start(hops[1])
    start(m_copies[1])
    start(hops[2])
    pl.semaphore_wait(y_in, 3)
    for step in (1, 2, 3):
        signal(z_in, z_peer(step))

    def users_of(s, m, cols):
        return rhs[s, :, :, m, :, cols].reshape(128, cols.stop - cols.start)

    near, far = slice(0, items), slice(items, 7 * items)
    def own_part(s):
        take(hop.at[s], own_sem.at[s])

        def near_step(i, carry):
            rows = pl.ds(pl.multiple_of(i * 640, 640), 640)
            home[s, rows, :] = dot_cols(o_all[rows, near], users_of(s, 0, near))
            return carry

        home[s, TRI:PACK, :] = dot_cols(vt_all[:, near], users_of(s, 1, near))
        lax.fori_loop(0, 2, near_step, 0)
    own_part(0)
    take(vt_all.at[:, 0:3 * items], v_recv.at[0])
    lax.fori_loop(1, 7, outer_step, 0)

    low = lax.broadcasted_iota(jnp.int32, (HALF, 128), 1) < 64
    pieces = (slice(0, CUT), slice(CUT, HALF))
    ways = (1, 3)

    def partial(s, dst, p):
        rows = pieces[p]
        for rows in (rows, slice(HALF + rows.start, min(HALF + rows.stop, TRI))):
            dst[rows, :] = home[s, rows, :] + dot_cols(o_all[rows, far], users_of(s, 0, far))
        if p:
            dst[TRI:PACK, :] = home[s, TRI:PACK, :] + dot_cols(vt_all[:, far], users_of(s, 1, far))

    def arrived(s):
        take(mqs.at[0, 0:3], m_recv.at[s])

    def pack_units(s, p):
        rows = pieces[p]
        partial(s, gram, p)
        here = low[:rows.stop - rows.start]
        top, bottom = gram[rows, :], gram[HALF + rows.start:HALF + rows.stop, :]
        unit[s, 0, rows, :] = jnp.where(here, top, pltpu.roll(bottom, 64, 1))
        unit[s, 1, rows, :] = jnp.where(here, pltpu.roll(top, 64, 1), bottom)

    arrived(0)
    for p, rows in enumerate(pieces):
        pack_units(0, p)
        for c in range(2):
            send(unit.at[0, c, rows], rel.at[c, rows], rel_send, rel_recv.at[p], z_peer(ways[c])).start()
    pass_on(1)
    start(m_copies[2])
    start(hops[3])
    own_part(1)
    pass_on(2)
    start(m_copies[3])
    own_part(2)
    arrived(1)
    for p, rows in enumerate(pieces):
        pack_units(1, p)
        take(rel.at[:, rows], rel_recv.at[p])
        for c in range(2):
            unit[1, c, rows, :] = unit[1, c, rows, :] + rel[c, rows, :]
            send(unit.at[1, c, rows], got.at[0, c, rows], got_send, got_recv.at[0], z_peer(ways[c])).start()
    pass_on(3)
    arrived(2)
    for p, rows in enumerate(pieces):
        pack_units(2, p)
        for c in range(2):
            send(
                unit.at[2, c, rows], got.at[1, c, rows], got_send, got_recv.at[1 + p], z_peer(ways[1 - c])
            ).start()
    own_part(3)
    arrived(3)
    for p in range(2):
        partial(3, tot, p)
    acc[PACK:FULL, :] = jnp.zeros((FULL - PACK, 128), jnp.float32)
    take(got.at[0], got_recv.at[0])
    pl.semaphore_wait(z_in, 3)
    for p, rows in enumerate(pieces):
        size = rows.stop - rows.start
        take(got.at[1, :, rows], got_recv.at[1 + p])
        sum_a = got[0, 0, rows] + got[1, 0, rows]
        sum_b = got[0, 1, rows] + got[1, 1, rows]
        here = low[:size]
        at = 2 * rows.start
        acc[at:at + size, :] = tot[rows, :] + jnp.where(here, sum_a, pltpu.roll(sum_b, 64, 1))
        acc[at + size:at + 2 * size, :] = (
            tot[HALF + rows.start:HALF + rows.stop, :] + jnp.where(here, pltpu.roll(sum_a, 64, 1), sum_b)
        )
        cols = slice(at, FULL if p else 2 * CUT)
        for i in range(cols.start // 128, cols.stop // 128):
            flat[:, i * 128:(i + 1) * 128] = acc[i * 128:(i + 1) * 128, :].T
        for d in (2, 1, 3):
            for c, pos in enumerate((y, x)):
                users = pl.ds(pl.multiple_of(64 * c + 16 * turn(pos, d), 16), 16)
                send(
                    flat.at[users, cols], fin.at[c, d - 1, :, cols], fin_send, fin_recv, axis_peer(1 - c, d)
                ).start()
    take(fin, fin_recv)

    zeros = jnp.zeros((96, 128), jnp.float32)
    for i in range(FULL // 128):
        cols = slice(i * 128, (i + 1) * 128)
        mine = [zeros]
        for c, pos in ((1, x), (0, y)):
            rows = pl.ds(pl.multiple_of(64 * c + 16 * pos, 16), 16)
            mine.insert(0, flat[rows, cols] + fin[c, 0, :, cols] + fin[c, 1, :, cols] + fin[c, 2, :, cols])
        acc[cols, :] = jnp.concatenate(mine, axis=0).T
    for rows in pieces:
        size = rows.stop - rows.start
        tot[rows, :] = acc[2 * rows.start:2 * rows.start + size, :]
        tot[HALF + rows.start:HALF + rows.stop, :] = acc[2 * rows.start + size:2 * rows.stop, :]
    solve_tiles(tot, tot.at[TRI:PACK], [fac], inv, sol)
    turned = jnp.concatenate([sol[...], jnp.zeros((72, 128), jnp.float32)], axis=0).T
    lane = lax.broadcasted_iota(jnp.int32, (16, 128), 1)
    pack[...] = jnp.where(lane < 64, turned[:16], pltpu.roll(turned[16:32], 64, 1)).astype(jnp.bfloat16)

    plane = SIDE * SIDE

    place = col - z * plane
    w_own = pltpu.make_async_copy(pack, w_all.at[col], w_recv.at[0])
    w_own.start()
    for t, turned_by in enumerate((0, 1, 3, 2)):
        base = turn(z, turned_by) * plane

        def send_step(i, carry):
            target = place + i
            target = base + jnp.where(target < plane, target, target - plane)
            send(pack, w_all.at[col], w_send, w_recv.at[(0, 2, 1, 3)[t]], {"col": target}).start()
            return carry

        lax.fori_loop(0 if t else 1, plane, send_step, 0)
    w_new[...] = turned[:32, :WIDTH]
    w_out = pltpu.make_async_copy(w_new, w_hbm, w_sem)
    w_out.start()

    users = 16 * count
    step = 16 * plane
    tall = tmp.at[:, 0:step]
    tall[1272:1280, :] = jnp.zeros((8, step), jnp.float32)

    def plane_step(t, carry):
        k = 3 - 2 * t + 3 * (t // 2)
        owner = turn(z, t + (t // 2) * (5 - 2 * t))

        take(w_all.at[0:plane], w_recv.at[t])
        for i in range(step // 128):
            rows = w_all[pl.ds(owner * plane + 8 * i, 8)].reshape(128, 128)
            wt[:, i * 128:(i + 1) * 128] = rows.astype(jnp.float32).T

        def colour_step(c, carry):
            vals = wt[pl.ds(pl.multiple_of(64 * c, 64), 64), :]
            cols = pl.ds(pl.multiple_of(c * users + k * step, step), step)
            wb[:, cols] = vals.astype(jnp.bfloat16)
            outer_tile(vals, tall)
            o_all[:, cols] = tall[...].astype(jnp.bfloat16)
            return carry

        lax.fori_loop(0, 2, colour_step, 0)
        return carry

    lax.fori_loop(0, SIDE, plane_step, 0)
    half = items // 2

    def item_rows(side, left, m):
        cols = pl.ds(pl.multiple_of(side * half, half), half)
        total = None
        for c in range(2):
            right = mqs[:, :, :, c, m, :, cols].reshape(users, half)
            term = jnp.dot(left(c), right, preferred_element_type=jnp.float32)
            total = term if total is None else total + term
        return total

    def rhs_rows(side):
        return item_rows(side, lambda c: wb[:, c * users:(c + 1) * users], 1)

    def gram_rows(side, rows):
        return item_rows(side, lambda c: o_all[rows, c * users:(c + 1) * users], 0)

    def swap_copy(i, rows):
        return send(part.at[rows], swap_got.at[rows], x_send, x_recv.at[i], other)

    def finish(i, rows, val):
        swap_copy(i, rows).wait_recv()
        item_sum[rows, :] = val + swap_got[rows, :]
        pltpu.make_async_copy(item_sum.at[rows], item_hbm.at[rows], out_sem).start()

    tail = pl.ds(TRI, PACK - TRI)
    part[tail, :] = rhs_rows(1 - row)
    swap_copy(2, tail).start()

    def away_step(i, carry):
        rows = pl.ds(pl.multiple_of(i * 640, 640), 640)
        part[rows, :] = gram_rows(1 - row, rows)
        swap_copy(i, rows).start()
        return carry

    def home_step(i, carry):
        rows = pl.ds(pl.multiple_of(i * 640, 640), 640)
        finish(i, rows, gram_rows(row, rows))
        return carry

    lax.fori_loop(0, 2, away_step, 0)
    finish(2, tail, rhs_rows(row))
    lax.fori_loop(0, 2, home_step, 0)
    w_out.wait()
    take(part, out_sem)
    take(vt_all.at[:, 0:3 * items], v_send.at[0])
    take(vt_all.at[:, 0:3 * items], v_send.at[1])
    take(mqs.at[0:2], m_send)
    take(hop, hop_send)
    take(hop, fwd_send)
    take(rel, rel_send)
    take(got, got_send)
    take(fin, fin_send)
    take(w_all.at[0:count - 1], w_send)
    take(part, x_send)


def half_steps(ratings, mask, vt, count):
    users, items = ratings.shape
    block = users // SIDE
    dma = pltpu.SemaphoreType.DMA
    any_spec = pl.BlockSpec(memory_space=pl.ANY)
    f32, bf16 = jnp.float32, jnp.bfloat16
    return pl.pallas_call(
        als_kernel,
        out_shape=(
            jax.ShapeDtypeStruct((32, WIDTH), f32),
            jax.ShapeDtypeStruct((PACK, items // 2), f32),
        ),
        in_specs=[any_spec, any_spec, any_spec],
        out_specs=(any_spec, any_spec),
        scratch_shapes=[
            pltpu.VMEM((4, block, items), f32),
            pltpu.VMEM((4, block, items), jnp.int32),
            pltpu.VMEM((WIDTH, items), f32),
            pltpu.VMEM((4, SIDE, SIDE, 2, 2, 16, items), bf16),
            pltpu.VMEM((4, 2, 2, SIDE, 16, items), bf16),
            pltpu.VMEM((4, 2, SIDE, 2, 16, 7 * items), bf16),
            pltpu.VMEM((64, 7 * items), bf16),
            pltpu.VMEM((TRI, 7 * items), bf16),
            pltpu.VMEM((TRI, items), f32),
            pltpu.VMEM((PACK, 128), f32),
            pltpu.VMEM((4, PACK, 128), f32),
            pltpu.VMEM((3, 2, HALF, 128), f32),
            pltpu.VMEM((2, HALF, 128), f32),
            pltpu.VMEM((2, 2, HALF, 128), f32),
            pltpu.VMEM((PACK, 128), f32),
            pltpu.VMEM((FULL, 128), f32),
            pltpu.VMEM((128, FULL), f32),
            pltpu.VMEM((2, 3, 16, FULL), f32),
            pltpu.VMEM((WIDTH * ROWS, 128), f32),
            pltpu.VMEM((ROWS, 128), f32),
            pltpu.VMEM((ROWS, 128), f32),
            pltpu.VMEM((32, WIDTH), f32),
            pltpu.VMEM((16, 128), bf16),
            pltpu.VMEM((count, 16, 128), bf16),
            pltpu.VMEM((128, 16 * SIDE * SIDE), f32),
            pltpu.VMEM((64, 32 * count), bf16),
            pltpu.VMEM((PACK, items // 2), f32),
            pltpu.VMEM((PACK, items // 2), f32),
            pltpu.VMEM((PACK, items // 2), f32),
            dma, dma((4,)), dma((2,)), dma((4,)), dma, dma((4,)), dma, dma((4,)), dma, dma((4,)),
            dma, dma((2,)), dma, dma((3,)), dma, dma, dma, dma((4,)), dma, dma, dma((3,)), dma,
            pltpu.SemaphoreType.REGULAR, pltpu.SemaphoreType.REGULAR,
        ],
        compiler_params=pltpu.CompilerParams(
            collective_id=0, has_side_effects=True, vmem_limit_bytes=60 * 1024 * 1024
        ),
    )(ratings, mask, vt)


def solution(mesh):
    block_spec = P(("part", "row"), "col")
    in_specs = (block_spec, block_spec, P(("part", "col"), None))
    out_specs = (P(("part", "row", "col"), None), P(("part", "col", "row"), None))
    count = mesh.shape["col"]

    def local_als(ratings, mask, v_init):
        w_own, packed = half_steps(ratings, mask, v_init.T, count)
        v_own, w_own = solve_items(packed, w_own)
        return w_own, v_own.T

    return jax.shard_map(local_als, mesh=mesh, in_specs=in_specs, out_specs=out_specs, check_vma=False)
```

```python
import jax
import jax.numpy as jnp
from jax import lax
from jax.experimental import pallas as pl
from jax.experimental.pallas import tpu as pltpu
from jax.sharding import PartitionSpec as P

RIDGE_WEIGHT = 0.05
WIDTH = 50
ROWS = 56
TRI = 1280
LANES = 128


def tri_off(j):
    return j * WIDTH - j * (j - 1) // 2


def outer_tile(vt, dst):
    lanes = vt.shape[1]
    for j in range(WIDTH):
        rows = WIDTH - j
        dst[tri_off(j):tri_off(j) + rows, :] = vt[j:WIDTH, :] * vt[j:j + 1, :]


def solve_tiles(g_ref, rhs_ref, facs, inv, sol, ready=None):
    groups = [slice(i * LANES, (i + 1) * LANES) for i in range(len(facs))]
    for pan in range(7):
        first = 8 * pan
        rows = ROWS - first
        count = min(8, WIDTH - first)
        if ready is not None:
            ready(pan)
        ids = lax.broadcasted_iota(jnp.int32, (rows, LANES), 0)

        def panel(here):
            accs = []
            for c in range(count):
                j = first + c
                start = tri_off(j) - c
                if j < WIDTH - 1:
                    raw = g_ref[start:start + rows, here]
                else:
                    raw = jnp.broadcast_to(g_ref[tri_off(j):tri_off(j) + 1, here], (rows, LANES))
                col = jnp.where(ids < WIDTH - first, raw, 0.0)
                col = jnp.where(ids == c, col + RIDGE_WEIGHT, col)
                accs.append(jnp.where(ids == WIDTH - first, rhs_ref[j:j + 1, here], col))
            return accs

        def update(fac, k, accs):
            base = pl.multiple_of(k * ROWS, 8)
            left = fac[pl.ds(base + first, rows), :]
            return [acc - left * fac[pl.ds(base + first + c, 1), :] for c, acc in enumerate(accs)]

        if not pan:
            parts = [panel(here) for here in groups]
        elif len(groups) * count * rows <= 48 * 8:
            parts = lax.fori_loop(
                0, first, lambda k, parts: [update(fac, k, accs) for fac, accs in zip(facs, parts)],
                [panel(here) for here in groups], unroll=4,
            )
        else:
            parts = []
            for here, fac in zip(groups, facs):
                parts.append(lax.fori_loop(0, first, lambda k, accs: update(fac, k, accs), panel(here), unroll=4))
        parts = [list(accs) for accs in parts]
        for c in range(count):
            j = first + c
            for here, fac, accs in zip(groups, facs, parts):
                diag = accs[c][c:c + 1, :]
                root = lax.rsqrt(diag)
                root = root * (1.5 - 0.5 * (diag * root) * root)
                inv[j:j + 1, here] = root
                col = accs[c] * root
                fac[pl.ds(j * ROWS + first, rows), :] = col
                for later in range(c + 1, count):
                    accs[later] = accs[later] - col * col[later:later + 1, :]
    for here in groups:
        sol[48:56, here] = jnp.zeros((8, LANES), jnp.float32)
    for pan in reversed(range(7)):
        first = 8 * pan
        count = min(8, WIDTH - first)
        lefts = []
        for here, fac in zip(groups, facs):
            left = []
            for c in range(count):
                j = first + c
                val = fac[j * ROWS + WIDTH:j * ROWS + WIDTH + 1, :]
                if pan < 6:
                    dot = fac[j * ROWS + first + 8:j * ROWS + ROWS, :] * sol[first + 8:ROWS, here]
                    val = val - jnp.sum(dot, axis=0, keepdims=True)
                left.append(val)
            lefts.append(left)
        for c in reversed(range(count)):
            j = first + c
            for here, fac, left in zip(groups, facs, lefts):
                got = left[c] * inv[j:j + 1, here]
                sol[j:j + 1, here] = got
                for early in range(c):
                    row = (first + early) * ROWS + j
                    left[early] = left[early] - fac[row:row + 1, :] * got


def item_solve_kernel(g_hbm, w_ref, out_ref, w_out, gram, inv, sol, sems, *facs):
    copies = []
    for i, (start, stop) in enumerate(((0, 384), (TRI, gram.shape[0]), (384, 688), (688, TRI))):
        copy = pltpu.make_async_copy(g_hbm.at[start:stop], gram.at[start:stop], sems.at[i])
        copy.start()
        copies.append(copy)
    w_out[...] = w_ref[...]

    def ready(pan):
        for copy in (copies[:2], copies[2:3], copies[3:], [], [], [], [])[pan]:
            copy.wait()

    solve_tiles(gram, gram.at[TRI:gram.shape[0]], facs, inv, sol, ready)
    out_ref[...] = sol[:WIDTH, :]


def solve_items(packed, w_own):
    n = packed.shape[1]
    vmem_spec = pl.BlockSpec(memory_space=pltpu.VMEM)
    return pl.pallas_call(
        item_solve_kernel,
        out_shape=(jax.ShapeDtypeStruct((WIDTH, n), jnp.float32), jax.ShapeDtypeStruct(w_own.shape, jnp.float32)),
        in_specs=[pl.BlockSpec(memory_space=pl.ANY), vmem_spec],
        out_specs=(vmem_spec, vmem_spec),
        scratch_shapes=[
            pltpu.VMEM(packed.shape, jnp.float32),
            pltpu.VMEM((ROWS, n), jnp.float32),
            pltpu.VMEM((ROWS, n), jnp.float32),
            pltpu.SemaphoreType.DMA((4,)),
        ] + [pltpu.VMEM((WIDTH * ROWS, LANES), jnp.float32)] * (n // LANES),
    )(packed, w_own)


PACK = 1344
FULL = 1408
SIDE = 4
HALF = PACK // 2
CUT = 384


def dot_cols(left, right):
    return lax.dot_general(left, right, (((1,), (1,)), ((), ())), preferred_element_type=jnp.float32)


def als_kernel(
    rate_hbm, mask_hbm, v_hbm, w_hbm, item_hbm,
    rate, mask, v_raw, mqs, hop, rhs, vt_all, o_all, tmp, gram, home, unit, rel, got, tot, acc, flat, fin,
    fac, inv, sol, w_new, pack, w_all, wt, wb, part, swap_got, item_sum,
    v_sem, load_sem, v_send, v_recv, m_send, m_recv, hop_send, hop_recv, fwd_send, own_sem,
    rel_send, rel_recv, got_send, got_recv, fin_send, fin_recv, w_send, w_recv, w_sem, x_send, x_recv, out_sem, y_in, z_in,
):
    items = v_raw.shape[1]
    count = w_all.shape[0]
    col = lax.axis_index("col")
    row = lax.axis_index("row")
    other = {"row": 1 - row}
    x = lax.rem(col, SIDE)
    y = lax.rem(col // SIDE, SIDE)
    z = col // (SIDE * SIDE)

    def turn(pos, step):
        return lax.rem(pos + step, SIDE)

    def x_peer(step):
        return {"col": col - x + turn(x, step)}

    def y_peer(step):
        return {"col": col + SIDE * (turn(y, step) - y)}

    def z_peer(step):
        return {"col": col + SIDE * SIDE * (turn(z, step) - z)}

    def send(src, dst, send_sem, recv_sem, peer):
        return pltpu.make_async_remote_copy(
            src_ref=src, dst_ref=dst, send_sem=send_sem, recv_sem=recv_sem,
            device_id=peer, device_id_type=pl.DeviceIdType.MESH,
        )

    def signal(sem, peer):
        pl.semaphore_signal(sem, inc=1, device_id=peer, device_id_type=pl.DeviceIdType.MESH)

    def start(copies):
        for copy in copies:
            copy.start()

    def take(ref, sem):
        pltpu.make_async_copy(ref, ref, sem).wait()

    barrier = pltpu.get_barrier_semaphore()
    peers = [peer(step) for step in (1, 2, 3) for peer in (x_peer, y_peer, z_peer)] + [other]
    for peer in peers:
        signal(barrier, peer)

    owners = [turn(z, 2), turn(z, 1), turn(z, 3), z]
    block = rate.shape[1]
    v_load = pltpu.make_async_copy(v_hbm, v_raw, v_sem)
    v_load.start()
    loads = []
    for k, owner in enumerate(owners):
        rows = pl.ds(pl.multiple_of(owner * block, block), block)
        pair = [
            pltpu.make_async_copy(rate_hbm.at[rows], rate.at[k], load_sem.at[k]),
            pltpu.make_async_copy(mask_hbm.at[rows], mask.at[k], load_sem.at[k]),
        ]
        loads.append(pair)
    start(loads[0])

    def cast_chunk(k):
        def cast_step(i, carry):
            rows = pl.ds(pl.multiple_of(i * 128, 128), 128)
            seen = mask[k, rows, :]
            mqs[k, i, :, :, 0] = seen.astype(jnp.float32).astype(jnp.bfloat16).reshape(SIDE, 2, 16, items)
            rated = jnp.where(seen != 0, rate[k, rows, :], 0.0)
            mqs[k, i, :, :, 1] = rated.astype(jnp.bfloat16).reshape(SIDE, 2, 16, items)
            return carry

        lax.fori_loop(0, SIDE, cast_step, 0)

    def axis_peer(c, step):
        return y_peer(step) if c else x_peer(step)

    def share(s, c, pos):
        return mqs.at[(0, 2, 1, 3)[s], pos, :, 1] if c else mqs.at[s, :, pos, 0]

    def columns(slot):
        return slice(slot * items, (slot + 1) * items)

    m_copies, own_copies, hops, passes = [], [], [], []
    for s in range(4):
        m_copies.append([])
        own_copies.append([])
        hops.append([])
        passes.append([])
        for c, pos in enumerate((x, y)):
            for m, step in enumerate((1, 3)):
                hops[s].append(send(
                    share(s, c, turn(pos, 2)).at[:, m], hop.at[s, c, m],
                    hop_send, hop_recv.at[s], axis_peer(c, step),
                ))
                m_copies[s].append(send(
                    share(s, c, turn(pos, step)), rhs.at[s, c, :, :, :, columns(3 * c + step)],
                    m_send, m_recv.at[s], axis_peer(c, step),
                ))
                passes[s].append(send(
                    hop.at[s, c, m], rhs.at[s, c, :, m, :, columns(3 * c + 2)],
                    fwd_send, m_recv.at[s], axis_peer(c, step),
                ))
            own_copies[s].append(pltpu.make_async_copy(
                share(s, c, pos), rhs.at[s, c, :, :, :, columns(0)], own_sem.at[s]
            ))

    def pass_on(s):
        take(hop.at[s], hop_recv.at[s])
        start(passes[s])

    def half_columns(slot, side):
        return pl.ds(pl.multiple_of(slot * items + side * (items // 2), items // 2), items // 2)

    v_copies, v_swaps = [], []
    for d in (1, 3, 2):
        for axis in range(2):
            slot = 3 * axis + d
            v_copies.append(send(
                vt_all.at[:, half_columns(0, row)], vt_all.at[:, half_columns(slot, row)],
                v_send.at[0], v_recv.at[d], axis_peer(axis, d),
            ))
            v_swaps.append(send(
                vt_all.at[:, half_columns(slot, row)], vt_all.at[:, half_columns(slot, row)],
                v_send.at[1], v_recv.at[0], other,
            ))

    tmp[48:64, :] = jnp.zeros((16, items), jnp.float32)
    v_load.wait()
    tmp[0:WIDTH, :] = v_raw[...]
    vt_all[:, 0:items] = tmp[0:64, :].astype(jnp.bfloat16)
    take(rate.at[0:2], load_sem.at[0])
    for k in range(1, 4):
        start(loads[k])
    cast_chunk(0)
    pl.semaphore_wait(barrier, len(peers))
    start(v_copies)
    start(hops[0])
    start(m_copies[0])
    for step in (1, 2, 3):
        signal(y_in, y_peer(step))
    for k in range(1, 4):
        take(rate.at[0:2], load_sem.at[k])
        cast_chunk(k)
    for s in range(4):
        start(own_copies[s])
    for s in range(4):
        rhs[s, 0, :, :, :, 4 * items:7 * items] = jnp.zeros((4, 2, 16, 3 * items), jnp.bfloat16)
        rhs[s, 1, :, :, :, items:4 * items] = jnp.zeros((4, 2, 16, 3 * items), jnp.bfloat16)
    tmp[1272:1280, :] = jnp.zeros((8, items), jnp.float32)

    def outer_step(slot, carry):
        cols = pl.ds(pl.multiple_of(slot * items, items), items)
        outer_tile(vt_all[:, cols].astype(jnp.float32), tmp)
        o_all[:, cols] = tmp[...].astype(jnp.bfloat16)
        return carry

    lax.fori_loop(0, 1, outer_step, 0)
    for i, d in enumerate((1, 3, 2)):
        take(vt_all.at[:, 0:items], v_recv.at[d])
        start(v_swaps[2 * i:2 * i + 2])
    pass_on(0)
    start(hops[1])
    start(m_copies[1])
    start(hops[2])
    pl.semaphore_wait(y_in, 3)
    for step in (1, 2, 3):
        signal(z_in, z_peer(step))

    def users_of(s, m, cols):
        return rhs[s, :, :, m, :, cols].reshape(128, cols.stop - cols.start)

    near, far = slice(0, items), slice(items, 7 * items)
    def own_part(s):
        take(hop.at[s], own_sem.at[s])

        def near_step(i, carry):
            rows = pl.ds(pl.multiple_of(i * 640, 640), 640)
            home[s, rows, :] = dot_cols(o_all[rows, near], users_of(s, 0, near))
            return carry

        home[s, TRI:PACK, :] = dot_cols(vt_all[:, near], users_of(s, 1, near))
        lax.fori_loop(0, 2, near_step, 0)
    own_part(0)
    take(vt_all.at[:, 0:3 * items], v_recv.at[0])
    lax.fori_loop(1, 7, outer_step, 0)

    low = lax.broadcasted_iota(jnp.int32, (HALF, 128), 1) < 64
    pieces = (slice(0, CUT), slice(CUT, HALF))
    ways = (1, 3)

    def partial(s, dst, p):
        rows = pieces[p]
        for rows in (rows, slice(HALF + rows.start, min(HALF + rows.stop, TRI))):
            dst[rows, :] = home[s, rows, :] + dot_cols(o_all[rows, far], users_of(s, 0, far))
        if p:
            dst[TRI:PACK, :] = home[s, TRI:PACK, :] + dot_cols(vt_all[:, far], users_of(s, 1, far))

    def arrived(s):
        take(mqs.at[0, 0:3], m_recv.at[s])

    def pack_units(s, p):
        rows = pieces[p]
        partial(s, gram, p)
        here = low[:rows.stop - rows.start]
        top, bottom = gram[rows, :], gram[HALF + rows.start:HALF + rows.stop, :]
        unit[s, 0, rows, :] = jnp.where(here, top, pltpu.roll(bottom, 64, 1))
        unit[s, 1, rows, :] = jnp.where(here, pltpu.roll(top, 64, 1), bottom)

    arrived(0)
    for p, rows in enumerate(pieces):
        pack_units(0, p)
        for c in range(2):
            send(unit.at[0, c, rows], rel.at[c, rows], rel_send, rel_recv.at[p], z_peer(ways[c])).start()
    pass_on(1)
    start(m_copies[2])
    start(hops[3])
    own_part(1)
    pass_on(2)
    start(m_copies[3])
    own_part(2)
    arrived(1)
    for p, rows in enumerate(pieces):
        pack_units(1, p)
        take(rel.at[:, rows], rel_recv.at[p])
        for c in range(2):
            unit[1, c, rows, :] = unit[1, c, rows, :] + rel[c, rows, :]
            send(unit.at[1, c, rows], got.at[0, c, rows], got_send, got_recv.at[0], z_peer(ways[c])).start()
    pass_on(3)
    arrived(2)
    for p, rows in enumerate(pieces):
        pack_units(2, p)
        for c in range(2):
            send(
                unit.at[2, c, rows], got.at[1, c, rows], got_send, got_recv.at[1 + p], z_peer(ways[1 - c])
            ).start()
    own_part(3)
    arrived(3)
    for p in range(2):
        partial(3, tot, p)
    acc[PACK:FULL, :] = jnp.zeros((FULL - PACK, 128), jnp.float32)
    take(got.at[0], got_recv.at[0])
    pl.semaphore_wait(z_in, 3)
    for p, rows in enumerate(pieces):
        size = rows.stop - rows.start
        take(got.at[1, :, rows], got_recv.at[1 + p])
        sum_a = got[0, 0, rows] + got[1, 0, rows]
        sum_b = got[0, 1, rows] + got[1, 1, rows]
        here = low[:size]
        at = 2 * rows.start
        acc[at:at + size, :] = tot[rows, :] + jnp.where(here, sum_a, pltpu.roll(sum_b, 64, 1))
        acc[at + size:at + 2 * size, :] = (
            tot[HALF + rows.start:HALF + rows.stop, :] + jnp.where(here, pltpu.roll(sum_a, 64, 1), sum_b)
        )
        cols = slice(at, FULL if p else 2 * CUT)
        for i in range(cols.start // 128, cols.stop // 128):
            flat[:, i * 128:(i + 1) * 128] = acc[i * 128:(i + 1) * 128, :].T
        for d in (2, 1, 3):
            for c, pos in enumerate((y, x)):
                users = pl.ds(pl.multiple_of(64 * c + 16 * turn(pos, d), 16), 16)
                send(
                    flat.at[users, cols], fin.at[c, d - 1, :, cols], fin_send, fin_recv, axis_peer(1 - c, d)
                ).start()
    take(fin, fin_recv)

    zeros = jnp.zeros((96, 128), jnp.float32)
    for i in range(FULL // 128):
        cols = slice(i * 128, (i + 1) * 128)
        mine = [zeros]
        for c, pos in ((1, x), (0, y)):
            rows = pl.ds(pl.multiple_of(64 * c + 16 * pos, 16), 16)
            mine.insert(0, flat[rows, cols] + fin[c, 0, :, cols] + fin[c, 1, :, cols] + fin[c, 2, :, cols])
        acc[cols, :] = jnp.concatenate(mine, axis=0).T
    for rows in pieces:
        size = rows.stop - rows.start
        tot[rows, :] = acc[2 * rows.start:2 * rows.start + size, :]
        tot[HALF + rows.start:HALF + rows.stop, :] = acc[2 * rows.start + size:2 * rows.stop, :]
    solve_tiles(tot, tot.at[TRI:PACK], [fac], inv, sol)
    turned = jnp.concatenate([sol[...], jnp.zeros((72, 128), jnp.float32)], axis=0).T
    lane = lax.broadcasted_iota(jnp.int32, (16, 128), 1)
    pack[...] = jnp.where(lane < 64, turned[:16], pltpu.roll(turned[16:32], 64, 1)).astype(jnp.bfloat16)

    plane = SIDE * SIDE

    place = col - z * plane
    w_own = pltpu.make_async_copy(pack, w_all.at[col], w_recv.at[0])
    w_own.start()
    for t, turned_by in enumerate((0, 1, 3, 2)):
        base = turn(z, turned_by) * plane

        def send_step(i, carry):
            target = place + i
            target = base + jnp.where(target < plane, target, target - plane)
            send(pack, w_all.at[col], w_send, w_recv.at[(0, 2, 1, 3)[t]], {"col": target}).start()
            return carry

        lax.fori_loop(0 if t else 1, plane, send_step, 0)
    w_new[...] = turned[:32, :WIDTH]
    w_out = pltpu.make_async_copy(w_new, w_hbm, w_sem)
    w_out.start()

    users = 16 * count
    step = 16 * plane
    tall = tmp.at[:, 0:step]
    tall[1272:1280, :] = jnp.zeros((8, step), jnp.float32)

    def plane_step(t, carry):
        k = 3 - 2 * t + 3 * (t // 2)
        owner = turn(z, t + (t // 2) * (5 - 2 * t))

        take(w_all.at[0:plane], w_recv.at[t])
        for i in range(step // 128):
            rows = w_all[pl.ds(owner * plane + 8 * i, 8)].reshape(128, 128)
            wt[:, i * 128:(i + 1) * 128] = rows.astype(jnp.float32).T

        def colour_step(c, carry):
            vals = wt[pl.ds(pl.multiple_of(64 * c, 64), 64), :]
            cols = pl.ds(pl.multiple_of(c * users + k * step, step), step)
            wb[:, cols] = vals.astype(jnp.bfloat16)
            outer_tile(vals, tall)
            o_all[:, cols] = tall[...].astype(jnp.bfloat16)
            return carry

        lax.fori_loop(0, 2, colour_step, 0)
        return carry

    lax.fori_loop(0, SIDE, plane_step, 0)
    half = items // 2

    def item_rows(side, left, m):
        cols = pl.ds(pl.multiple_of(side * half, half), half)
        total = None
        for c in range(2):
            right = mqs[:, :, :, c, m, :, cols].reshape(users, half)
            term = jnp.dot(left(c), right, preferred_element_type=jnp.float32)
            total = term if total is None else total + term
        return total

    def rhs_rows(side):
        return item_rows(side, lambda c: wb[:, c * users:(c + 1) * users], 1)

    def gram_rows(side, rows):
        return item_rows(side, lambda c: o_all[rows, c * users:(c + 1) * users], 0)

    def swap_copy(i, rows):
        return send(part.at[rows], swap_got.at[rows], x_send, x_recv.at[i], other)

    def finish(i, rows, val):
        swap_copy(i, rows).wait_recv()
        item_sum[rows, :] = val + swap_got[rows, :]
        pltpu.make_async_copy(item_sum.at[rows], item_hbm.at[rows], out_sem).start()

    tail = pl.ds(TRI, PACK - TRI)
    part[tail, :] = rhs_rows(1 - row)
    swap_copy(2, tail).start()

    def away_step(i, carry):
        rows = pl.ds(pl.multiple_of(i * 640, 640), 640)
        part[rows, :] = gram_rows(1 - row, rows)
        swap_copy(i, rows).start()
        return carry

    def home_step(i, carry):
        rows = pl.ds(pl.multiple_of(i * 640, 640), 640)
        finish(i, rows, gram_rows(row, rows))
        return carry

    lax.fori_loop(0, 2, away_step, 0)
    finish(2, tail, rhs_rows(row))
    lax.fori_loop(0, 2, home_step, 0)
    w_out.wait()
    take(part, out_sem)
    take(vt_all.at[:, 0:3 * items], v_send.at[0])
    take(vt_all.at[:, 0:3 * items], v_send.at[1])
    take(mqs.at[0:2], m_send)
    take(hop, hop_send)
    take(hop, fwd_send)
    take(rel, rel_send)
    take(got, got_send)
    take(fin, fin_send)
    take(w_all.at[0:count - 1], w_send)
    take(part, x_send)


def half_steps(ratings, mask, vt, count):
    users, items = ratings.shape
    block = users // SIDE
    dma = pltpu.SemaphoreType.DMA
    any_spec = pl.BlockSpec(memory_space=pl.ANY)
    f32, bf16 = jnp.float32, jnp.bfloat16
    return pl.pallas_call(
        als_kernel,
        out_shape=(
            jax.ShapeDtypeStruct((32, WIDTH), f32),
            jax.ShapeDtypeStruct((PACK, items // 2), f32),
        ),
        in_specs=[any_spec, any_spec, any_spec],
        out_specs=(any_spec, any_spec),
        scratch_shapes=[
            pltpu.VMEM((4, block, items), f32),
            pltpu.VMEM((4, block, items), jnp.int32),
            pltpu.VMEM((WIDTH, items), f32),
            pltpu.VMEM((4, SIDE, SIDE, 2, 2, 16, items), bf16),
            pltpu.VMEM((4, 2, 2, SIDE, 16, items), bf16),
            pltpu.VMEM((4, 2, SIDE, 2, 16, 7 * items), bf16),
            pltpu.VMEM((64, 7 * items), bf16),
            pltpu.VMEM((TRI, 7 * items), bf16),
            pltpu.VMEM((TRI, items), f32),
            pltpu.VMEM((PACK, 128), f32),
            pltpu.VMEM((4, PACK, 128), f32),
            pltpu.VMEM((3, 2, HALF, 128), f32),
            pltpu.VMEM((2, HALF, 128), f32),
            pltpu.VMEM((2, 2, HALF, 128), f32),
            pltpu.VMEM((PACK, 128), f32),
            pltpu.VMEM((FULL, 128), f32),
            pltpu.VMEM((128, FULL), f32),
            pltpu.VMEM((2, 3, 16, FULL), f32),
            pltpu.VMEM((WIDTH * ROWS, 128), f32),
            pltpu.VMEM((ROWS, 128), f32),
            pltpu.VMEM((ROWS, 128), f32),
            pltpu.VMEM((32, WIDTH), f32),
            pltpu.VMEM((16, 128), bf16),
            pltpu.VMEM((count, 16, 128), bf16),
            pltpu.VMEM((128, 16 * SIDE * SIDE), f32),
            pltpu.VMEM((64, 32 * count), bf16),
            pltpu.VMEM((PACK, items // 2), f32),
            pltpu.VMEM((PACK, items // 2), f32),
            pltpu.VMEM((PACK, items // 2), f32),
            dma, dma((4,)), dma((2,)), dma((4,)), dma, dma((4,)), dma, dma((4,)), dma, dma((4,)),
            dma, dma((2,)), dma, dma((3,)), dma, dma, dma, dma((4,)), dma, dma, dma((3,)), dma,
            pltpu.SemaphoreType.REGULAR, pltpu.SemaphoreType.REGULAR,
        ],
        compiler_params=pltpu.CompilerParams(
            collective_id=0, has_side_effects=True, vmem_limit_bytes=60 * 1024 * 1024
        ),
    )(ratings, mask, vt)


def solution(mesh):
    block_spec = P(("part", "row"), "col")
    in_specs = (block_spec, block_spec, P(("part", "col"), None))
    out_specs = (P(("part", "row", "col"), None), P(("part", "col", "row"), None))
    count = mesh.shape["col"]

    def local_als(ratings, mask, v_init):
        w_own, packed = half_steps(ratings, mask, v_init.T, count)
        v_own, w_own = solve_items(packed, w_own)
        return w_own, v_own.T

    return jax.shard_map(local_als, mesh=mesh, in_specs=in_specs, out_specs=out_specs, check_vma=False)
```

```python
import jax
import jax.numpy as jnp
from jax import lax
from jax.experimental import pallas as pl
from jax.experimental.pallas import tpu as pltpu
from jax.sharding import PartitionSpec as P

RIDGE_WEIGHT = 0.05
WIDTH = 50
ROWS = 56
TRI = 1280
LANES = 128


def tri_off(j):
    return j * WIDTH - j * (j - 1) // 2


def outer_tile(vt, dst):
    lanes = vt.shape[1]
    for j in range(WIDTH):
        rows = WIDTH - j
        dst[tri_off(j):tri_off(j) + rows, :] = vt[j:WIDTH, :] * vt[j:j + 1, :]


def solve_tiles(g_ref, rhs_ref, facs, inv, sol, ready=None):
    groups = [slice(i * LANES, (i + 1) * LANES) for i in range(len(facs))]
    for pan in range(7):
        first = 8 * pan
        rows = ROWS - first
        count = min(8, WIDTH - first)
        if ready is not None:
            ready(pan)
        ids = lax.broadcasted_iota(jnp.int32, (rows, LANES), 0)

        def panel(here):
            accs = []
            for c in range(count):
                j = first + c
                start = tri_off(j) - c
                if j < WIDTH - 1:
                    raw = g_ref[start:start + rows, here]
                else:
                    raw = jnp.broadcast_to(g_ref[tri_off(j):tri_off(j) + 1, here], (rows, LANES))
                col = jnp.where(ids < WIDTH - first, raw, 0.0)
                col = jnp.where(ids == c, col + RIDGE_WEIGHT, col)
                accs.append(jnp.where(ids == WIDTH - first, rhs_ref[j:j + 1, here], col))
            return accs

        def update(fac, k, accs):
            base = pl.multiple_of(k * ROWS, 8)
            left = fac[pl.ds(base + first, rows), :]
            return [acc - left * fac[pl.ds(base + first + c, 1), :] for c, acc in enumerate(accs)]

        if not pan:
            parts = [panel(here) for here in groups]
        elif len(groups) * count * rows <= 48 * 8:
            parts = lax.fori_loop(
                0, first, lambda k, parts: [update(fac, k, accs) for fac, accs in zip(facs, parts)],
                [panel(here) for here in groups], unroll=8,
            )
        else:
            parts = []
            for here, fac in zip(groups, facs):
                parts.append(lax.fori_loop(0, first, lambda k, accs: update(fac, k, accs), panel(here), unroll=8))
        parts = [list(accs) for accs in parts]
        for c in range(count):
            j = first + c
            for here, fac, accs in zip(groups, facs, parts):
                diag = accs[c][c:c + 1, :]
                root = lax.rsqrt(diag)
                root = root * (1.5 - 0.5 * (diag * root) * root)
                inv[j:j + 1, here] = root
                col = accs[c] * root
                fac[pl.ds(j * ROWS + first, rows), :] = col
                for later in range(c + 1, count):
                    accs[later] = accs[later] - col * col[later:later + 1, :]
    for here in groups:
        sol[48:56, here] = jnp.zeros((8, LANES), jnp.float32)
    for pan in reversed(range(7)):
        first = 8 * pan
        count = min(8, WIDTH - first)
        lefts = []
        for here, fac in zip(groups, facs):
            left = []
            for c in range(count):
                j = first + c
                val = fac[j * ROWS + WIDTH:j * ROWS + WIDTH + 1, :]
                if pan < 6:
                    dot = fac[j * ROWS + first + 8:j * ROWS + ROWS, :] * sol[first + 8:ROWS, here]
                    val = val - jnp.sum(dot, axis=0, keepdims=True)
                left.append(val)
            lefts.append(left)
        for c in reversed(range(count)):
            j = first + c
            for here, fac, left in zip(groups, facs, lefts):
                got = left[c] * inv[j:j + 1, here]
                sol[j:j + 1, here] = got
                for early in range(c):
                    row = (first + early) * ROWS + j
                    left[early] = left[early] - fac[row:row + 1, :] * got


def item_solve_kernel(g_hbm, w_ref, out_ref, w_out, gram, inv, sol, sems, *facs):
    copies = []
    for i, (start, stop) in enumerate(((0, 384), (TRI, gram.shape[0]), (384, 688), (688, TRI))):
        copy = pltpu.make_async_copy(g_hbm.at[start:stop], gram.at[start:stop], sems.at[i])
        copy.start()
        copies.append(copy)
    w_out[...] = w_ref[...]

    def ready(pan):
        for copy in (copies[:2], copies[2:3], copies[3:], [], [], [], [])[pan]:
            copy.wait()

    solve_tiles(gram, gram.at[TRI:gram.shape[0]], facs, inv, sol, ready)
    out_ref[...] = sol[:WIDTH, :]


def solve_items(packed, w_own):
    n = packed.shape[1]
    vmem_spec = pl.BlockSpec(memory_space=pltpu.VMEM)
    return pl.pallas_call(
        item_solve_kernel,
        out_shape=(jax.ShapeDtypeStruct((WIDTH, n), jnp.float32), jax.ShapeDtypeStruct(w_own.shape, jnp.float32)),
        in_specs=[pl.BlockSpec(memory_space=pl.ANY), vmem_spec],
        out_specs=(vmem_spec, vmem_spec),
        scratch_shapes=[
            pltpu.VMEM(packed.shape, jnp.float32),
            pltpu.VMEM((ROWS, n), jnp.float32),
            pltpu.VMEM((ROWS, n), jnp.float32),
            pltpu.SemaphoreType.DMA((4,)),
        ] + [pltpu.VMEM((WIDTH * ROWS, LANES), jnp.float32)] * (n // LANES),
    )(packed, w_own)


PACK = 1344
FULL = 1408
SIDE = 4
HALF = PACK // 2
CUT = 384


def dot_cols(left, right):
    return lax.dot_general(left, right, (((1,), (1,)), ((), ())), preferred_element_type=jnp.float32)


def als_kernel(
    rate_hbm, mask_hbm, v_hbm, w_hbm, item_hbm,
    rate, mask, v_raw, mqs, hop, rhs, vt_all, o_all, tmp, gram, home, unit, rel, got, tot, acc, flat, fin,
    fac, inv, sol, w_new, pack, w_all, wt, wb, part, swap_got, item_sum,
    v_sem, load_sem, v_send, v_recv, m_send, m_recv, hop_send, hop_recv, fwd_send, own_sem,
    rel_send, rel_recv, got_send, got_recv, fin_send, fin_recv, w_send, w_recv, w_sem, x_send, x_recv, out_sem, y_in, z_in,
):
    items = v_raw.shape[1]
    count = w_all.shape[0]
    col = lax.axis_index("col")
    row = lax.axis_index("row")
    other = {"row": 1 - row}
    x = lax.rem(col, SIDE)
    y = lax.rem(col // SIDE, SIDE)
    z = col // (SIDE * SIDE)

    def turn(pos, step):
        return lax.rem(pos + step, SIDE)

    def x_peer(step):
        return {"col": col - x + turn(x, step)}

    def y_peer(step):
        return {"col": col + SIDE * (turn(y, step) - y)}

    def z_peer(step):
        return {"col": col + SIDE * SIDE * (turn(z, step) - z)}

    def send(src, dst, send_sem, recv_sem, peer):
        return pltpu.make_async_remote_copy(
            src_ref=src, dst_ref=dst, send_sem=send_sem, recv_sem=recv_sem,
            device_id=peer, device_id_type=pl.DeviceIdType.MESH,
        )

    def signal(sem, peer):
        pl.semaphore_signal(sem, inc=1, device_id=peer, device_id_type=pl.DeviceIdType.MESH)

    def start(copies):
        for copy in copies:
            copy.start()

    def take(ref, sem):
        pltpu.make_async_copy(ref, ref, sem).wait()

    barrier = pltpu.get_barrier_semaphore()
    peers = [peer(step) for step in (1, 2, 3) for peer in (x_peer, y_peer, z_peer)] + [other]
    for peer in peers:
        signal(barrier, peer)

    owners = [turn(z, 2), turn(z, 1), turn(z, 3), z]
    block = rate.shape[1]
    v_load = pltpu.make_async_copy(v_hbm, v_raw, v_sem)
    v_load.start()
    loads = []
    for k, owner in enumerate(owners):
        rows = pl.ds(pl.multiple_of(owner * block, block), block)
        pair = [
            pltpu.make_async_copy(rate_hbm.at[rows], rate.at[k], load_sem.at[k]),
            pltpu.make_async_copy(mask_hbm.at[rows], mask.at[k], load_sem.at[k]),
        ]
        loads.append(pair)
    start(loads[0])

    def cast_chunk(k):
        def cast_step(i, carry):
            rows = pl.ds(pl.multiple_of(i * 128, 128), 128)
            seen = mask[k, rows, :]
            mqs[k, i, :, :, 0] = seen.astype(jnp.float32).astype(jnp.bfloat16).reshape(SIDE, 2, 16, items)
            rated = jnp.where(seen != 0, rate[k, rows, :], 0.0)
            mqs[k, i, :, :, 1] = rated.astype(jnp.bfloat16).reshape(SIDE, 2, 16, items)
            return carry

        lax.fori_loop(0, SIDE, cast_step, 0)

    def axis_peer(c, step):
        return y_peer(step) if c else x_peer(step)

    def share(s, c, pos):
        return mqs.at[(0, 2, 1, 3)[s], pos, :, 1] if c else mqs.at[s, :, pos, 0]

    def columns(slot):
        return slice(slot * items, (slot + 1) * items)

    m_copies, own_copies, hops, passes = [], [], [], []
    for s in range(4):
        m_copies.append([])
        own_copies.append([])
        hops.append([])
        passes.append([])
        for c, pos in enumerate((x, y)):
            for m, step in enumerate((1, 3)):
                hops[s].append(send(
                    share(s, c, turn(pos, 2)).at[:, m], hop.at[s, c, m],
                    hop_send, hop_recv.at[s], axis_peer(c, step),
                ))
                m_copies[s].append(send(
                    share(s, c, turn(pos, step)), rhs.at[s, c, :, :, :, columns(3 * c + step)],
                    m_send, m_recv.at[s], axis_peer(c, step),
                ))
                passes[s].append(send(
                    hop.at[s, c, m], rhs.at[s, c, :, m, :, columns(3 * c + 2)],
                    fwd_send, m_recv.at[s], axis_peer(c, step),
                ))
            own_copies[s].append(pltpu.make_async_copy(
                share(s, c, pos), rhs.at[s, c, :, :, :, columns(0)], own_sem.at[s]
            ))

    def pass_on(s):
        take(hop.at[s], hop_recv.at[s])
        start(passes[s])

    def half_columns(slot, side):
        return pl.ds(pl.multiple_of(slot * items + side * (items // 2), items // 2), items // 2)

    v_copies, v_swaps = [], []
    for d in (1, 3, 2):
        for axis in range(2):
            slot = 3 * axis + d
            v_copies.append(send(
                vt_all.at[:, half_columns(0, row)], vt_all.at[:, half_columns(slot, row)],
                v_send.at[0], v_recv.at[d], axis_peer(axis, d),
            ))
            v_swaps.append(send(
                vt_all.at[:, half_columns(slot, row)], vt_all.at[:, half_columns(slot, row)],
                v_send.at[1], v_recv.at[0], other,
            ))

    tmp[48:64, :] = jnp.zeros((16, items), jnp.float32)
    v_load.wait()
    tmp[0:WIDTH, :] = v_raw[...]
    vt_all[:, 0:items] = tmp[0:64, :].astype(jnp.bfloat16)
    take(rate.at[0:2], load_sem.at[0])
    for k in range(1, 4):
        start(loads[k])
    cast_chunk(0)
    pl.semaphore_wait(barrier, len(peers))
    start(v_copies)
    start(hops[0])
    start(m_copies[0])
    for step in (1, 2, 3):
        signal(y_in, y_peer(step))
    for k in range(1, 4):
        take(rate.at[0:2], load_sem.at[k])
        cast_chunk(k)
    for s in range(4):
        start(own_copies[s])
    for s in range(4):
        rhs[s, 0, :, :, :, 4 * items:7 * items] = jnp.zeros((4, 2, 16, 3 * items), jnp.bfloat16)
        rhs[s, 1, :, :, :, items:4 * items] = jnp.zeros((4, 2, 16, 3 * items), jnp.bfloat16)
    tmp[1272:1280, :] = jnp.zeros((8, items), jnp.float32)

    def outer_step(slot, carry):
        cols = pl.ds(pl.multiple_of(slot * items, items), items)
        outer_tile(vt_all[:, cols].astype(jnp.float32), tmp)
        o_all[:, cols] = tmp[...].astype(jnp.bfloat16)
        return carry

    lax.fori_loop(0, 1, outer_step, 0)
    for i, d in enumerate((1, 3, 2)):
        take(vt_all.at[:, 0:items], v_recv.at[d])
        start(v_swaps[2 * i:2 * i + 2])
    pass_on(0)
    start(hops[1])
    start(m_copies[1])
    start(hops[2])
    pl.semaphore_wait(y_in, 3)
    for step in (1, 2, 3):
        signal(z_in, z_peer(step))

    def users_of(s, m, cols):
        return rhs[s, :, :, m, :, cols].reshape(128, cols.stop - cols.start)

    near, far = slice(0, items), slice(items, 7 * items)
    def own_part(s):
        take(hop.at[s], own_sem.at[s])

        def near_step(i, carry):
            rows = pl.ds(pl.multiple_of(i * 640, 640), 640)
            home[s, rows, :] = dot_cols(o_all[rows, near], users_of(s, 0, near))
            return carry

        home[s, TRI:PACK, :] = dot_cols(vt_all[:, near], users_of(s, 1, near))
        lax.fori_loop(0, 2, near_step, 0)
    own_part(0)
    take(vt_all.at[:, 0:3 * items], v_recv.at[0])
    lax.fori_loop(1, 7, outer_step, 0)

    low = lax.broadcasted_iota(jnp.int32, (HALF, 128), 1) < 64
    pieces = (slice(0, CUT), slice(CUT, HALF))
    ways = (1, 3)

    def partial(s, dst, p):
        rows = pieces[p]
        for rows in (rows, slice(HALF + rows.start, min(HALF + rows.stop, TRI))):
            dst[rows, :] = home[s, rows, :] + dot_cols(o_all[rows, far], users_of(s, 0, far))
        if p:
            dst[TRI:PACK, :] = home[s, TRI:PACK, :] + dot_cols(vt_all[:, far], users_of(s, 1, far))

    def arrived(s):
        take(mqs.at[0, 0:3], m_recv.at[s])

    def pack_units(s, p):
        rows = pieces[p]
        partial(s, gram, p)
        here = low[:rows.stop - rows.start]
        top, bottom = gram[rows, :], gram[HALF + rows.start:HALF + rows.stop, :]
        unit[s, 0, rows, :] = jnp.where(here, top, pltpu.roll(bottom, 64, 1))
        unit[s, 1, rows, :] = jnp.where(here, pltpu.roll(top, 64, 1), bottom)

    arrived(0)
    for p, rows in enumerate(pieces):
        pack_units(0, p)
        for c in range(2):
            send(unit.at[0, c, rows], rel.at[c, rows], rel_send, rel_recv.at[p], z_peer(ways[c])).start()
    pass_on(1)
    start(m_copies[2])
    start(hops[3])
    own_part(1)
    pass_on(2)
    start(m_copies[3])
    own_part(2)
    arrived(1)
    for p, rows in enumerate(pieces):
        pack_units(1, p)
        take(rel.at[:, rows], rel_recv.at[p])
        for c in range(2):
            unit[1, c, rows, :] = unit[1, c, rows, :] + rel[c, rows, :]
            send(unit.at[1, c, rows], got.at[0, c, rows], got_send, got_recv.at[0], z_peer(ways[c])).start()
    pass_on(3)
    arrived(2)
    for p, rows in enumerate(pieces):
        pack_units(2, p)
        for c in range(2):
            send(
                unit.at[2, c, rows], got.at[1, c, rows], got_send, got_recv.at[1 + p], z_peer(ways[1 - c])
            ).start()
    own_part(3)
    arrived(3)
    for p in range(2):
        partial(3, tot, p)
    acc[PACK:FULL, :] = jnp.zeros((FULL - PACK, 128), jnp.float32)
    take(got.at[0], got_recv.at[0])
    pl.semaphore_wait(z_in, 3)
    for p, rows in enumerate(pieces):
        size = rows.stop - rows.start
        take(got.at[1, :, rows], got_recv.at[1 + p])
        sum_a = got[0, 0, rows] + got[1, 0, rows]
        sum_b = got[0, 1, rows] + got[1, 1, rows]
        here = low[:size]
        at = 2 * rows.start
        acc[at:at + size, :] = tot[rows, :] + jnp.where(here, sum_a, pltpu.roll(sum_b, 64, 1))
        acc[at + size:at + 2 * size, :] = (
            tot[HALF + rows.start:HALF + rows.stop, :] + jnp.where(here, pltpu.roll(sum_a, 64, 1), sum_b)
        )
        cols = slice(at, FULL if p else 2 * CUT)
        for i in range(cols.start // 128, cols.stop // 128):
            flat[:, i * 128:(i + 1) * 128] = acc[i * 128:(i + 1) * 128, :].T
        for d in (2, 1, 3):
            for c, pos in enumerate((y, x)):
                users = pl.ds(pl.multiple_of(64 * c + 16 * turn(pos, d), 16), 16)
                send(
                    flat.at[users, cols], fin.at[c, d - 1, :, cols], fin_send, fin_recv, axis_peer(1 - c, d)
                ).start()
    take(fin, fin_recv)

    zeros = jnp.zeros((96, 128), jnp.float32)
    for i in range(FULL // 128):
        cols = slice(i * 128, (i + 1) * 128)
        mine = [zeros]
        for c, pos in ((1, x), (0, y)):
            rows = pl.ds(pl.multiple_of(64 * c + 16 * pos, 16), 16)
            mine.insert(0, flat[rows, cols] + fin[c, 0, :, cols] + fin[c, 1, :, cols] + fin[c, 2, :, cols])
        acc[cols, :] = jnp.concatenate(mine, axis=0).T
    for rows in pieces:
        size = rows.stop - rows.start
        tot[rows, :] = acc[2 * rows.start:2 * rows.start + size, :]
        tot[HALF + rows.start:HALF + rows.stop, :] = acc[2 * rows.start + size:2 * rows.stop, :]
    solve_tiles(tot, tot.at[TRI:PACK], [fac], inv, sol)
    turned = jnp.concatenate([sol[...], jnp.zeros((72, 128), jnp.float32)], axis=0).T
    lane = lax.broadcasted_iota(jnp.int32, (16, 128), 1)
    pack[...] = jnp.where(lane < 64, turned[:16], pltpu.roll(turned[16:32], 64, 1)).astype(jnp.bfloat16)

    plane = SIDE * SIDE

    place = col - z * plane
    w_own = pltpu.make_async_copy(pack, w_all.at[col], w_recv.at[0])
    w_own.start()
    for t, turned_by in enumerate((0, 1, 3, 2)):
        base = turn(z, turned_by) * plane

        def send_step(i, carry):
            target = place + i
            target = base + jnp.where(target < plane, target, target - plane)
            send(pack, w_all.at[col], w_send, w_recv.at[(0, 2, 1, 3)[t]], {"col": target}).start()
            return carry

        lax.fori_loop(0 if t else 1, plane, send_step, 0)
    w_new[...] = turned[:32, :WIDTH]
    w_out = pltpu.make_async_copy(w_new, w_hbm, w_sem)
    w_out.start()

    users = 16 * count
    step = 16 * plane
    tall = tmp.at[:, 0:step]
    tall[1272:1280, :] = jnp.zeros((8, step), jnp.float32)

    def plane_step(t, carry):
        k = 3 - 2 * t + 3 * (t // 2)
        owner = turn(z, t + (t // 2) * (5 - 2 * t))

        take(w_all.at[0:plane], w_recv.at[t])
        for i in range(step // 128):
            rows = w_all[pl.ds(owner * plane + 8 * i, 8)].reshape(128, 128)
            wt[:, i * 128:(i + 1) * 128] = rows.astype(jnp.float32).T

        def colour_step(c, carry):
            vals = wt[pl.ds(pl.multiple_of(64 * c, 64), 64), :]
            cols = pl.ds(pl.multiple_of(c * users + k * step, step), step)
            wb[:, cols] = vals.astype(jnp.bfloat16)
            outer_tile(vals, tall)
            o_all[:, cols] = tall[...].astype(jnp.bfloat16)
            return carry

        lax.fori_loop(0, 2, colour_step, 0)
        return carry

    lax.fori_loop(0, SIDE, plane_step, 0)
    half = items // 2

    def item_rows(side, left, m):
        cols = pl.ds(pl.multiple_of(side * half, half), half)
        total = None
        for c in range(2):
            right = mqs[:, :, :, c, m, :, cols].reshape(users, half)
            term = jnp.dot(left(c), right, preferred_element_type=jnp.float32)
            total = term if total is None else total + term
        return total

    def rhs_rows(side):
        return item_rows(side, lambda c: wb[:, c * users:(c + 1) * users], 1)

    def gram_rows(side, rows):
        return item_rows(side, lambda c: o_all[rows, c * users:(c + 1) * users], 0)

    def swap_copy(i, rows):
        return send(part.at[rows], swap_got.at[rows], x_send, x_recv.at[i], other)

    def finish(i, rows, val):
        swap_copy(i, rows).wait_recv()
        item_sum[rows, :] = val + swap_got[rows, :]
        pltpu.make_async_copy(item_sum.at[rows], item_hbm.at[rows], out_sem).start()

    tail = pl.ds(TRI, PACK - TRI)
    part[tail, :] = rhs_rows(1 - row)
    swap_copy(2, tail).start()

    def away_step(i, carry):
        rows = pl.ds(pl.multiple_of(i * 640, 640), 640)
        part[rows, :] = gram_rows(1 - row, rows)
        swap_copy(i, rows).start()
        return carry

    def home_step(i, carry):
        rows = pl.ds(pl.multiple_of(i * 640, 640), 640)
        finish(i, rows, gram_rows(row, rows))
        return carry

    lax.fori_loop(0, 2, away_step, 0)
    finish(2, tail, rhs_rows(row))
    lax.fori_loop(0, 2, home_step, 0)
    w_out.wait()
    take(part, out_sem)
    take(vt_all.at[:, 0:3 * items], v_send.at[0])
    take(vt_all.at[:, 0:3 * items], v_send.at[1])
    take(mqs.at[0:2], m_send)
    take(hop, hop_send)
    take(hop, fwd_send)
    take(rel, rel_send)
    take(got, got_send)
    take(fin, fin_send)
    take(w_all.at[0:count - 1], w_send)
    take(part, x_send)


def half_steps(ratings, mask, vt, count):
    users, items = ratings.shape
    block = users // SIDE
    dma = pltpu.SemaphoreType.DMA
    any_spec = pl.BlockSpec(memory_space=pl.ANY)
    f32, bf16 = jnp.float32, jnp.bfloat16
    return pl.pallas_call(
        als_kernel,
        out_shape=(
            jax.ShapeDtypeStruct((32, WIDTH), f32),
            jax.ShapeDtypeStruct((PACK, items // 2), f32),
        ),
        in_specs=[any_spec, any_spec, any_spec],
        out_specs=(any_spec, any_spec),
        scratch_shapes=[
            pltpu.VMEM((4, block, items), f32),
            pltpu.VMEM((4, block, items), jnp.int32),
            pltpu.VMEM((WIDTH, items), f32),
            pltpu.VMEM((4, SIDE, SIDE, 2, 2, 16, items), bf16),
            pltpu.VMEM((4, 2, 2, SIDE, 16, items), bf16),
            pltpu.VMEM((4, 2, SIDE, 2, 16, 7 * items), bf16),
            pltpu.VMEM((64, 7 * items), bf16),
            pltpu.VMEM((TRI, 7 * items), bf16),
            pltpu.VMEM((TRI, items), f32),
            pltpu.VMEM((PACK, 128), f32),
            pltpu.VMEM((4, PACK, 128), f32),
            pltpu.VMEM((3, 2, HALF, 128), f32),
            pltpu.VMEM((2, HALF, 128), f32),
            pltpu.VMEM((2, 2, HALF, 128), f32),
            pltpu.VMEM((PACK, 128), f32),
            pltpu.VMEM((FULL, 128), f32),
            pltpu.VMEM((128, FULL), f32),
            pltpu.VMEM((2, 3, 16, FULL), f32),
            pltpu.VMEM((WIDTH * ROWS, 128), f32),
            pltpu.VMEM((ROWS, 128), f32),
            pltpu.VMEM((ROWS, 128), f32),
            pltpu.VMEM((32, WIDTH), f32),
            pltpu.VMEM((16, 128), bf16),
            pltpu.VMEM((count, 16, 128), bf16),
            pltpu.VMEM((128, 16 * SIDE * SIDE), f32),
            pltpu.VMEM((64, 32 * count), bf16),
            pltpu.VMEM((PACK, items // 2), f32),
            pltpu.VMEM((PACK, items // 2), f32),
            pltpu.VMEM((PACK, items // 2), f32),
            dma, dma((4,)), dma((2,)), dma((4,)), dma, dma((4,)), dma, dma((4,)), dma, dma((4,)),
            dma, dma((2,)), dma, dma((3,)), dma, dma, dma, dma((4,)), dma, dma, dma((3,)), dma,
            pltpu.SemaphoreType.REGULAR, pltpu.SemaphoreType.REGULAR,
        ],
        compiler_params=pltpu.CompilerParams(
            collective_id=0, has_side_effects=True, vmem_limit_bytes=60 * 1024 * 1024
        ),
    )(ratings, mask, vt)


def solution(mesh):
    block_spec = P(("part", "row"), "col")
    in_specs = (block_spec, block_spec, P(("part", "col"), None))
    out_specs = (P(("part", "row", "col"), None), P(("part", "col", "row"), None))
    count = mesh.shape["col"]

    def local_als(ratings, mask, v_init):
        w_own, packed = half_steps(ratings, mask, v_init.T, count)
        v_own, w_own = solve_items(packed, w_own)
        return w_own, v_own.T

    return jax.shard_map(local_als, mesh=mesh, in_specs=in_specs, out_specs=out_specs, check_vma=False)
```
